256 devices in a mesh: parts: 2 (over y), seq: 16 (over z), head: 4 (over x), rep: 2 (over core).
Axes of the slice: x: 4, y: 2, z: 16, core: 2. Of those that a mesh axis runs over, the one named last changes fastest.
The devices are a block of a 4x16x16 slice.
Arguments:
- queries: bfloat16 [4, 4096, 2048], P(('parts', 'rep'), 'seq', 'head'), parts along dimension 0, may hold values from -6 to 6
- reflect_keys: bfloat16 [4, 4096, 2, 2048], P(('parts', 'rep'), 'seq', None, 'head'), parts along dimension 0, may hold values from -6 to 6
- reflect_values: bfloat16 [4, 4096, 2, 2048], P(('parts', 'rep'), 'seq', None, 'head'), parts along dimension 0, may hold values from -6 to 6
- reflect_beta: float32 [4, 4096, 2, 16], P(('parts', 'rep'), 'seq', None, 'head'), parts along dimension 0, may hold values from 0.2 to 2
- log_decay: float32 [4, 4096, 16], P(('parts', 'rep'), 'seq', 'head'), parts along dimension 0, may hold values from -2.5 to 0
- prompt_lengths: int32 [4, 6], P(('parts', 'rep')), parts along dimension 0, may hold values from 1 to 2048, 4096 in all within a row
- norm_gain: float32 [128], replicated, may hold values from 0.1 to 1.9
- out_weight: bfloat16 [2048, 2048], P('head'), may hold values from -0.125 to 0.125
Outputs:
- layer_out: bfloat16 [4, 4096, 2048], P(('parts', 'rep'), ('seq', 'head')), parts along dimension 0
The draws below stay inside these ranges and needn't reach their ends.
There are 2 independent parts, one for each index of `parts`. The reference program is written for one: setup_inputs(seed, part) draws one part's arguments, and reference() takes and returns one part's arrays. A program takes and returns all parts, laid end to end along the dimension named above; an argument that names none is the same for every part. Nothing has to cross between parts.
Inputs may be any that keep to these rules, and one draw needn't show every extreme that they name: `prompt_lengths`: the 6 prompts of a pack lie end to end from its first token and cover all 4096 tokens; the longest has exactly 2048.
All inputs are finite; a program needn't handle non-finite values.
Results may differ from the reference program's by a relative error of at most 0.0095.
Values may be sent and summed in bfloat16 or wider, within the bound.
A program may use at most 64 MiB of HBM per device.

```python
import math
import jax
import jax.numpy as jnp
import numpy as np
from jax import lax

D = 2048
HEADS = 16
DK = 128
REFL = 2
BLOCK = 64
DOCS = 6
TOK_DEV = 256
BUNDLE_COUNT = 2
BUNDLE_SPAN = 4096
MOST_LEN = 2048
N_HEAD = 4


def slow_heads(key):
    chances = jax.random.uniform(jax.random.fold_in(key, 11), (HEADS,))
    return chances < 0.5


def draw_log_decay(key, part):
    slow_mask = slow_heads(key)
    slow_rate = jnp.exp(jax.random.uniform(jax.random.fold_in(key, 21), (HEADS,), minval=jnp.log(0.1 / MOST_LEN), maxval=jnp.log(1.0 / MOST_LEN)))
    fast_rate = jnp.exp(jax.random.uniform(jax.random.fold_in(key, 22), (HEADS,), minval=jnp.log(1.0 / 50.0), maxval=jnp.log(1.0 / 20.0)))
    channel_speed = jnp.where(slow_mask, slow_rate, fast_rate)
    uneven_quantity = jax.random.uniform(jax.random.fold_in(key, 23), (BUNDLE_COUNT, BUNDLE_SPAN, HEADS), minval=0.4, maxval=1.6)
    symbol_span = jnp.exp(jax.random.uniform(jax.random.fold_in(key, 24), (BUNDLE_COUNT, BUNDLE_SPAN // TOK_DEV, HEADS), minval=jnp.log(0.5), maxval=jnp.log(2.0)))
    symbol_span = jnp.repeat(symbol_span, TOK_DEV, axis=1)
    spike_position = jax.random.randint(jax.random.fold_in(key, 25), (BUNDLE_COUNT, 3), 0, BUNDLE_SPAN)
    spike_kept = jax.random.uniform(jax.random.fold_in(key, 26), (BUNDLE_COUNT, 3), minval=0.5, maxval=0.8)
    spike_hits = jnp.arange(BUNDLE_SPAN)[None, None, :] == spike_position[:, :, None]
    spike_log_scale = jnp.sum(jnp.where(spike_hits, jnp.log(spike_kept)[:, :, None], 0.0), axis=1)
    return (spike_log_scale[:, :, None] - channel_speed * uneven_quantity * symbol_span).astype(jnp.float32)


def draw_reflect_beta(key, part):
    slow_mask = slow_heads(key)
    margin = jnp.exp(jax.random.uniform(jax.random.fold_in(key, 31), (BUNDLE_COUNT, BUNDLE_SPAN, REFL, HEADS), minval=jnp.log(0.0001), maxval=jnp.log(0.02)))
    spread = jax.random.uniform(jax.random.fold_in(key, 32), (BUNDLE_COUNT, BUNDLE_SPAN, REFL, HEADS), minval=0.2, maxval=1.9)
    return jnp.where(slow_mask, 2.0 - margin, spread).astype(jnp.float32)


def shard_levels(rng, shape, pieces, least, top_value):
    gain, own = 1.0, jax.random.fold_in(rng, 6)
    for position, blocks in pieces:
        draws = jnp.exp(jax.random.uniform(jax.random.fold_in(own, position), (blocks,), jnp.float32, least / len(pieces), top_value / len(pieces)))
        gain = gain * jnp.repeat(draws, shape[position] // blocks).reshape([-1 if axis == position else 1 for axis in range(len(shape))])
    return gain


def profile(amount, total, reach, skew):
    loads = [(1 << 20) // math.isqrt(standing ** skew) + 1 for standing in range(2, amount + 1)]
    rest, holding = total - reach - (amount - 1), [1] * (amount - 1)
    while rest > 0:
        candidates = [i for i in range(amount - 1) if holding[i] < reach]
        pool, budget = sum([loads[i] for i in candidates]), rest
        for i in candidates:
            extra = min(reach - holding[i], max(1, budget * loads[i] // pool), rest)
            holding[i] = holding[i] + extra
            rest = rest - extra
    return np.array([reach] + holding)


def ragged(rng, count, total, limit, lean):
    if count == 2:
        one = jax.random.randint(rng, (), max(1, total - limit), min(limit, total - 1) + 1)
        return jnp.stack([one, total - one])
    tallies = jnp.asarray(profile(count, total, limit, lean), jnp.int32)
    twos = (count - 1) // 2
    donor, taker = tallies[1:1 + 2 * twos:2], tallies[2:2 + 2 * twos:2]
    room = jnp.minimum(donor - 1, limit - taker)
    moved = jax.random.randint(jax.random.fold_in(rng, 1), (twos,), 0, 1 << 20) % (room + 1)
    tallies = tallies.at[1:1 + 2 * twos:2].set(donor - moved).at[2:2 + 2 * twos:2].set(taker + moved)
    return tallies[jax.random.permutation(jax.random.fold_in(rng, 2), count)]


def scatter_about(key, extent, width, most, cuts=(), held_as=jnp.bfloat16):
    factor_of = shard_levels(key, extent, cuts, -0.22, 0.18) if cuts else 1.0
    entries = jax.random.normal(key, extent, jnp.float32) * width * factor_of
    return jnp.minimum(jnp.maximum(entries, -most), most).astype(held_as)


def setup_inputs(seed: int = 0, part: int = 0) -> dict:
    streams_of = jax.random.split(jax.random.key(seed), 9)
    own_keys = jax.random.split(jax.random.fold_in(streams_of[8], part), 9)
    queries = scatter_about(own_keys[0], (BUNDLE_COUNT, BUNDLE_SPAN, HEADS * DK), 1.0, 6.0, ((0, 2), (1, 16), (2, 4)))
    reflect_keys = scatter_about(own_keys[1], (BUNDLE_COUNT, BUNDLE_SPAN, REFL, HEADS * DK), 1.0, 6.0, ((0, 2), (1, 16), (3, 4)))
    reflect_values = scatter_about(own_keys[2], (BUNDLE_COUNT, BUNDLE_SPAN, REFL, HEADS * DK), 1.0, 6.0, ((0, 2), (1, 16), (3, 4)))
    reflect_beta = draw_reflect_beta(jax.random.fold_in(jax.random.fold_in(streams_of[8], part), 71), part)
    log_decay = draw_log_decay(jax.random.fold_in(jax.random.fold_in(streams_of[8], part), 71), part)
    prompt_lengths = jax.vmap(lambda own: ragged(own, DOCS, BUNDLE_SPAN, MOST_LEN, 2))(jax.random.split(own_keys[5], BUNDLE_COUNT)).reshape((BUNDLE_COUNT, DOCS)).astype(jnp.int32)
    norm_gain = jnp.clip(1.0 + 0.18 * jax.random.normal(streams_of[6], (DK,), jnp.float32), 0.1, 1.9)
    out_weight = scatter_about(streams_of[7], (HEADS * DK, D), (HEADS * DK) ** -0.5, 0.125, ((0, 4),))
    return dict(queries=queries, reflect_keys=reflect_keys, reflect_values=reflect_values, reflect_beta=reflect_beta, log_decay=log_decay, prompt_lengths=prompt_lengths, norm_gain=norm_gain, out_weight=out_weight)


highest = lax.Precision.HIGHEST
epsilon = 1e-06

def unit_rows(vectors):
    return vectors * lax.rsqrt(lax.optimization_barrier(jnp.sum(vectors * vectors, axis=-1, keepdims=True)) + epsilon)

def block_parts(key_rows, value_rows, beta_rows, decay_rows, seg_rows, seg_before):
    steps_here = key_rows.shape[-2]
    cum_decay = jnp.cumsum(decay_rows, axis=-1)
    ordinal = jnp.arange(steps_here)
    incl_mask = ordinal[:, None] >= ordinal[None, :]
    strict_mask = ordinal[:, None] > ordinal[None, :]
    same_doc = seg_rows[:, None, :, None] == seg_rows[:, None, None, :]
    decay_gap = cum_decay[..., :, None] - cum_decay[..., None, :]
    decay_ratio = jnp.where(incl_mask & same_doc, jnp.exp(jnp.minimum(decay_gap, 0.0)), 0.0)
    carry_in = jnp.where(seg_rows[:, None, :] == seg_before[:, None, None], jnp.exp(cum_decay), 0.0)
    key_inner = jnp.einsum('bhik,bhjk->bhij', key_rows, key_rows, precision=highest)
    system = jnp.eye(steps_here, dtype=key_rows.dtype) + jnp.where(strict_mask, beta_rows[..., :, None] * decay_ratio * key_inner, 0.0)
    right_side = jnp.concatenate([beta_rows[..., None] * value_rows, (beta_rows * carry_in)[..., None] * key_rows], axis=-1)
    solved = lax.linalg.triangular_solve(system, right_side, left_side=True, lower=True, unit_diagonal=True)
    val_width = value_rows.shape[-1]
    return (decay_ratio, carry_in, solved[..., :val_width], solved[..., val_width:])

def reference(queries, reflect_keys, reflect_values, reflect_beta, log_decay, prompt_lengths, norm_gain, out_weight):
    pack_count = queries.shape[0]
    length = queries.shape[1]
    blocks = length // BLOCK
    sub_steps = REFL * BLOCK
    doc_ends = jnp.cumsum(prompt_lengths, axis=-1).astype(jnp.int32)
    positions = jnp.arange(length, dtype=jnp.int32)
    segment = lax.optimization_barrier(jnp.sum((positions[None, :, None] >= doc_ends[:, None, :]).astype(jnp.int32), axis=-1)).astype(jnp.int32)
    query_rows = unit_rows(queries.astype(jnp.float32).reshape(pack_count, blocks, BLOCK, HEADS, DK)) * DK ** (-0.5)
    query_rows = query_rows.transpose(1, 0, 3, 2, 4)
    key_rows = unit_rows(reflect_keys.astype(jnp.float32).reshape(pack_count, blocks, BLOCK, REFL, HEADS, DK))
    key_rows = key_rows.transpose(1, 0, 4, 2, 3, 5).reshape(blocks, pack_count, HEADS, sub_steps, DK)
    value_rows = reflect_values.astype(jnp.float32).reshape(pack_count, blocks, BLOCK, REFL, HEADS, DK)
    value_rows = value_rows.transpose(1, 0, 4, 2, 3, 5).reshape(blocks, pack_count, HEADS, sub_steps, DK)
    beta_rows = reflect_beta.reshape(pack_count, blocks, BLOCK, REFL, HEADS).transpose(1, 0, 4, 2, 3).reshape(blocks, pack_count, HEADS, sub_steps)
    gate_rows = log_decay.reshape(pack_count, blocks, BLOCK, HEADS).transpose(1, 0, 3, 2)
    decay_rows = jnp.concatenate([gate_rows[..., None], jnp.zeros(gate_rows.shape + (REFL - 1,), jnp.float32)], axis=-1).reshape(blocks, pack_count, HEADS, sub_steps)
    seg_rows = jnp.repeat(segment.reshape(pack_count, blocks, BLOCK), REFL, axis=-1).transpose(1, 0, 2).astype(jnp.int32)
    last_row = REFL - 1

    def one_block(carried, inputs):
        state, seg_before = carried
        query_block, key_block, value_block, beta_block, decay_block, seg_block = inputs
        decay_ratio, carry_in, write_vals, write_keys = block_parts(key_block, value_block, beta_block, decay_block, seg_block, seg_before)
        updates = write_vals - jnp.einsum('bhck,bhkv->bhcv', write_keys, state, precision=highest)
        read_weights = decay_ratio[..., last_row::REFL, :] * jnp.einsum('bhik,bhjk->bhij', query_block, key_block, precision=highest)
        carry_read = carry_in[..., last_row::REFL]
        head_out = carry_read[..., None] * jnp.einsum('bhik,bhkv->bhiv', query_block, state, precision=highest) + jnp.einsum('bhij,bhjv->bhiv', read_weights, updates, precision=highest)
        end_keys = decay_ratio[..., -1, :, None] * key_block
        new_state = carry_in[..., -1, None, None] * state + jnp.einsum('bhjk,bhjl->bhkl', end_keys, updates, precision=highest)
        return ((new_state, seg_block[:, -1].astype(jnp.int32)), head_out)
    initial = (jnp.zeros((pack_count, HEADS, DK, DK), jnp.float32), jnp.full((pack_count,), -1, jnp.int32))
    finished, outputs = lax.scan(one_block, initial, (query_rows, key_rows, value_rows, beta_rows, decay_rows, seg_rows))
    outputs = outputs.transpose(1, 0, 3, 2, 4)
    normed = (outputs * lax.rsqrt(lax.optimization_barrier(jnp.mean(outputs * outputs, axis=-1, keepdims=True)) + epsilon) * norm_gain).astype(jnp.bfloat16)
    flat_rows = normed.reshape(pack_count, length, HEADS * DK)
    group_width = HEADS * DK // N_HEAD
    total_sum = jnp.zeros((pack_count, length, out_weight.shape[1]), jnp.float32)
    for group_index in range(N_HEAD):
        lower_col = group_index * group_width
        upper_col = lower_col + group_width
        partial_sum = jnp.dot(flat_rows[..., lower_col:upper_col].astype(jnp.float32), out_weight[lower_col:upper_col].astype(jnp.float32), preferred_element_type=jnp.float32).astype(jnp.bfloat16)
        partial_sum = lax.optimization_barrier(partial_sum)
        total_sum = total_sum + partial_sum.astype(jnp.float32)
    return total_sum.astype(jnp.bfloat16)
```

```python
import functools

import jax
import jax.numpy as jnp
from jax import lax
from jax.experimental import pallas as pl
from jax.experimental.pallas import tpu as pltpu
from jax.sharding import PartitionSpec as P

BLOCK = 64
LONGEST = 2048
EPS = 1e-06
FAR = -1e30
MESH = pl.DeviceIdType.MESH
f32 = jnp.float32
bf16 = jnp.bfloat16


def mm(a, b):
    return lax.dot_general(a, b, (((1,), (0,)), ((), ())), preferred_element_type=f32)


def mm_t(a, b):
    return lax.dot_general(a, b, (((1,), (1,)), ((), ())), preferred_element_type=f32)


def split(x):
    hi = x.astype(bf16)
    return hi, (x - hi.astype(f32)).astype(bf16)


def iota(shape, dim):
    return lax.broadcasted_iota(jnp.int32, shape, dim)


def exact(a, b):
    return lax.dot_general(
        a, b, (((1,), (0,)), ((), ())), preferred_element_type=f32, precision=lax.Precision.HIGHEST
    )


def seg_of(pos, ends):
    total = jnp.zeros_like(pos)
    for end in ends:
        total = total + (pos >= end).astype(jnp.int32)
    return total


def rows_of(gate, beta, refl):
    tokens = gate.shape[1]
    subs = tokens * refl
    t, r = iota((tokens, subs), 0), iota((tokens, subs), 1) // refl
    upto = ((t <= r) & (t // BLOCK == r // BLOCK)).astype(f32)
    src, dst = iota((subs, subs), 0), iota((subs, subs), 1)
    place = (dst == (src % tokens) * refl + src // tokens).astype(f32)
    t2, r2 = iota((tokens, tokens), 0), iota((tokens, tokens), 1)
    upto_token = ((t2 <= r2) & (t2 // BLOCK == r2 // BLOCK)).astype(f32)
    return exact(gate, upto), exact(beta, place), exact(gate, upto_token)


def block_masks(offset, ends, block, refl):
    n = refl * BLOCK
    start = offset + block * BLOCK
    before = sum((start - 1 >= e).astype(jnp.int32) for e in ends)
    before = jnp.where(start == 0, -1, before)
    last = sum((start + BLOCK - 1 >= e).astype(jnp.int32) for e in ends)
    seg_row = seg_of(start + iota((1, n), 1) // refl, ends)
    seg_col = seg_of(start + iota((n, 1), 0) // refl, ends)
    seg_tok = seg_of(start + iota((BLOCK, 1), 0), ends)
    i, j = iota((n, n), 0), iota((n, n), 1)
    pair = jnp.where((i >= j) & (seg_col == seg_row), 0.0, FAR)
    ti, tj = iota((BLOCK, n), 0), iota((BLOCK, n), 1)
    read = jnp.where((ti >= tj // refl) & (seg_tok == seg_row), 0.0, FAR)
    carry_row = jnp.where(seg_row == before, 0.0, FAR)
    carry_tok = jnp.where(seg_tok == before, 0.0, FAR)
    end_col = jnp.where(seg_col == last, 0.0, FAR)
    return pair, read, carry_row, carry_tok, end_col


def level_mask(n, level):
    i, j = iota((n, n), 0), iota((n, n), 1)
    return ((i > j) & (lax.shift_right_logical(i ^ j, level) == 1)).astype(f32).astype(bf16)


def levels_of(n):
    return n.bit_length() - 1


def head_maps(blocks, masks, eye, levels):
    n = eye.shape[0]
    width = blocks[0][0].shape[1]
    scale = width**-0.5
    eye16 = eye.astype(bf16)
    grams, lowers, xs, norms = [], [], [], []
    for (k, v, q, c_row, c_col, b_row, b_col, ct_col), (pair, *_) in zip(blocks, masks):
        both = mm_t(jnp.concatenate([k, q], axis=0), k)
        gram, qk = both[:n], both[n:]
        diag = gram * eye
        n_row = lax.rsqrt(jnp.sum(diag, axis=0, keepdims=True) + EPS)
        n_col = lax.rsqrt(jnp.sum(diag, axis=1, keepdims=True) + EPS)
        ratio = jnp.exp((c_col - c_row) + pair)
        lower = ((b_col * n_col) * ratio) * (n_row * gram)
        lower = lower - lower * eye
        grams.append(qk)
        norms.append((n_row, n_col))
        lowers.append(split(lower))
    xs = [eye16 - low[0] * levels(0) for low in lowers]
    for level in range(1, levels_of(n)):
        mask = levels(level)
        ys = [mm(low[0] * mask, x).astype(bf16) for low, x in zip(lowers, xs)]
        xs = [x - mm(x, y).astype(bf16) for x, y in zip(xs, ys)]
    outs = []
    lefts = [
        mm(jnp.concatenate(low, axis=1), jnp.concatenate([x, x], axis=0))
        for low, x in zip(lowers, xs)
    ]
    rests = [((eye - x.astype(f32)) - left).astype(bf16) for x, left in zip(xs, lefts)]
    invs = [x.astype(f32) + mm(x, rest) for x, rest in zip(xs, rests)]
    values, keys = [], []
    for inv, (k, v, q, c_row, c_col, b_row, b_col, ct_col), m, (n_row, n_col) in zip(
        invs, blocks, masks, norms
    ):
        carry_row = jnp.exp(c_row + m[2])
        for_value = inv * b_row
        for_key = inv * (b_row * carry_row * n_row)
        values.append(
            mm(jnp.concatenate(split(for_value), axis=1), jnp.concatenate([v, v], axis=0))
        )
        keys.append(mm(jnp.concatenate(split(for_key), axis=1), jnp.concatenate([k, k], axis=0)))
    maps, reads = [], []
    for wv, wk, qk, (k, v, q, c_row, c_col, b_row, b_col, ct_col), m, (n_row, n_col) in zip(
        values, keys, grams, blocks, masks, norms
    ):
        both = jnp.concatenate([wv, wk], axis=1)
        c_last = c_row[:, n - 1 :]
        end = jnp.exp((c_last - c_col) + m[4]) * n_col
        hi, lo = split(both * end)
        kt = jnp.transpose(k)
        ew = mm(jnp.concatenate([kt, kt], axis=1), jnp.concatenate([hi, lo], axis=0))
        carry_last = jnp.exp(c_last + m[2][:, n - 1 :])
        maps.append((carry_last * eye - ew[:, width:], ew[:, :width]))
        qf = q.astype(f32)
        nq = lax.rsqrt(jnp.sum(qf * qf, axis=1, keepdims=True) + EPS) * scale
        weights = jnp.exp((ct_col - c_row) + m[1]) * nq * (n_row * qk)
        got = mm(weights.astype(bf16), both.astype(bf16))
        carry_tok = jnp.exp(ct_col + m[3])
        reads.append(((carry_tok * nq) * qf - got[:, width:], got[:, :width]))
    total = jnp.concatenate(maps[0], axis=1)
    g_rows, o_rows = [reads[0][0].astype(bf16)], [reads[0][1]]
    for (map_b, add_b), (qeff, o) in zip(maps[1:], reads[1:]):
        hi, lo = split(total)
        m_hi, m_lo = split(map_b)
        q16 = qeff.astype(bf16)
        left = jnp.concatenate(
            [
                jnp.concatenate([m_hi, m_lo], axis=1),
                jnp.concatenate([q16, jnp.zeros_like(q16)], axis=1),
            ],
            axis=0,
        )
        wide = mm(left, jnp.concatenate([hi, hi], axis=0))
        total = wide[:n] + mm(m_hi, lo)
        total = jnp.concatenate([total[:, :width], total[:, width:] + add_b], axis=1)
        g_rows.append(wide[n:, :width].astype(bf16))
        o_rows.append(o + wide[n:, width:])
    return total[:, :width], total[:, width:], g_rows, o_rows


def kernel(
    n_seq,
    n_head,
    rounds,
    q_hbm,
    k_hbm,
    v_hbm,
    beta_ref,
    gate_ref,
    len_ref,
    gain_ref,
    w_hbm,
    out_ref,
    q_s,
    k_s,
    v_s,
    w_s,
    row_s,
    col_c,
    col_b,
    col_t,
    pair_s,
    read_s,
    crow_s,
    ctok_s,
    ecol_s,
    eye_s,
    lev_s,
    map_s,
    add_s,
    g_s,
    o_s,
    send_s,
    recv_s,
    norm_s,
    part_s,
    got_s,
    in_sem,
    w_sem,
    ring_send,
    ring_recv,
    x_send,
    x_recv,
):
    z = lax.axis_index("seq")
    x = lax.axis_index("head")
    heads, subs, width = k_s.shape
    tokens = q_s.shape[1]
    refl = subs // tokens
    blocks = tokens // BLOCK
    n = refl * BLOCK
    ahead, behind = lax.rem(z + 1, n_seq), lax.rem(z + n_seq - 1, n_seq)

    barrier = pltpu.get_barrier_semaphore()
    pl.semaphore_signal(barrier, inc=1, device_id={"seq": ahead}, device_id_type=MESH)
    pl.semaphore_signal(barrier, inc=1, device_id={"seq": behind}, device_id_type=MESH)
    for o in range(1, n_head):
        pl.semaphore_signal(
            barrier, inc=1, device_id={"head": lax.rem(x + o, n_head)}, device_id_type=MESH
        )

    k_rows = k_hbm.reshape(subs, heads * width)
    v_rows = v_hbm.reshape(subs, heads * width)

    def loads(h):
        lanes = pl.ds(pl.multiple_of(h * width, width), width)
        return (
            pltpu.make_async_copy(k_rows.at[:, lanes], k_s.at[h], in_sem.at[0, h]),
            pltpu.make_async_copy(v_rows.at[:, lanes], v_s.at[h], in_sem.at[1, h]),
            pltpu.make_async_copy(q_hbm.at[:, lanes], q_s.at[h], in_sem.at[2, h]),
        )

    for h in range(heads):
        for copy in loads(h):
            copy.start()
    w_copy = pltpu.make_async_copy(w_hbm, w_s, w_sem)
    w_copy.start()

    offset = z * tokens
    ends, run = [], 0
    for i in range(len_ref.shape[0]):
        run = run + len_ref[i]
        ends.append(run)
    beta = jnp.concatenate([beta_ref[j] for j in range(refl)], axis=1)
    c_exp, b_exp, c_tok = rows_of(gate_ref[...], beta, refl)
    rows = jnp.concatenate([c_exp, b_exp], axis=0)
    for i in range(2 * heads):
        row_s[i] = rows[i : i + 1]
    cols = jnp.transpose(rows)
    cols_t = jnp.transpose(jnp.concatenate([c_tok, c_tok], axis=0))
    for h in range(heads):
        col_c[h] = cols[:, h : h + 1]
        col_b[h] = cols[:, heads + h : heads + h + 1]
        col_t[h] = cols_t[:, h : h + 1]
    for b in range(blocks):
        pair_s[b], read_s[b], crow_s[b], ctok_s[b], ecol_s[b] = block_masks(offset, ends, b, refl)
    eye_s[...] = (iota((n, n), 0) == iota((n, n), 1)).astype(f32)
    for level in range(levels_of(n)):
        lev_s[level] = level_mask(n, level)

    def hop(r, h):
        return pltpu.make_async_remote_copy(
            src_ref=send_s.at[r, h],
            dst_ref=recv_s.at[r, h],
            send_sem=ring_send.at[r, h],
            recv_sem=ring_recv.at[r, h],
            device_id={"seq": ahead},
            device_id_type=MESH,
        )

    def step(r, h):
        hop(r - 1, h).wait_recv()
        got = recv_s[r - 1, h]
        state = add_s[h] + mm(map_s[h], jnp.concatenate([got, got], axis=0))
        send_s[r, h] = state.astype(bf16)
        hop(r, h).start()

    def one_head(h, carry):
        for copy in loads(h):
            copy.wait()
        data, masks = [], []
        for b in range(blocks):
            subs_b, toks_b = pl.ds(b * n, n), pl.ds(b * BLOCK, BLOCK)
            data.append(
                (
                    k_s[h, subs_b, :],
                    v_s[h, subs_b, :],
                    q_s[h, toks_b, :],
                    row_s[h, :, subs_b],
                    col_c[h, subs_b, :],
                    row_s[heads + h, :, subs_b],
                    col_b[h, subs_b, :],
                    col_t[h, toks_b, :],
                )
            )
            masks.append((pair_s[b], read_s[b], crow_s[b], ctok_s[b], ecol_s[b]))
        total, add, g_rows, o_rows = head_maps(data, masks, eye_s[...], lambda l: lev_s[l])
        map_s[h] = jnp.concatenate(split(total), axis=1)
        add_s[h] = add
        for b in range(blocks):
            g_s[h, pl.ds(b * BLOCK, BLOCK), :] = g_rows[b]
            o_s[h, pl.ds(b * BLOCK, BLOCK), :] = o_rows[b]

        @pl.when(h == 0)
        def _():
            pl.semaphore_wait(barrier, n_head + 1)

        send_s[0, h] = add.astype(bf16)
        hop(0, h).start()

        def earlier(e, c):
            step(h - e, e)
            return c

        lax.fori_loop(0, h, earlier, 0)
        return carry

    lax.fori_loop(0, heads, one_head, 0)

    for wave in range(heads, rounds - 1 + heads):
        for h in range(heads):
            r = wave - h
            if 1 <= r < rounds:
                step(r, h)

    w_copy.wait()
    for h in range(heads):
        hop(rounds - 1, h).wait_recv()
        out = o_s[h] + mm(g_s[h], recv_s[rounds - 1, h])
        mean = jnp.sum(out * out, axis=1, keepdims=True) * (1.0 / width)
        norm_s[:, h * width : (h + 1) * width] = (
            out * lax.rsqrt(mean + EPS) * gain_ref[...]
        ).astype(bf16)

    chunks = part_s.shape[0]
    cols_n = part_s.shape[2]
    share = out_ref.shape[0]

    def give(o, c):
        dest = lax.rem(x + o, n_head)
        return pltpu.make_async_remote_copy(
            src_ref=part_s.at[c, pl.ds(pl.multiple_of(dest * share, share), share), :],
            dst_ref=got_s.at[o - 1, c],
            send_sem=x_send.at[o - 1, c],
            recv_sem=x_recv.at[o - 1, c],
            device_id={"head": dest},
            device_id_type=MESH,
        )

    normed = norm_s[...]
    for c in range(chunks):
        part_s[c] = mm(normed, w_s[:, c * cols_n : (c + 1) * cols_n]).astype(bf16)
        for o in (2, 1, 3):
            give(o, c).start()
    own = pl.ds(pl.multiple_of(x * share, share), share)
    for c in range(chunks):
        total = part_s[c, own, :].astype(f32)
        for o in (1, 3, 2):
            give(o, c).wait_recv()
            total = total + got_s[o - 1, c].astype(f32)
        out_ref[:, c * cols_n : (c + 1) * cols_n] = total.astype(bf16)

    def drain(r, c):
        for h in range(heads):
            hop(r, h).wait_send()
        return c

    lax.fori_loop(0, rounds, drain, 0)
    for c in range(chunks):
        for o in range(1, n_head):
            give(o, c).wait_send()


def solution(mesh):
    n_seq, n_head = mesh.shape["seq"], mesh.shape["head"]

    def body(queries, keys, values, beta, gate, lengths, gain, weight):
        tokens, lanes = queries.shape[1:]
        refl, heads = beta.shape[2:]
        width = lanes // heads
        subs = tokens * refl
        blocks = tokens // BLOCK
        n = refl * BLOCK
        model = weight.shape[1]
        share = tokens // n_head
        rounds = min(n_seq - 1, -(-LONGEST // tokens))
        chunks = 4
        hbm = pl.BlockSpec(memory_space=pl.ANY)
        vmem = pl.BlockSpec(memory_space=pltpu.VMEM)
        smem = pl.BlockSpec(memory_space=pltpu.SMEM)
        out = pl.pallas_call(
            functools.partial(kernel, n_seq, n_head, rounds),
            out_shape=jax.ShapeDtypeStruct((share, model), bf16),
            in_specs=[hbm, hbm, hbm, vmem, vmem, smem, vmem, hbm],
            out_specs=vmem,
            scratch_shapes=[
                pltpu.VMEM((heads, tokens, width), bf16),
                pltpu.VMEM((heads, subs, width), bf16),
                pltpu.VMEM((heads, subs, width), bf16),
                pltpu.VMEM((lanes, model), bf16),
                pltpu.VMEM((2 * heads, 1, subs), f32),
                pltpu.VMEM((heads, subs, 1), f32),
                pltpu.VMEM((heads, subs, 1), f32),
                pltpu.VMEM((heads, tokens, 1), f32),
                pltpu.VMEM((blocks, n, n), f32),
                pltpu.VMEM((blocks, BLOCK, n), f32),
                pltpu.VMEM((blocks, 1, n), f32),
                pltpu.VMEM((blocks, BLOCK, 1), f32),
                pltpu.VMEM((blocks, n, 1), f32),
                pltpu.VMEM((n, n), f32),
                pltpu.VMEM((levels_of(n), n, n), bf16),
                pltpu.VMEM((heads, width, 2 * width), bf16),
                pltpu.VMEM((heads, width, width), f32),
                pltpu.VMEM((heads, tokens, width), bf16),
                pltpu.VMEM((heads, tokens, width), f32),
                pltpu.VMEM((rounds, heads, width, width), bf16),
                pltpu.VMEM((rounds, heads, width, width), bf16),
                pltpu.VMEM((tokens, lanes), bf16),
                pltpu.VMEM((chunks, tokens, model // chunks), bf16),
                pltpu.VMEM((n_head - 1, chunks, share, model // chunks), bf16),
                pltpu.SemaphoreType.DMA((3, heads)),
                pltpu.SemaphoreType.DMA,
                pltpu.SemaphoreType.DMA((rounds, heads)),
                pltpu.SemaphoreType.DMA((rounds, heads)),
                pltpu.SemaphoreType.DMA((n_head - 1, chunks)),
                pltpu.SemaphoreType.DMA((n_head - 1, chunks)),
            ],
            compiler_params=pltpu.CompilerParams(
                collective_id=0, has_side_effects=True, vmem_limit_bytes=48 * 1024 * 1024
            ),
        )(
            queries[0],
            keys[0],
            values[0],
            jnp.transpose(beta[0], (1, 2, 0)),
            jnp.transpose(gate[0], (1, 0)),
            lengths[0],
            gain[None, :],
            weight,
        )
        return out[None]

    packs = ("parts", "rep")
    in_specs = (
        P(packs, "seq", "head"),
        P(packs, "seq", None, "head"),
        P(packs, "seq", None, "head"),
        P(packs, "seq", None, "head"),
        P(packs, "seq", "head"),
        P(packs, None),
        P(),
        P("head", None),
    )
    out_specs = P(packs, ("seq", "head"), None)
    return jax.shard_map(body, mesh=mesh, in_specs=in_specs, out_specs=out_specs, check_vma=False)
```

```python
import functools

import jax
import jax.numpy as jnp
from jax import lax
from jax.experimental import pallas as pl
from jax.experimental.pallas import tpu as pltpu
from jax.sharding import PartitionSpec as P

BLOCK = 64
LONGEST = 2048
EPS = 1e-06
FAR = -1e30
MESH = pl.DeviceIdType.MESH
f32 = jnp.float32
bf16 = jnp.bfloat16


def mm(a, b):
    return lax.dot_general(a, b, (((1,), (0,)), ((), ())), preferred_element_type=f32)


def mm_t(a, b):
    return lax.dot_general(a, b, (((1,), (1,)), ((), ())), preferred_element_type=f32)


def split(x):
    hi = x.astype(bf16)
    return hi, (x - hi.astype(f32)).astype(bf16)


def iota(shape, dim):
    return lax.broadcasted_iota(jnp.int32, shape, dim)


def split3(x):
    first = x.astype(bf16)
    rest = x - first.astype(f32)
    second = rest.astype(bf16)
    return first, second, (rest - second.astype(f32)).astype(bf16)


def seg_of(pos, ends):
    total = jnp.zeros_like(pos)
    for end in ends:
        total = total + (pos >= end).astype(jnp.int32)
    return total


def vectors(gate, beta):
    heads, tokens = gate.shape
    n = 2 * BLOCK
    blocks = tokens // BLOCK
    left = []
    for b in range(blocks):
        at = slice(b * BLOCK, (b + 1) * BLOCK)
        part = gate[:, at]
        left.append(jnp.concatenate([part, jnp.zeros_like(part)], axis=1))
        left.append(jnp.concatenate([beta[0][:, at], beta[1][:, at]], axis=1))
    left = jnp.concatenate(left, axis=0)
    count = left.shape[0]
    k, r = iota((n, n), 0), iota((n, n), 1)
    upto = ((k < BLOCK) & (k <= r // 2)).astype(f32)
    place = (r == 2 * (k % BLOCK) + k // BLOCK).astype(f32)
    token = ((k < BLOCK) & (k <= r)).astype(f32)
    table = jnp.concatenate([upto, place, token], axis=1).astype(bf16)
    got = mm(jnp.concatenate(split3(left), axis=0), table)
    got = got[:count] + got[count : 2 * count] + got[2 * count :]
    both = 2 * heads
    first = iota((both, n), 0) < heads
    rows, toks = [], []
    for b in range(blocks):
        mine = got[b * both : (b + 1) * both]
        rows.append(jnp.where(first, mine[:, :n], mine[:, n : 2 * n]))
        toks.append(mine[:, 2 * n :])
    return rows, toks


def block_masks(offset, ends, block):
    n = 2 * BLOCK
    start = offset + block * BLOCK
    before = sum((start - 1 >= e).astype(jnp.int32) for e in ends)
    before = jnp.where(start == 0, -1, before)
    last = sum((start + BLOCK - 1 >= e).astype(jnp.int32) for e in ends)
    seg_row = seg_of(start + iota((1, n), 1) // 2, ends)
    seg_col = seg_of(start + iota((n, 1), 0) // 2, ends)
    seg_tok = seg_of(start + iota((BLOCK, 1), 0), ends)
    i, j = iota((n, n), 0), iota((n, n), 1)
    pair = jnp.where((i >= j) & (seg_col == seg_row), 0.0, FAR)
    ti, tj = iota((BLOCK, n), 0), iota((BLOCK, n), 1)
    read = jnp.where((ti >= tj // 2) & (seg_tok == seg_row), 0.0, FAR)
    carry_row = jnp.where(seg_row == before, 0.0, FAR)
    carry_tok = jnp.where(seg_tok == before, 0.0, FAR)
    end_row = jnp.where(seg_row == last, 0.0, FAR)
    return pair, read, carry_row, carry_tok, end_row


def level_mask(n, level):
    i, j = iota((n, n), 0), iota((n, n), 1)
    return ((i > j) & (lax.shift_right_logical(i ^ j, level) == 1)).astype(f32).astype(bf16)


def levels_of(n):
    return n.bit_length() - 1


def as_cols(rows):
    cols = jnp.transpose(jnp.concatenate(rows, axis=0))
    return [cols[:, u : u + 1] for u in range(len(rows))]


def state_maps(units, masks, eye, levels):
    n = eye.shape[0]
    width = units[0][0].shape[1]
    eye16 = eye.astype(bf16)
    grams = [mm_t(k, k) for k, *_ in units]
    norms = [
        lax.rsqrt(jnp.sum(gram * eye, axis=0, keepdims=True) + EPS) for gram in grams
    ]
    beta_cols = as_cols([norm * unit[4] for norm, unit in zip(norms, units)])
    end_cols = as_cols(
        [
            jnp.exp((unit[2][:, n - 1 :] - unit[2]) + mask[4]) * norm
            for norm, unit, mask in zip(norms, units, masks)
        ]
    )
    lowers = []
    for gram, norm, beta_col, (k, v, c_row, c_col, b_row), mask in zip(
        grams, norms, beta_cols, units, masks
    ):
        ratio = jnp.exp((c_col - c_row) + mask[0])
        lower = (beta_col * ratio) * (norm * gram)
        lowers.append(split(lower - lower * eye))
    xs = [eye16 - low[0] * levels(0) for low in lowers]
    for level in range(1, levels_of(n)):
        mask = levels(level)
        ys = [mm(low[0] * mask, x).astype(bf16) for low, x in zip(lowers, xs)]
        xs = [x - mm(x, y).astype(bf16) for x, y in zip(xs, ys)]
    lefts = [
        mm(jnp.concatenate(low, axis=1), jnp.concatenate([x, x], axis=0))
        for low, x in zip(lowers, xs)
    ]
    rests = [((eye - x.astype(f32)) - left).astype(bf16) for x, left in zip(xs, lefts)]
    invs = [x.astype(f32) + mm(x, rest) for x, rest in zip(xs, rests)]
    writes = []
    for inv, norm, (k, v, c_row, c_col, b_row), mask in zip(invs, norms, units, masks):
        for_value = inv * b_row
        for_key = inv * (b_row * jnp.exp(c_row + mask[2]) * norm)
        wv = mm(jnp.concatenate(split(for_value), axis=1), jnp.concatenate([v, v], axis=0))
        wk = mm(jnp.concatenate(split(for_key), axis=1), jnp.concatenate([k, k], axis=0))
        writes.append(jnp.concatenate([wv, wk], axis=1))
    outs = []
    for write, end, norm, (k, v, c_row, c_col, b_row), mask in zip(
        writes, end_cols, norms, units, masks
    ):
        hi, lo = split(write * end)
        kt = jnp.transpose(k)
        ew = mm(jnp.concatenate([kt, kt], axis=1), jnp.concatenate([hi, lo], axis=0))
        carry_last = jnp.exp(c_row[:, n - 1 :] + mask[2][:, n - 1 :])
        outs.append((carry_last * eye - ew[:, width:], ew[:, :width], write.astype(bf16), norm))
    return outs


def compose(maps):
    width = maps[0][0].shape[1]
    totals = [jnp.concatenate(maps[0], axis=1)]
    for map_b, add_b in maps[1:]:
        hi, lo = split(totals[-1])
        m_hi, m_lo = split(map_b)
        total = mm(jnp.concatenate([m_hi, m_lo], axis=1), jnp.concatenate([hi, hi], axis=0))
        total = total + mm(m_hi, lo)
        totals.append(jnp.concatenate([total[:, :width], total[:, width:] + add_b], axis=1))
    return totals


def block_reads(q, k, write, norm, c_row, ct_col, mask, before):
    width = q.shape[1]
    qf = q.astype(f32)
    nq = lax.rsqrt(jnp.sum(qf * qf, axis=1, keepdims=True) + EPS) * width**-0.5
    weights = (jnp.exp((ct_col - c_row) + mask[1]) * nq) * (norm * mm_t(q, k))
    got = mm(weights.astype(bf16), write)
    reads = (jnp.exp(ct_col + mask[3]) * nq) * qf - got[:, width:]
    if before is None:
        return reads.astype(bf16), got[:, :width]
    wide = mm(reads.astype(bf16), before)
    return wide[:, :width].astype(bf16), got[:, :width] + wide[:, width:]


def kernel(
    n_seq,
    n_head,
    rounds,
    q_hbm,
    k_hbm,
    v_hbm,
    beta_hbm,
    gate_hbm,
    len_hbm,
    gain_hbm,
    w_hbm,
    out_ref,
    q_s,
    k_s,
    v_s,
    w_s,
    beta_s,
    gate_s,
    len_s,
    gain_s,
    row_s,
    col_s,
    tok_s,
    pair_s,
    read_s,
    crow_s,
    ctok_s,
    erow_s,
    eye_s,
    lev_s,
    write_s,
    norm_s,
    before_s,
    map_s,
    add_s,
    g_s,
    o_s,
    send_s,
    recv_s,
    flat_s,
    part_s,
    relay_s,
    sum_s,
    got_s,
    in_sem,
    small_sem,
    w_sem,
    ring_send,
    ring_recv,
    relay_send,
    relay_recv,
    x_send,
    x_recv,
):
    z = lax.axis_index("seq")
    x = lax.axis_index("head")
    heads, subs, width = k_s.shape
    tokens = q_s.shape[1]
    blocks = tokens // BLOCK
    n = 2 * BLOCK
    right, left = lax.rem(x + 1, n_head), lax.rem(x + n_head - 1, n_head)
    has_before, has_after = z > 0, z < n_seq - 1

    smalls = [
        pltpu.make_async_copy(src, dst, small_sem.at[i])
        for i, (src, dst) in enumerate(
            ((len_hbm, len_s), (gate_hbm, gate_s), (beta_hbm, beta_s), (gain_hbm, gain_s))
        )
    ]
    for copy in smalls:
        copy.start()
    k_rows = k_hbm.reshape(subs, heads * width)
    v_rows = v_hbm.reshape(subs, heads * width)

    def loads(h):
        lanes = pl.ds(pl.multiple_of(h * width, width), width)
        return (
            pltpu.make_async_copy(k_rows.at[:, lanes], k_s.at[h], in_sem.at[0, h]),
            pltpu.make_async_copy(v_rows.at[:, lanes], v_s.at[h], in_sem.at[1, h]),
            pltpu.make_async_copy(q_hbm.at[:, lanes], q_s.at[h], in_sem.at[2, h]),
        )

    for h in range(heads):
        for copy in loads(h)[:2]:
            copy.start()
    for h in range(heads):
        loads(h)[2].start()
    w_copy = pltpu.make_async_copy(w_hbm, w_s, w_sem)
    w_copy.start()

    barrier = pltpu.get_barrier_semaphore()
    for side in (right, left):
        pl.semaphore_signal(barrier, inc=1, device_id={"head": side}, device_id_type=MESH)

    @pl.when(has_before)
    def _():
        pl.semaphore_signal(barrier, inc=1, device_id={"seq": z - 1}, device_id_type=MESH)

    eye_s[...] = (iota((n, n), 0) == iota((n, n), 1)).astype(f32)
    for level in range(levels_of(n)):
        lev_s[level] = level_mask(n, level)
    for copy in smalls:
        copy.wait()
    offset = z * tokens
    ends, run = [], 0
    for i in range(len_s.shape[0]):
        run = run + len_s[i]
        ends.append(run)
    rows, toks = vectors(gate_s[...], [beta_s[j] for j in range(2)])
    for b in range(blocks):
        cols = jnp.transpose(rows[b])
        t_cols = jnp.transpose(toks[b])
        for h in range(heads):
            row_s[h, b] = rows[b][h : h + 1]
            row_s[heads + h, b] = rows[b][heads + h : heads + h + 1]
            col_s[h, b] = cols[:, h : h + 1]
            tok_s[h, b] = t_cols[:BLOCK, h : h + 1]
        pair_s[b], read_s[b], crow_s[b], ctok_s[b], erow_s[b] = block_masks(offset, ends, b)

    @pl.when(jnp.logical_not(has_before))
    def _():
        recv_s[...] = jnp.zeros_like(recv_s)

    def hop(r, h):
        return pltpu.make_async_remote_copy(
            src_ref=send_s.at[r, h],
            dst_ref=recv_s.at[r, h],
            send_sem=ring_send.at[r, h],
            recv_sem=ring_recv.at[r, h],
            device_id={"seq": jnp.minimum(z + 1, n_seq - 1)},
            device_id_type=MESH,
        )

    def leave(r, h, state):
        send_s[r, h] = state.astype(bf16)

        @pl.when(has_after)
        def _():
            hop(r, h).start()

    def arrive(r, h):
        @pl.when(has_before)
        def _():
            hop(r, h).wait_recv()

        return recv_s[r, h]

    def masks_of(b):
        return pair_s[b], read_s[b], crow_s[b], ctok_s[b], erow_s[b]

    def two_heads(pair, carry):
        hs = [2 * pair, 2 * pair + 1]
        units, masks = [], []
        for h in hs:
            for copy in loads(h)[:2]:
                copy.wait()
        for h in hs:
            for b in range(blocks):
                at = pl.ds(b * n, n)
                units.append(
                    (
                        k_s[h, at, :],
                        v_s[h, at, :],
                        row_s[h, b],
                        col_s[h, b],
                        row_s[heads + h, b],
                    )
                )
                masks.append(masks_of(b))
        outs = state_maps(units, masks, eye_s[...], lambda l: lev_s[l])

        totals = [
            compose([m[:2] for m in outs[i * blocks : (i + 1) * blocks]]) for i in range(len(hs))
        ]

        @pl.when(pair == 0)
        def _():
            pl.semaphore_wait(barrier, 2 + has_after.astype(jnp.int32))

        for h, total in zip(hs, totals):
            leave(0, h, total[-1][:, width:])
        for i, h in enumerate(hs):
            for b in range(blocks):
                write_s[h, b] = outs[i * blocks + b][2]
                norm_s[h, b] = outs[i * blocks + b][3]
            for b in range(1, blocks):
                before_s[h, b - 1] = totals[i][b - 1].astype(bf16)
            map_s[h] = jnp.concatenate(split(totals[i][-1][:, :width]), axis=1)
            add_s[h] = totals[i][-1][:, width:]
        return carry

    lax.fori_loop(0, heads // 2, two_heads, 0)

    def step(r):
        for h in range(heads):
            got = arrive(r - 1, h)
            leave(r, h, add_s[h] + mm(map_s[h], jnp.concatenate([got, got], axis=0)))

    def reads_and_step(h, carry):
        loads(h)[2].wait()
        for b in range(blocks):
            at = pl.ds(b * BLOCK, BLOCK)
            g_s[h, at, :], o_s[h, at, :] = block_reads(
                q_s[h, at, :],
                k_s[h, pl.ds(b * n, n), :],
                write_s[h, b],
                norm_s[h, b],
                row_s[h, b],
                tok_s[h, b],
                masks_of(b),
                before_s[h, b - 1] if b else None,
            )

        step(h + 1)
        return carry

    def just_step(r, carry):
        step(r)
        return carry

    lax.fori_loop(0, heads, reads_and_step, 0)
    lax.fori_loop(heads + 1, rounds, just_step, 0)

    for h in range(heads):
        got = arrive(rounds - 1, h)
        out = o_s[h] + mm(g_s[h], got)
        mean = jnp.sum(out * out, axis=1, keepdims=True) * (1.0 / width)
        flat_s[:, h * width : (h + 1) * width] = (
            out * lax.rsqrt(mean + EPS) * gain_s[...]
        ).astype(bf16)

    chunks, _, chunk = part_s.shape
    share = out_ref.shape[0]
    lower = chunks // 2
    far = lax.rem(x + 2, n_head)

    def rows_for(dest):
        return pl.ds(pl.multiple_of(dest * share, share), share)

    def relay(c):
        return pltpu.make_async_remote_copy(
            src_ref=part_s.at[c, rows_for(far), :],
            dst_ref=relay_s.at[c],
            send_sem=relay_send.at[c],
            recv_sem=relay_recv.at[c],
            device_id={"head": right if c < lower else left},
            device_id_type=MESH,
        )

    def direct(c):
        to = left if c < lower else right
        return pltpu.make_async_remote_copy(
            src_ref=part_s.at[c, rows_for(to), :],
            dst_ref=got_s.at[0, c],
            send_sem=x_send.at[0, c],
            recv_sem=x_recv.at[0, c],
            device_id={"head": to},
            device_id_type=MESH,
        )

    def summed(c):
        to = right if c < lower else left
        return pltpu.make_async_remote_copy(
            src_ref=sum_s.at[c],
            dst_ref=got_s.at[1, c],
            send_sem=x_send.at[1, c],
            recv_sem=x_recv.at[1, c],
            device_id={"head": to},
            device_id_type=MESH,
        )

    order = [c for pair in zip(range(lower), range(lower, chunks)) for c in pair]
    w_copy.wait()
    flat = flat_s[...]
    for c in order:
        part_s[c] = mm(flat, w_s[:, c * chunk : (c + 1) * chunk]).astype(bf16)
        relay(c).start()
    for c in order:
        direct(c).start()
    for c in order:
        relay(c).wait_recv()
        to = right if c < lower else left
        sum_s[c] = (part_s[c, rows_for(to), :].astype(f32) + relay_s[c].astype(f32)).astype(bf16)
        summed(c).start()
    for c in order:
        direct(c).wait_recv()
        total = part_s[c, rows_for(x), :].astype(f32) + got_s[0, c].astype(f32)
        summed(c).wait_recv()
        out_ref[:, c * chunk : (c + 1) * chunk] = (total + got_s[1, c].astype(f32)).astype(bf16)

    @pl.when(has_after)
    def _():
        def drain(r, carry):
            for h in range(heads):
                hop(r, h).wait_send()
            return carry

        lax.fori_loop(0, rounds, drain, 0)

    for c in order:
        relay(c).wait_send()
        direct(c).wait_send()
        summed(c).wait_send()


def solution(mesh):
    n_seq, n_head = mesh.shape["seq"], mesh.shape["head"]

    def body(queries, keys, values, beta, gate, lengths, gain, weight):
        tokens, lanes = queries.shape[1:]
        refl, heads = beta.shape[2:]
        width = lanes // heads
        subs = tokens * refl
        blocks = tokens // BLOCK
        n = refl * BLOCK
        model = weight.shape[1]
        share = tokens // n_head
        rounds = min(n_seq - 1, -(-LONGEST // tokens))
        chunks = 4
        chunk = model // chunks
        hbm = pl.BlockSpec(memory_space=pltpu.HBM)
        vmem = pl.BlockSpec(memory_space=pltpu.VMEM)
        dma = pltpu.SemaphoreType.DMA
        out = pl.pallas_call(
            functools.partial(kernel, n_seq, n_head, rounds),
            out_shape=jax.ShapeDtypeStruct((share, model), bf16),
            in_specs=[hbm] * 8,
            out_specs=vmem,
            scratch_shapes=[
                pltpu.VMEM((heads, tokens, width), bf16),
                pltpu.VMEM((heads, subs, width), bf16),
                pltpu.VMEM((heads, subs, width), bf16),
                pltpu.VMEM((lanes, model), bf16),
                pltpu.VMEM((refl, heads, tokens), f32),
                pltpu.VMEM((heads, tokens), f32),
                pltpu.SMEM((lengths.shape[1],), jnp.int32),
                pltpu.VMEM((1, width), f32),
                pltpu.VMEM((2 * heads, blocks, 1, n), f32),
                pltpu.VMEM((heads, blocks, n, 1), f32),
                pltpu.VMEM((heads, blocks, BLOCK, 1), f32),
                pltpu.VMEM((blocks, n, n), f32),
                pltpu.VMEM((blocks, BLOCK, n), f32),
                pltpu.VMEM((blocks, 1, n), f32),
                pltpu.VMEM((blocks, BLOCK, 1), f32),
                pltpu.VMEM((blocks, 1, n), f32),
                pltpu.VMEM((n, n), f32),
                pltpu.VMEM((levels_of(n), n, n), bf16),
                pltpu.VMEM((heads, blocks, n, 2 * width), bf16),
                pltpu.VMEM((heads, blocks, 1, n), f32),
                pltpu.VMEM((heads, blocks - 1, width, 2 * width), bf16),
                pltpu.VMEM((heads, width, 2 * width), bf16),
                pltpu.VMEM((heads, width, width), f32),
                pltpu.VMEM((heads, tokens, width), bf16),
                pltpu.VMEM((heads, tokens, width), f32),
                pltpu.VMEM((rounds, heads, width, width), bf16),
                pltpu.VMEM((rounds, heads, width, width), bf16),
                pltpu.VMEM((tokens, lanes), bf16),
                pltpu.VMEM((chunks, tokens, chunk), bf16),
                pltpu.VMEM((chunks, share, chunk), bf16),
                pltpu.VMEM((chunks, share, chunk), bf16),
                pltpu.VMEM((2, chunks, share, chunk), bf16),
                dma((3, heads)),
                dma((4,)),
                dma,
                dma((rounds, heads)),
                dma((rounds, heads)),
                dma((chunks,)),
                dma((chunks,)),
                dma((2, chunks)),
                dma((2, chunks)),
            ],
            compiler_params=pltpu.CompilerParams(
                collective_id=0, has_side_effects=True, vmem_limit_bytes=67043328
            ),
        )(
            queries[0],
            keys[0],
            values[0],
            jnp.transpose(beta[0], (1, 2, 0)),
            jnp.transpose(gate[0], (1, 0)),
            lengths[0],
            gain[None, :],
            weight,
        )
        return out[None]

    packs = ("parts", "rep")
    in_specs = (
        P(packs, "seq", "head"),
        P(packs, "seq", None, "head"),
        P(packs, "seq", None, "head"),
        P(packs, "seq", None, "head"),
        P(packs, "seq", "head"),
        P(packs, None),
        P(),
        P("head", None),
    )
    out_specs = P(packs, ("seq", "head"), None)
    return jax.shard_map(body, mesh=mesh, in_specs=in_specs, out_specs=out_specs, check_vma=False)
```

```python
import functools

import jax
import jax.numpy as jnp
from jax import lax
from jax.experimental import pallas as pl
from jax.experimental.pallas import tpu as pltpu
from jax.sharding import PartitionSpec as P

BLOCK = 64
LONGEST = 2048
EPS = 1e-06
FAR = -1e30
MESH = pl.DeviceIdType.MESH
f32 = jnp.float32
bf16 = jnp.bfloat16


def mm(a, b):
    return lax.dot_general(a, b, (((1,), (0,)), ((), ())), preferred_element_type=f32)


def mm_t(a, b):
    return lax.dot_general(a, b, (((1,), (1,)), ((), ())), preferred_element_type=f32)


def split(x):
    hi = x.astype(bf16)
    return hi, (x - hi.astype(f32)).astype(bf16)


def iota(shape, dim):
    return lax.broadcasted_iota(jnp.int32, shape, dim)


def split3(x):
    first = x.astype(bf16)
    rest = x - first.astype(f32)
    second = rest.astype(bf16)
    return first, second, (rest - second.astype(f32)).astype(bf16)


def seg_of(pos, ends):
    total = jnp.zeros_like(pos)
    for end in ends:
        total = total + (pos >= end).astype(jnp.int32)
    return total


def vectors(gate, beta):
    heads, tokens = gate.shape
    n = 2 * BLOCK
    blocks = tokens // BLOCK
    left = []
    for b in range(blocks):
        at = slice(b * BLOCK, (b + 1) * BLOCK)
        part = gate[:, at]
        left.append(jnp.concatenate([part, jnp.zeros_like(part)], axis=1))
        left.append(jnp.concatenate([beta[0][:, at], beta[1][:, at]], axis=1))
    left = jnp.concatenate(left, axis=0)
    count = left.shape[0]
    k, r = iota((n, n), 0), iota((n, n), 1)
    upto = ((k < BLOCK) & (k <= r // 2)).astype(f32)
    place = (r == 2 * (k % BLOCK) + k // BLOCK).astype(f32)
    token = ((k < BLOCK) & (k <= r)).astype(f32)
    table = jnp.concatenate([upto, place, token], axis=1).astype(bf16)
    got = mm(jnp.concatenate(split3(left), axis=0), table)
    got = got[:count] + got[count : 2 * count] + got[2 * count :]
    both = 2 * heads
    first = iota((both, n), 0) < heads
    rows, toks = [], []
    for b in range(blocks):
        mine = got[b * both : (b + 1) * both]
        rows.append(jnp.where(first, mine[:, :n], mine[:, n : 2 * n]))
        toks.append(mine[:, 2 * n :])
    return rows, toks


def block_masks(offset, ends, block):
    n = 2 * BLOCK
    start = offset + block * BLOCK
    before = sum((start - 1 >= e).astype(jnp.int32) for e in ends)
    before = jnp.where(start == 0, -1, before)
    last = sum((start + BLOCK - 1 >= e).astype(jnp.int32) for e in ends)
    seg_row = seg_of(start + iota((1, n), 1) // 2, ends)
    seg_col = seg_of(start + iota((n, 1), 0) // 2, ends)
    seg_tok = seg_of(start + iota((BLOCK, 1), 0), ends)
    i, j = iota((n, n), 0), iota((n, n), 1)
    pair = jnp.where((i >= j) & (seg_col == seg_row), 0.0, FAR)
    ti, tj = iota((BLOCK, n), 0), iota((BLOCK, n), 1)
    read = jnp.where((ti >= tj // 2) & (seg_tok == seg_row), 0.0, FAR)
    carry_row = jnp.where(seg_row == before, 0.0, FAR)
    carry_tok = jnp.where(seg_tok == before, 0.0, FAR)
    end_row = jnp.where(seg_row == last, 0.0, FAR)
    return pair, read, carry_row, carry_tok, end_row


def level_mask(n, level):
    i, j = iota((n, n), 0), iota((n, n), 1)
    return ((i > j) & (lax.shift_right_logical(i ^ j, level) == 1)).astype(f32).astype(bf16)


def levels_of(n):
    return n.bit_length() - 1


def as_cols(rows):
    cols = jnp.transpose(jnp.concatenate(rows, axis=0))
    return [cols[:, u : u + 1] for u in range(len(rows))]


def state_maps(units, masks, eye, levels):
    n = eye.shape[0]
    width = units[0][0].shape[1]
    eye16 = eye.astype(bf16)
    grams = [mm_t(k, k) for k, *_ in units]
    norms = [
        lax.rsqrt(jnp.sum(gram * eye, axis=0, keepdims=True) + EPS) for gram in grams
    ]
    beta_cols = as_cols([norm * unit[4] for norm, unit in zip(norms, units)])
    end_cols = as_cols(
        [
            jnp.exp((unit[2][:, n - 1 :] - unit[2]) + mask[4]) * norm
            for norm, unit, mask in zip(norms, units, masks)
        ]
    )
    lowers = []
    for gram, norm, beta_col, (k, v, c_row, c_col, b_row), mask in zip(
        grams, norms, beta_cols, units, masks
    ):
        ratio = jnp.exp((c_col - c_row) + mask[0])
        lower = (beta_col * ratio) * (norm * gram)
        lowers.append(split(lower - lower * eye))
    xs = [eye16 - low[0] * levels(0) for low in lowers]
    for level in range(1, levels_of(n)):
        mask = levels(level)
        ys = [mm(low[0] * mask, x).astype(bf16) for low, x in zip(lowers, xs)]
        xs = [x - mm(x, y).astype(bf16) for x, y in zip(xs, ys)]
    lefts = [
        mm(jnp.concatenate(low, axis=1), jnp.concatenate([x, x], axis=0))
        for low, x in zip(lowers, xs)
    ]
    rests = [((eye - x.astype(f32)) - left).astype(bf16) for x, left in zip(xs, lefts)]
    invs = [x.astype(f32) + mm(x, rest) for x, rest in zip(xs, rests)]
    writes = []
    for inv, norm, (k, v, c_row, c_col, b_row), mask in zip(invs, norms, units, masks):
        for_value = inv * b_row
        for_key = inv * (b_row * jnp.exp(c_row + mask[2]) * norm)
        wv = mm(jnp.concatenate(split(for_value), axis=1), jnp.concatenate([v, v], axis=0))
        wk = mm(jnp.concatenate(split(for_key), axis=1), jnp.concatenate([k, k], axis=0))
        writes.append(jnp.concatenate([wv, wk], axis=1))
    outs = []
    for write, end, norm, (k, v, c_row, c_col, b_row), mask in zip(
        writes, end_cols, norms, units, masks
    ):
        hi, lo = split(write * end)
        kt = jnp.transpose(k)
        ew = mm(jnp.concatenate([kt, kt], axis=1), jnp.concatenate([hi, lo], axis=0))
        carry_last = jnp.exp(c_row[:, n - 1 :] + mask[2][:, n - 1 :])
        outs.append((carry_last * eye - ew[:, width:], ew[:, :width], write.astype(bf16), norm))
    return outs


def compose(maps):
    width = maps[0][0].shape[1]
    totals = [jnp.concatenate(maps[0], axis=1)]
    for map_b, add_b in maps[1:]:
        hi, lo = split(totals[-1])
        m_hi, m_lo = split(map_b)
        total = mm(jnp.concatenate([m_hi, m_lo], axis=1), jnp.concatenate([hi, hi], axis=0))
        total = total + mm(m_hi, lo)
        totals.append(jnp.concatenate([total[:, :width], total[:, width:] + add_b], axis=1))
    return totals


def block_reads(q, k, write, norm, c_row, ct_col, mask, before):
    width = q.shape[1]
    qf = q.astype(f32)
    nq = lax.rsqrt(jnp.sum(qf * qf, axis=1, keepdims=True) + EPS) * width**-0.5
    weights = (jnp.exp((ct_col - c_row) + mask[1]) * nq) * (norm * mm_t(q, k))
    got = mm(weights.astype(bf16), write)
    reads = (jnp.exp(ct_col + mask[3]) * nq) * qf - got[:, width:]
    if before is None:
        return reads.astype(bf16), got[:, :width]
    wide = mm(reads.astype(bf16), before)
    return wide[:, :width].astype(bf16), got[:, :width] + wide[:, width:]


def kernel(
    n_seq,
    n_head,
    rounds,
    q_hbm,
    k_hbm,
    v_hbm,
    beta_hbm,
    gate_hbm,
    len_hbm,
    gain_hbm,
    w_hbm,
    out_ref,
    q_s,
    k_s,
    v_s,
    w_s,
    beta_s,
    gate_s,
    len_s,
    gain_s,
    row_s,
    col_s,
    tok_s,
    pair_s,
    read_s,
    crow_s,
    ctok_s,
    erow_s,
    eye_s,
    lev_s,
    write_s,
    norm_s,
    before_s,
    map_s,
    add_s,
    g_s,
    o_s,
    send_s,
    recv_s,
    flat_s,
    part_s,
    relay_s,
    sum_s,
    got_s,
    in_sem,
    small_sem,
    w_sem,
    ring_send,
    ring_recv,
    relay_send,
    relay_recv,
    x_send,
    x_recv,
):
    z = lax.axis_index("seq")
    x = lax.axis_index("head")
    heads, subs, width = k_s.shape
    tokens = q_s.shape[1]
    blocks = tokens // BLOCK
    n = 2 * BLOCK
    right, left = lax.rem(x + 1, n_head), lax.rem(x + n_head - 1, n_head)
    has_before, has_after = z > 0, z < n_seq - 1
    rounds_in = jnp.minimum(rounds, z)
    rounds_out = jnp.where(has_after, jnp.minimum(rounds, z + 1), 0)

    smalls = [
        pltpu.make_async_copy(src, dst, small_sem.at[i])
        for i, (src, dst) in enumerate(
            ((len_hbm, len_s), (gate_hbm, gate_s), (beta_hbm, beta_s), (gain_hbm, gain_s))
        )
    ]
    for copy in smalls:
        copy.start()
    k_rows = k_hbm.reshape(subs, heads * width)
    v_rows = v_hbm.reshape(subs, heads * width)

    def loads(h):
        lanes = pl.ds(pl.multiple_of(h * width, width), width)
        return (
            pltpu.make_async_copy(k_rows.at[:, lanes], k_s.at[h], in_sem.at[0, h]),
            pltpu.make_async_copy(v_rows.at[:, lanes], v_s.at[h], in_sem.at[1, h]),
            pltpu.make_async_copy(q_hbm.at[:, lanes], q_s.at[h], in_sem.at[2, h]),
        )

    for h in range(heads):
        for copy in loads(h)[:2]:
            copy.start()
    for h in range(heads):
        loads(h)[2].start()
    w_copy = pltpu.make_async_copy(w_hbm, w_s, w_sem)
    w_copy.start()

    barrier = pltpu.get_barrier_semaphore()
    for side in (right, left):
        pl.semaphore_signal(barrier, inc=1, device_id={"head": side}, device_id_type=MESH)

    @pl.when(has_before)
    def _():
        pl.semaphore_signal(barrier, inc=1, device_id={"seq": z - 1}, device_id_type=MESH)

    eye_s[...] = (iota((n, n), 0) == iota((n, n), 1)).astype(f32)
    for level in range(levels_of(n)):
        lev_s[level] = level_mask(n, level)
    for copy in smalls:
        copy.wait()
    offset = z * tokens
    ends, run = [], 0
    for i in range(len_s.shape[0]):
        run = run + len_s[i]
        ends.append(run)
    rows, toks = vectors(gate_s[...], [beta_s[j] for j in range(2)])
    for b in range(blocks):
        cols = jnp.transpose(rows[b])
        t_cols = jnp.transpose(toks[b])
        for h in range(heads):
            row_s[h, b] = rows[b][h : h + 1]
            row_s[heads + h, b] = rows[b][heads + h : heads + h + 1]
            col_s[h, b] = cols[:, h : h + 1]
            tok_s[h, b] = t_cols[:BLOCK, h : h + 1]
        pair_s[b], read_s[b], crow_s[b], ctok_s[b], erow_s[b] = block_masks(offset, ends, b)

    @pl.when(jnp.logical_not(has_before))
    def _():
        recv_s[0] = jnp.zeros_like(recv_s[0])

    def hop(r, h):
        return pltpu.make_async_remote_copy(
            src_ref=send_s.at[r, h],
            dst_ref=recv_s.at[r, h],
            send_sem=ring_send.at[r, h],
            recv_sem=ring_recv.at[r, h],
            device_id={"seq": jnp.minimum(z + 1, n_seq - 1)},
            device_id_type=MESH,
        )

    def masks_of(b):
        return pair_s[b], read_s[b], crow_s[b], ctok_s[b], erow_s[b]

    def two_heads(pair, carry):
        hs = [2 * pair, 2 * pair + 1]
        units, masks = [], []
        for h in hs:
            for copy in loads(h)[:2]:
                copy.wait()
        for h in hs:
            for b in range(blocks):
                at = pl.ds(b * n, n)
                units.append(
                    (
                        k_s[h, at, :],
                        v_s[h, at, :],
                        row_s[h, b],
                        col_s[h, b],
                        row_s[heads + h, b],
                    )
                )
                masks.append(masks_of(b))
        outs = state_maps(units, masks, eye_s[...], lambda l: lev_s[l])

        totals = [
            compose([m[:2] for m in outs[i * blocks : (i + 1) * blocks]]) for i in range(len(hs))
        ]

        @pl.when(pair == 0)
        def _():
            pl.semaphore_wait(barrier, 2 + has_after.astype(jnp.int32))

        for h, total in zip(hs, totals):
            send_s[0, h] = total[-1][:, width:].astype(bf16)

        @pl.when(has_after)
        def _():
            for h in hs:
                hop(0, h).start()

        for i, h in enumerate(hs):
            for b in range(blocks):
                write_s[h, b] = outs[i * blocks + b][2]
                norm_s[h, b] = outs[i * blocks + b][3]
            for b in range(1, blocks):
                before_s[h, b - 1] = totals[i][b - 1].astype(bf16)
            map_s[h] = jnp.concatenate(split(totals[i][-1][:, :width]), axis=1)
            add_s[h] = totals[i][-1][:, width:]
        return carry

    lax.fori_loop(0, heads // 2, two_heads, 0)

    def step(r):
        for h in range(heads):
            hop(r - 1, h).wait_recv()
            got = recv_s[r - 1, h]
            state = add_s[h] + mm(map_s[h], jnp.concatenate([got, got], axis=0))
            send_s[r, h] = state.astype(bf16)
            hop(r, h).start()

    def reads_and_step(h, carry):
        loads(h)[2].wait()
        for b in range(blocks):
            at = pl.ds(b * BLOCK, BLOCK)
            g_s[h, at, :], o_s[h, at, :] = block_reads(
                q_s[h, at, :],
                k_s[h, pl.ds(b * n, n), :],
                write_s[h, b],
                norm_s[h, b],
                row_s[h, b],
                tok_s[h, b],
                masks_of(b),
                before_s[h, b - 1] if b else None,
            )

        @pl.when(h + 1 < rounds_out)
        def _():
            step(h + 1)

        return carry

    def just_step(r, carry):
        step(r)
        return carry

    lax.fori_loop(0, heads, reads_and_step, 0)
    lax.fori_loop(heads + 1, rounds_out, just_step, 0)

    @pl.when(jnp.logical_not(has_after))
    def _():
        def skip(r, carry):
            for h in range(heads):
                hop(r, h).wait_recv()
            return carry

        lax.fori_loop(0, rounds_in - 1, skip, 0)

    last = jnp.maximum(rounds_in - 1, 0)
    for h in range(heads):

        @pl.when(rounds_in >= jnp.maximum(rounds_out, 1))
        def _():
            hop(last, h).wait_recv()

        got = recv_s[last, h]
        out = o_s[h] + mm(g_s[h], got)
        mean = jnp.sum(out * out, axis=1, keepdims=True) * (1.0 / width)
        flat_s[:, h * width : (h + 1) * width] = (
            out * lax.rsqrt(mean + EPS) * gain_s[...]
        ).astype(bf16)

    chunks, _, chunk = part_s.shape
    share = out_ref.shape[0]
    lower = chunks // 2
    far = lax.rem(x + 2, n_head)

    def rows_for(dest):
        return pl.ds(pl.multiple_of(dest * share, share), share)

    def relay(c):
        return pltpu.make_async_remote_copy(
            src_ref=part_s.at[c, rows_for(far), :],
            dst_ref=relay_s.at[c],
            send_sem=relay_send.at[c],
            recv_sem=relay_recv.at[c],
            device_id={"head": right if c < lower else left},
            device_id_type=MESH,
        )

    def direct(c):
        to = left if c < lower else right
        return pltpu.make_async_remote_copy(
            src_ref=part_s.at[c, rows_for(to), :],
            dst_ref=got_s.at[0, c],
            send_sem=x_send.at[0, c],
            recv_sem=x_recv.at[0, c],
            device_id={"head": to},
            device_id_type=MESH,
        )

    def summed(c):
        to = right if c < lower else left
        return pltpu.make_async_remote_copy(
            src_ref=sum_s.at[c],
            dst_ref=got_s.at[1, c],
            send_sem=x_send.at[1, c],
            recv_sem=x_recv.at[1, c],
            device_id={"head": to},
            device_id_type=MESH,
        )

    order = [c for pair in zip(range(lower), range(lower, chunks)) for c in pair]
    w_copy.wait()
    flat = flat_s[...]
    for c in order:
        part_s[c] = mm(flat, w_s[:, c * chunk : (c + 1) * chunk]).astype(bf16)
        relay(c).start()
    for c in order:
        direct(c).start()
    for c in order:
        relay(c).wait_recv()
        to = right if c < lower else left
        sum_s[c] = (part_s[c, rows_for(to), :].astype(f32) + relay_s[c].astype(f32)).astype(bf16)
        summed(c).start()
    for c in order:
        direct(c).wait_recv()
        total = part_s[c, rows_for(x), :].astype(f32) + got_s[0, c].astype(f32)
        summed(c).wait_recv()
        out_ref[:, c * chunk : (c + 1) * chunk] = (total + got_s[1, c].astype(f32)).astype(bf16)

    def drain(r, carry):
        for h in range(heads):
            hop(r, h).wait_send()
        return carry

    lax.fori_loop(0, rounds_out, drain, 0)
    for c in order:
        relay(c).wait_send()
        direct(c).wait_send()
        summed(c).wait_send()


def solution(mesh):
    n_seq, n_head = mesh.shape["seq"], mesh.shape["head"]

    def body(queries, keys, values, beta, gate, lengths, gain, weight):
        tokens, lanes = queries.shape[1:]
        refl, heads = beta.shape[2:]
        width = lanes // heads
        subs = tokens * refl
        blocks = tokens // BLOCK
        n = refl * BLOCK
        model = weight.shape[1]
        share = tokens // n_head
        rounds = min(n_seq - 1, -(-LONGEST // tokens))
        chunks = 4
        chunk = model // chunks
        hbm = pl.BlockSpec(memory_space=pltpu.HBM)
        vmem = pl.BlockSpec(memory_space=pltpu.VMEM)
        dma = pltpu.SemaphoreType.DMA
        out = pl.pallas_call(
            functools.partial(kernel, n_seq, n_head, rounds),
            out_shape=jax.ShapeDtypeStruct((share, model), bf16),
            in_specs=[hbm] * 8,
            out_specs=vmem,
            scratch_shapes=[
                pltpu.VMEM((heads, tokens, width), bf16),
                pltpu.VMEM((heads, subs, width), bf16),
                pltpu.VMEM((heads, subs, width), bf16),
                pltpu.VMEM((lanes, model), bf16),
                pltpu.VMEM((refl, heads, tokens), f32),
                pltpu.VMEM((heads, tokens), f32),
                pltpu.SMEM((lengths.shape[1],), jnp.int32),
                pltpu.VMEM((1, width), f32),
                pltpu.VMEM((2 * heads, blocks, 1, n), f32),
                pltpu.VMEM((heads, blocks, n, 1), f32),
                pltpu.VMEM((heads, blocks, BLOCK, 1), f32),
                pltpu.VMEM((blocks, n, n), f32),
                pltpu.VMEM((blocks, BLOCK, n), f32),
                pltpu.VMEM((blocks, 1, n), f32),
                pltpu.VMEM((blocks, BLOCK, 1), f32),
                pltpu.VMEM((blocks, 1, n), f32),
                pltpu.VMEM((n, n), f32),
                pltpu.VMEM((levels_of(n), n, n), bf16),
                pltpu.VMEM((heads, blocks, n, 2 * width), bf16),
                pltpu.VMEM((heads, blocks, 1, n), f32),
                pltpu.VMEM((heads, blocks - 1, width, 2 * width), bf16),
                pltpu.VMEM((heads, width, 2 * width), bf16),
                pltpu.VMEM((heads, width, width), f32),
                pltpu.VMEM((heads, tokens, width), bf16),
                pltpu.VMEM((heads, tokens, width), f32),
                pltpu.VMEM((rounds, heads, width, width), bf16),
                pltpu.VMEM((rounds, heads, width, width), bf16),
                pltpu.VMEM((tokens, lanes), bf16),
                pltpu.VMEM((chunks, tokens, chunk), bf16),
                pltpu.VMEM((chunks, share, chunk), bf16),
                pltpu.VMEM((chunks, share, chunk), bf16),
                pltpu.VMEM((2, chunks, share, chunk), bf16),
                dma((3, heads)),
                dma((4,)),
                dma,
                dma((rounds, heads)),
                dma((rounds, heads)),
                dma((chunks,)),
                dma((chunks,)),
                dma((2, chunks)),
                dma((2, chunks)),
            ],
            compiler_params=pltpu.CompilerParams(
                collective_id=0, has_side_effects=True, vmem_limit_bytes=40 * 1024 * 1024
            ),
        )(
            *[
                pltpu.with_memory_space_constraint(a, pltpu.HBM)
                for a in (
            queries[0],
            keys[0],
            values[0],
            jnp.transpose(beta[0], (1, 2, 0)),
            jnp.transpose(gate[0], (1, 0)),
            lengths[0],
            gain[None, :],
            weight,
                )
            ]
        )
        return out[None]

    packs = ("parts", "rep")
    in_specs = (
        P(packs, "seq", "head"),
        P(packs, "seq", None, "head"),
        P(packs, "seq", None, "head"),
        P(packs, "seq", None, "head"),
        P(packs, "seq", "head"),
        P(packs, None),
        P(),
        P("head", None),
    )
    out_specs = P(packs, ("seq", "head"), None)
    return jax.shard_map(body, mesh=mesh, in_specs=in_specs, out_specs=out_specs, check_vma=False)
```

```python
import functools

import jax
import jax.numpy as jnp
from jax import lax
from jax.experimental import pallas as pl
from jax.experimental.pallas import tpu as pltpu
from jax.sharding import PartitionSpec as P

BLOCK = 64
LONGEST = 2048
EPS = 1e-06
FAR = -1e30
MESH = pl.DeviceIdType.MESH
f32 = jnp.float32
bf16 = jnp.bfloat16


def mm(a, b):
    return lax.dot_general(a, b, (((1,), (0,)), ((), ())), preferred_element_type=f32)


def mm_t(a, b):
    return lax.dot_general(a, b, (((1,), (1,)), ((), ())), preferred_element_type=f32)


def split(x):
    hi = x.astype(bf16)
    return hi, (x - hi.astype(f32)).astype(bf16)


def iota(shape, dim):
    return lax.broadcasted_iota(jnp.int32, shape, dim)


def split3(x):
    first = x.astype(bf16)
    rest = x - first.astype(f32)
    second = rest.astype(bf16)
    return first, second, (rest - second.astype(f32)).astype(bf16)


def seg_of(pos, ends):
    total = jnp.zeros_like(pos)
    for end in ends:
        total = total + (pos >= end).astype(jnp.int32)
    return total


def vectors(gate, beta):
    heads, tokens = gate.shape
    n = 2 * BLOCK
    blocks = tokens // BLOCK
    left = []
    for b in range(blocks):
        at = slice(b * BLOCK, (b + 1) * BLOCK)
        part = gate[:, at]
        left.append(jnp.concatenate([part, jnp.zeros_like(part)], axis=1))
        left.append(jnp.concatenate([beta[0][:, at], beta[1][:, at]], axis=1))
    left = jnp.concatenate(left, axis=0)
    count = left.shape[0]
    k, r = iota((n, n), 0), iota((n, n), 1)
    upto = ((k < BLOCK) & (k <= r // 2)).astype(f32)
    place = (r == 2 * (k % BLOCK) + k // BLOCK).astype(f32)
    token = ((k < BLOCK) & (k <= r)).astype(f32)
    table = jnp.concatenate([upto, place, token], axis=1).astype(bf16)
    got = mm(jnp.concatenate(split3(left), axis=0), table)
    got = got[:count] + got[count : 2 * count] + got[2 * count :]
    both = 2 * heads
    first = iota((both, n), 0) < heads
    rows, toks = [], []
    for b in range(blocks):
        mine = got[b * both : (b + 1) * both]
        rows.append(jnp.where(first, mine[:, :n], mine[:, n : 2 * n]))
        toks.append(mine[:, 2 * n :])
    return rows, toks


def block_masks(offset, ends, block):
    n = 2 * BLOCK
    start = offset + block * BLOCK
    before = sum((start - 1 >= e).astype(jnp.int32) for e in ends)
    before = jnp.where(start == 0, -1, before)
    last = sum((start + BLOCK - 1 >= e).astype(jnp.int32) for e in ends)
    seg_row = seg_of(start + iota((1, n), 1) // 2, ends)
    seg_col = seg_of(start + iota((n, 1), 0) // 2, ends)
    seg_tok = seg_of(start + iota((BLOCK, 1), 0), ends)
    i, j = iota((n, n), 0), iota((n, n), 1)
    pair = jnp.where((i >= j) & (seg_col == seg_row), 0.0, FAR)
    ti, tj = iota((BLOCK, n), 0), iota((BLOCK, n), 1)
    read = jnp.where((ti >= tj // 2) & (seg_tok == seg_row), 0.0, FAR)
    carry_row = jnp.where(seg_row == before, 0.0, FAR)
    carry_tok = jnp.where(seg_tok == before, 0.0, FAR)
    end_row = jnp.where(seg_row == last, 0.0, FAR)
    return pair, read, carry_row, carry_tok, end_row


def level_mask(n, level):
    i, j = iota((n, n), 0), iota((n, n), 1)
    return ((i > j) & (lax.shift_right_logical(i ^ j, level) == 1)).astype(f32).astype(bf16)


def levels_of(n):
    return n.bit_length() - 1


def as_cols(rows):
    cols = jnp.transpose(jnp.concatenate(rows, axis=0))
    return [cols[:, u : u + 1] for u in range(len(rows))]


def state_maps(units, masks, eye, levels):
    n = eye.shape[0]
    width = units[0][0].shape[1]
    eye16 = eye.astype(bf16)
    grams = [mm_t(k, k) for k, *_ in units]
    norms = [
        lax.rsqrt(jnp.sum(gram * eye, axis=0, keepdims=True) + EPS) for gram in grams
    ]
    beta_cols = as_cols([norm * unit[4] for norm, unit in zip(norms, units)])
    end_cols = as_cols(
        [
            jnp.exp((unit[2][:, n - 1 :] - unit[2]) + mask[4]) * norm
            for norm, unit, mask in zip(norms, units, masks)
        ]
    )
    lowers = []
    for gram, norm, beta_col, (k, v, c_row, c_col, b_row), mask in zip(
        grams, norms, beta_cols, units, masks
    ):
        ratio = jnp.exp((c_col - c_row) + mask[0])
        lower = (beta_col * ratio) * (norm * gram)
        lowers.append(split(lower - lower * eye))
    xs = [eye16 - low[0] * levels(0) for low in lowers]
    for level in range(1, levels_of(n)):
        mask = levels(level)
        ys = [mm(low[0] * mask, x).astype(bf16) for low, x in zip(lowers, xs)]
        xs = [x - mm(x, y).astype(bf16) for x, y in zip(xs, ys)]
    lefts = [
        mm(jnp.concatenate(low, axis=1), jnp.concatenate([x, x], axis=0))
        for low, x in zip(lowers, xs)
    ]
    rests = [((eye - x.astype(f32)) - left).astype(bf16) for x, left in zip(xs, lefts)]
    invs = [x.astype(f32) + mm(x, rest) for x, rest in zip(xs, rests)]
    writes = []
    for inv, norm, (k, v, c_row, c_col, b_row), mask in zip(invs, norms, units, masks):
        for_value = inv * b_row
        for_key = inv * (b_row * jnp.exp(c_row + mask[2]) * norm)
        wv = mm(jnp.concatenate(split(for_value), axis=1), jnp.concatenate([v, v], axis=0))
        wk = mm(jnp.concatenate(split(for_key), axis=1), jnp.concatenate([k, k], axis=0))
        writes.append(jnp.concatenate([wv, wk], axis=1))
    outs = []
    for write, end, norm, (k, v, c_row, c_col, b_row), mask in zip(
        writes, end_cols, norms, units, masks
    ):
        hi, lo = split(write * end)
        kt = jnp.transpose(k)
        ew = mm(jnp.concatenate([kt, kt], axis=1), jnp.concatenate([hi, lo], axis=0))
        carry_last = jnp.exp(c_row[:, n - 1 :] + mask[2][:, n - 1 :])
        outs.append((carry_last * eye - ew[:, width:], ew[:, :width], write.astype(bf16), norm))
    return outs


def compose(maps):
    width = maps[0][0].shape[1]
    totals = [jnp.concatenate(maps[0], axis=1)]
    for map_b, add_b in maps[1:]:
        hi, lo = split(totals[-1])
        m_hi, m_lo = split(map_b)
        total = mm(jnp.concatenate([m_hi, m_lo], axis=1), jnp.concatenate([hi, hi], axis=0))
        total = total + mm(m_hi, lo)
        totals.append(jnp.concatenate([total[:, :width], total[:, width:] + add_b], axis=1))
    return totals


def block_reads(q, k, write, norm, c_row, ct_col, mask, before):
    width = q.shape[1]
    qf = q.astype(f32)
    nq = lax.rsqrt(jnp.sum(qf * qf, axis=1, keepdims=True) + EPS) * width**-0.5
    weights = (jnp.exp((ct_col - c_row) + mask[1]) * nq) * (norm * mm_t(q, k))
    got = mm(weights.astype(bf16), write)
    reads = (jnp.exp(ct_col + mask[3]) * nq) * qf - got[:, width:]
    if before is None:
        return reads.astype(bf16), got[:, :width]
    wide = mm(reads.astype(bf16), before)
    return wide[:, :width].astype(bf16), got[:, :width] + wide[:, width:]


def kernel(
    n_seq,
    n_head,
    rounds,
    q_hbm,
    k_hbm,
    v_hbm,
    beta_hbm,
    gate_hbm,
    len_hbm,
    gain_hbm,
    w_hbm,
    out_ref,
    q_s,
    k_s,
    v_s,
    w_s,
    beta_s,
    gate_s,
    len_s,
    gain_s,
    row_s,
    col_s,
    tok_s,
    pair_s,
    read_s,
    crow_s,
    ctok_s,
    erow_s,
    eye_s,
    lev_s,
    write_s,
    norm_s,
    before_s,
    map_s,
    add_s,
    g_s,
    o_s,
    send_s,
    recv_s,
    flat_s,
    part_s,
    relay_s,
    sum_s,
    got_s,
    in_sem,
    small_sem,
    w_sem,
    ring_send,
    ring_recv,
    relay_send,
    relay_recv,
    x_send,
    x_recv,
):
    z = lax.axis_index("seq")
    x = lax.axis_index("head")
    heads, subs, width = k_s.shape
    tokens = q_s.shape[1]
    blocks = tokens // BLOCK
    n = 2 * BLOCK
    right, left = lax.rem(x + 1, n_head), lax.rem(x + n_head - 1, n_head)
    has_before, has_after = z > 0, z < n_seq - 1
    odd = lax.rem(z, 2)
    first = 1 - odd
    ages = jnp.where(has_after, (jnp.minimum(rounds, z - 1) - first + 2) // 2, 0)
    ages = jnp.where(z > 0, ages, 0)
    lead = has_after & (z < rounds)
    last = jnp.where(z <= rounds, z - 1, jnp.where(odd == 1, rounds - 1, rounds))
    last = jnp.maximum(last, 0)
    starts = has_after & ((odd == 1) | (z == 0))

    smalls = [
        pltpu.make_async_copy(src, dst, small_sem.at[i])
        for i, (src, dst) in enumerate(
            ((len_hbm, len_s), (gate_hbm, gate_s), (beta_hbm, beta_s), (gain_hbm, gain_s))
        )
    ]
    for copy in smalls:
        copy.start()
    k_rows = k_hbm.reshape(subs, heads * width)
    v_rows = v_hbm.reshape(subs, heads * width)

    def loads(h):
        lanes = pl.ds(pl.multiple_of(h * width, width), width)
        return (
            pltpu.make_async_copy(k_rows.at[:, lanes], k_s.at[h], in_sem.at[0, h]),
            pltpu.make_async_copy(v_rows.at[:, lanes], v_s.at[h], in_sem.at[1, h]),
            pltpu.make_async_copy(q_hbm.at[:, lanes], q_s.at[h], in_sem.at[2, h]),
        )

    for h in range(heads):
        for copy in loads(h)[:2]:
            copy.start()
    for h in range(heads):
        loads(h)[2].start()
    w_copy = pltpu.make_async_copy(w_hbm, w_s, w_sem)
    w_copy.start()

    barrier = pltpu.get_barrier_semaphore()
    for side in (right, left):
        pl.semaphore_signal(barrier, inc=1, device_id={"head": side}, device_id_type=MESH)

    @pl.when(has_before)
    def _():
        pl.semaphore_signal(barrier, inc=1, device_id={"seq": z - 1}, device_id_type=MESH)

    eye_s[...] = (iota((n, n), 0) == iota((n, n), 1)).astype(f32)
    for level in range(levels_of(n)):
        lev_s[level] = level_mask(n, level)
    for copy in smalls:
        copy.wait()
    offset = z * tokens
    ends, run = [], 0
    for i in range(len_s.shape[0]):
        run = run + len_s[i]
        ends.append(run)
    rows, toks = vectors(gate_s[...], [beta_s[j] for j in range(2)])
    for b in range(blocks):
        cols = jnp.transpose(rows[b])
        t_cols = jnp.transpose(toks[b])
        for h in range(heads):
            row_s[h, b] = rows[b][h : h + 1]
            row_s[heads + h, b] = rows[b][heads + h : heads + h + 1]
            col_s[h, b] = cols[:, h : h + 1]
            tok_s[h, b] = t_cols[:BLOCK, h : h + 1]
        pair_s[b], read_s[b], crow_s[b], ctok_s[b], erow_s[b] = block_masks(offset, ends, b)

    @pl.when(jnp.logical_not(has_before))
    def _():
        recv_s[0] = jnp.zeros_like(recv_s[0])

    def hop(r, h):
        return pltpu.make_async_remote_copy(
            src_ref=send_s.at[r, h],
            dst_ref=recv_s.at[r, h],
            send_sem=ring_send.at[r, h],
            recv_sem=ring_recv.at[r, h],
            device_id={"seq": jnp.minimum(z + 1, n_seq - 1)},
            device_id_type=MESH,
        )

    def masks_of(b):
        return pair_s[b], read_s[b], crow_s[b], ctok_s[b], erow_s[b]

    def two_heads(pair, carry):
        hs = [2 * pair, 2 * pair + 1]
        units, masks = [], []
        for h in hs:
            for copy in loads(h)[:2]:
                copy.wait()
        for h in hs:
            for b in range(blocks):
                at = pl.ds(b * n, n)
                units.append(
                    (
                        k_s[h, at, :],
                        v_s[h, at, :],
                        row_s[h, b],
                        col_s[h, b],
                        row_s[heads + h, b],
                    )
                )
                masks.append(masks_of(b))
        outs = state_maps(units, masks, eye_s[...], lambda l: lev_s[l])

        totals = [
            compose([m[:2] for m in outs[i * blocks : (i + 1) * blocks]]) for i in range(len(hs))
        ]

        @pl.when(pair == 0)
        def _():
            pl.semaphore_wait(barrier, 2 + has_after.astype(jnp.int32))

        for h, total in zip(hs, totals):
            send_s[0, h] = total[-1][:, width:].astype(bf16)

        @pl.when(starts)
        def _():
            for h in hs:
                hop(0, h).start()

        for i, h in enumerate(hs):
            for b in range(blocks):
                write_s[h, b] = outs[i * blocks + b][2]
                norm_s[h, b] = outs[i * blocks + b][3]
            for b in range(1, blocks):
                before_s[h, b - 1] = totals[i][b - 1].astype(bf16)
            map_s[h] = jnp.concatenate(split(totals[i][-1][:, :width]), axis=1)
            add_s[h] = totals[i][-1][:, width:]
        return carry

    lax.fori_loop(0, heads // 2, two_heads, 0)

    def step(r):
        for h in range(heads):
            hop(r - 1, h).wait_recv()
            got = recv_s[r - 1, h]
            state = add_s[h] + mm(map_s[h], jnp.concatenate([got, got], axis=0))
            send_s[r, h] = state.astype(bf16)
            hop(r, h).start()

    def next_age(i):
        @pl.when((i < ages) & (first + 2 * i > 0))
        def _():
            step(first + 2 * i)

    def reads_and_step(h, carry):
        loads(h)[2].wait()
        for b in range(blocks):
            at = pl.ds(b * BLOCK, BLOCK)
            g_s[h, at, :], o_s[h, at, :] = block_reads(
                q_s[h, at, :],
                k_s[h, pl.ds(b * n, n), :],
                write_s[h, b],
                norm_s[h, b],
                row_s[h, b],
                tok_s[h, b],
                masks_of(b),
                before_s[h, b - 1] if b else None,
            )

        next_age(h)
        return carry

    def just_step(i, carry):
        next_age(i)
        return carry

    lax.fori_loop(0, heads, reads_and_step, 0)
    lax.fori_loop(heads, ages, just_step, 0)

    @pl.when(lead & (z > 0))
    def _():
        step(z)

    @pl.when(jnp.logical_not(has_after))
    def _():
        def skip(i, carry):
            for h in range(heads):
                hop(1 + 2 * i, h).wait_recv()
            return carry

        lax.fori_loop(0, (rounds - 1) // 2, skip, 0)

    waits = jnp.logical_not(has_after) | ((odd == 0) & (z >= rounds))
    for h in range(heads):

        @pl.when(waits)
        def _():
            hop(last, h).wait_recv()

        got = recv_s[last, h]
        out = o_s[h] + mm(g_s[h], got)
        mean = jnp.sum(out * out, axis=1, keepdims=True) * (1.0 / width)
        flat_s[:, h * width : (h + 1) * width] = (
            out * lax.rsqrt(mean + EPS) * gain_s[...]
        ).astype(bf16)

    chunks, _, chunk = part_s.shape
    share = out_ref.shape[0]
    lower = chunks // 2
    far = lax.rem(x + 2, n_head)

    def rows_for(dest):
        return pl.ds(pl.multiple_of(dest * share, share), share)

    def relay(c):
        return pltpu.make_async_remote_copy(
            src_ref=part_s.at[c, rows_for(far), :],
            dst_ref=relay_s.at[c],
            send_sem=relay_send.at[c],
            recv_sem=relay_recv.at[c],
            device_id={"head": right if c < lower else left},
            device_id_type=MESH,
        )

    def direct(c):
        to = left if c < lower else right
        return pltpu.make_async_remote_copy(
            src_ref=part_s.at[c, rows_for(to), :],
            dst_ref=got_s.at[0, c],
            send_sem=x_send.at[0, c],
            recv_sem=x_recv.at[0, c],
            device_id={"head": to},
            device_id_type=MESH,
        )

    def summed(c):
        to = right if c < lower else left
        return pltpu.make_async_remote_copy(
            src_ref=sum_s.at[c],
            dst_ref=got_s.at[1, c],
            send_sem=x_send.at[1, c],
            recv_sem=x_recv.at[1, c],
            device_id={"head": to},
            device_id_type=MESH,
        )

    order = [c for pair in zip(range(lower), range(lower, chunks)) for c in pair]
    w_copy.wait()
    flat = flat_s[...]
    for c in order:
        part_s[c] = mm(flat, w_s[:, c * chunk : (c + 1) * chunk]).astype(bf16)
        relay(c).start()
    for c in order:
        direct(c).start()
    for c in order:
        relay(c).wait_recv()
        to = right if c < lower else left
        sum_s[c] = (part_s[c, rows_for(to), :].astype(f32) + relay_s[c].astype(f32)).astype(bf16)
        summed(c).start()
    for c in order:
        direct(c).wait_recv()
        total = part_s[c, rows_for(x), :].astype(f32) + got_s[0, c].astype(f32)
        summed(c).wait_recv()
        out_ref[:, c * chunk : (c + 1) * chunk] = (total + got_s[1, c].astype(f32)).astype(bf16)

    def drain(i, carry):
        for h in range(heads):
            hop(first + 2 * i, h).wait_send()
        return carry

    lax.fori_loop(0, ages, drain, 0)

    @pl.when(lead)
    def _():
        for h in range(heads):
            hop(z, h).wait_send()

    for c in order:
        relay(c).wait_send()
        direct(c).wait_send()
        summed(c).wait_send()


def solution(mesh):
    n_seq, n_head = mesh.shape["seq"], mesh.shape["head"]

    def body(queries, keys, values, beta, gate, lengths, gain, weight):
        tokens, lanes = queries.shape[1:]
        refl, heads = beta.shape[2:]
        width = lanes // heads
        subs = tokens * refl
        blocks = tokens // BLOCK
        n = refl * BLOCK
        model = weight.shape[1]
        share = tokens // n_head
        rounds = min(n_seq - 1, -(-LONGEST // tokens))
        chunks = 4
        chunk = model // chunks
        hbm = pl.BlockSpec(memory_space=pltpu.HBM)
        vmem = pl.BlockSpec(memory_space=pltpu.VMEM)
        dma = pltpu.SemaphoreType.DMA
        out = pl.pallas_call(
            functools.partial(kernel, n_seq, n_head, rounds),
            out_shape=jax.ShapeDtypeStruct((share, model), bf16),
            in_specs=[hbm] * 8,
            out_specs=vmem,
            scratch_shapes=[
                pltpu.VMEM((heads, tokens, width), bf16),
                pltpu.VMEM((heads, subs, width), bf16),
                pltpu.VMEM((heads, subs, width), bf16),
                pltpu.VMEM((lanes, model), bf16),
                pltpu.VMEM((refl, heads, tokens), f32),
                pltpu.VMEM((heads, tokens), f32),
                pltpu.SMEM((lengths.shape[1],), jnp.int32),
                pltpu.VMEM((1, width), f32),
                pltpu.VMEM((2 * heads, blocks, 1, n), f32),
                pltpu.VMEM((heads, blocks, n, 1), f32),
                pltpu.VMEM((heads, blocks, BLOCK, 1), f32),
                pltpu.VMEM((blocks, n, n), f32),
                pltpu.VMEM((blocks, BLOCK, n), f32),
                pltpu.VMEM((blocks, 1, n), f32),
                pltpu.VMEM((blocks, BLOCK, 1), f32),
                pltpu.VMEM((blocks, 1, n), f32),
                pltpu.VMEM((n, n), f32),
                pltpu.VMEM((levels_of(n), n, n), bf16),
                pltpu.VMEM((heads, blocks, n, 2 * width), bf16),
                pltpu.VMEM((heads, blocks, 1, n), f32),
                pltpu.VMEM((heads, blocks - 1, width, 2 * width), bf16),
                pltpu.VMEM((heads, width, 2 * width), bf16),
                pltpu.VMEM((heads, width, width), f32),
                pltpu.VMEM((heads, tokens, width), bf16),
                pltpu.VMEM((heads, tokens, width), f32),
                pltpu.VMEM((rounds + 1, heads, width, width), bf16),
                pltpu.VMEM((rounds + 1, heads, width, width), bf16),
                pltpu.VMEM((tokens, lanes), bf16),
                pltpu.VMEM((chunks, tokens, chunk), bf16),
                pltpu.VMEM((chunks, share, chunk), bf16),
                pltpu.VMEM((chunks, share, chunk), bf16),
                pltpu.VMEM((2, chunks, share, chunk), bf16),
                dma((3, heads)),
                dma((4,)),
                dma,
                dma((rounds + 1, heads)),
                dma((rounds + 1, heads)),
                dma((chunks,)),
                dma((chunks,)),
                dma((2, chunks)),
                dma((2, chunks)),
            ],
            compiler_params=pltpu.CompilerParams(
                collective_id=0, has_side_effects=True, vmem_limit_bytes=40 * 1024 * 1024
            ),
        )(
            *[
                pltpu.with_memory_space_constraint(a, pltpu.HBM)
                for a in (
            queries[0],
            keys[0],
            values[0],
            jnp.transpose(beta[0], (1, 2, 0)),
            jnp.transpose(gate[0], (1, 0)),
            lengths[0],
            gain[None, :],
            weight,
                )
            ]
        )
        return out[None]

    packs = ("parts", "rep")
    in_specs = (
        P(packs, "seq", "head"),
        P(packs, "seq", None, "head"),
        P(packs, "seq", None, "head"),
        P(packs, "seq", None, "head"),
        P(packs, "seq", "head"),
        P(packs, None),
        P(),
        P("head", None),
    )
    out_specs = P(packs, ("seq", "head"), None)
    return jax.shard_map(body, mesh=mesh, in_specs=in_specs, out_specs=out_specs, check_vma=False)
```

```python
import functools

import jax
import jax.numpy as jnp
from jax import lax
from jax.experimental import pallas as pl
from jax.experimental.pallas import tpu as pltpu
from jax.sharding import PartitionSpec as P

BLOCK = 64
LONGEST = 2048
EPS = 1e-06
FAR = -1e30
MESH = pl.DeviceIdType.MESH
f32 = jnp.float32
bf16 = jnp.bfloat16


def mm(a, b):
    return lax.dot_general(a, b, (((1,), (0,)), ((), ())), preferred_element_type=f32)


def mm_t(a, b):
    return lax.dot_general(a, b, (((1,), (1,)), ((), ())), preferred_element_type=f32)


def split(x):
    hi = x.astype(bf16)
    return hi, (x - hi.astype(f32)).astype(bf16)


def iota(shape, dim):
    return lax.broadcasted_iota(jnp.int32, shape, dim)


def split3(x):
    first = x.astype(bf16)
    rest = x - first.astype(f32)
    second = rest.astype(bf16)
    return first, second, (rest - second.astype(f32)).astype(bf16)


def seg_of(pos, ends):
    total = jnp.zeros_like(pos)
    for end in ends:
        total = total + (pos >= end).astype(jnp.int32)
    return total


def vectors(gate, beta):
    heads, tokens = gate.shape
    n = 2 * BLOCK
    blocks = tokens // BLOCK
    left = []
    for b in range(blocks):
        at = slice(b * BLOCK, (b + 1) * BLOCK)
        part = gate[:, at]
        left.append(jnp.concatenate([part, jnp.zeros_like(part)], axis=1))
        left.append(jnp.concatenate([beta[0][:, at], beta[1][:, at]], axis=1))
    left = jnp.concatenate(left, axis=0)
    count = left.shape[0]
    k, r = iota((n, n), 0), iota((n, n), 1)
    upto = ((k < BLOCK) & (k <= r // 2)).astype(f32)
    place = (r == 2 * (k % BLOCK) + k // BLOCK).astype(f32)
    token = ((k < BLOCK) & (k <= r)).astype(f32)
    table = jnp.concatenate([upto, place, token], axis=1).astype(bf16)
    got = mm(jnp.concatenate(split3(left), axis=0), table)
    got = got[:count] + got[count : 2 * count] + got[2 * count :]
    both = 2 * heads
    first = iota((both, n), 0) < heads
    rows, toks = [], []
    for b in range(blocks):
        mine = got[b * both : (b + 1) * both]
        rows.append(jnp.where(first, mine[:, :n], mine[:, n : 2 * n]))
        toks.append(mine[:, 2 * n :])
    return rows, toks


def block_masks(offset, ends, block):
    n = 2 * BLOCK
    start = offset + block * BLOCK
    before = sum((start - 1 >= e).astype(jnp.int32) for e in ends)
    before = jnp.where(start == 0, -1, before)
    last = sum((start + BLOCK - 1 >= e).astype(jnp.int32) for e in ends)
    seg_row = seg_of(start + iota((1, n), 1) // 2, ends)
    seg_col = seg_of(start + iota((n, 1), 0) // 2, ends)
    seg_tok = seg_of(start + iota((BLOCK, 1), 0), ends)
    i, j = iota((n, n), 0), iota((n, n), 1)
    pair = jnp.where((i >= j) & (seg_col == seg_row), 0.0, FAR)
    ti, tj = iota((BLOCK, n), 0), iota((BLOCK, n), 1)
    read = jnp.where((ti >= tj // 2) & (seg_tok == seg_row), 0.0, FAR)
    carry_row = jnp.where(seg_row == before, 0.0, FAR)
    carry_tok = jnp.where(seg_tok == before, 0.0, FAR)
    end_row = jnp.where(seg_row == last, 0.0, FAR)
    return pair, read, carry_row, carry_tok, end_row


def level_mask(n, level):
    i, j = iota((n, n), 0), iota((n, n), 1)
    return ((i > j) & (lax.shift_right_logical(i ^ j, level) == 1)).astype(f32).astype(bf16)


def levels_of(n):
    return n.bit_length() - 1


def as_cols(rows):
    cols = jnp.transpose(jnp.concatenate(rows, axis=0))
    return [cols[:, u : u + 1] for u in range(len(rows))]


def state_maps(units, masks, eye, levels):
    n = eye.shape[0]
    width = units[0][0].shape[1]
    eye16 = eye.astype(bf16)
    grams = [mm_t(k, k) for k, *_ in units]
    norms = [
        lax.rsqrt(jnp.sum(gram * eye, axis=0, keepdims=True) + EPS) for gram in grams
    ]
    beta_cols = as_cols([norm * unit[4] for norm, unit in zip(norms, units)])
    end_cols = as_cols(
        [
            jnp.exp((unit[2][:, n - 1 :] - unit[2]) + mask[4]) * norm
            for norm, unit, mask in zip(norms, units, masks)
        ]
    )
    lowers = []
    for gram, norm, beta_col, (k, v, c_row, c_col, b_row), mask in zip(
        grams, norms, beta_cols, units, masks
    ):
        ratio = jnp.exp((c_col - c_row) + mask[0])
        lower = (beta_col * ratio) * (norm * gram)
        lowers.append(split(lower - lower * eye))
    xs = [eye16 - low[0] * levels(0) for low in lowers]
    for level in range(1, levels_of(n)):
        mask = levels(level)
        ys = [mm(low[0] * mask, x).astype(bf16) for low, x in zip(lowers, xs)]
        xs = [x - mm(x, y).astype(bf16) for x, y in zip(xs, ys)]
    lefts = [
        mm(jnp.concatenate(low, axis=1), jnp.concatenate([x, x], axis=0))
        for low, x in zip(lowers, xs)
    ]
    rests = [((eye - x.astype(f32)) - left).astype(bf16) for x, left in zip(xs, lefts)]
    invs = [x.astype(f32) + mm(x, rest) for x, rest in zip(xs, rests)]
    writes = []
    for inv, norm, (k, v, c_row, c_col, b_row), mask in zip(invs, norms, units, masks):
        for_value = inv * b_row
        for_key = inv * (b_row * jnp.exp(c_row + mask[2]) * norm)
        wv = mm(jnp.concatenate(split(for_value), axis=1), jnp.concatenate([v, v], axis=0))
        wk = mm(jnp.concatenate(split(for_key), axis=1), jnp.concatenate([k, k], axis=0))
        writes.append(jnp.concatenate([wv, wk], axis=1))
    outs = []
    for write, end, norm, (k, v, c_row, c_col, b_row), mask in zip(
        writes, end_cols, norms, units, masks
    ):
        hi, lo = split(write * end)
        kt = jnp.transpose(k)
        ew = mm(jnp.concatenate([kt, kt], axis=1), jnp.concatenate([hi, lo], axis=0))
        carry_last = jnp.exp(c_row[:, n - 1 :] + mask[2][:, n - 1 :])
        outs.append((carry_last * eye - ew[:, width:], ew[:, :width], write.astype(bf16), norm))
    return outs


def compose(maps):
    width = maps[0][0].shape[1]
    totals = [jnp.concatenate(maps[0], axis=1)]
    for map_b, add_b in maps[1:]:
        hi, lo = split(totals[-1])
        m_hi, m_lo = split(map_b)
        total = mm(jnp.concatenate([m_hi, m_lo], axis=1), jnp.concatenate([hi, hi], axis=0))
        total = total + mm(m_hi, lo)
        totals.append(jnp.concatenate([total[:, :width], total[:, width:] + add_b], axis=1))
    return totals


def block_reads(q, k, write, norm, c_row, ct_col, mask, before):
    width = q.shape[1]
    qf = q.astype(f32)
    nq = lax.rsqrt(jnp.sum(qf * qf, axis=1, keepdims=True) + EPS) * width**-0.5
    weights = (jnp.exp((ct_col - c_row) + mask[1]) * nq) * (norm * mm_t(q, k))
    got = mm(weights.astype(bf16), write)
    reads = (jnp.exp(ct_col + mask[3]) * nq) * qf - got[:, width:]
    if before is None:
        return reads.astype(bf16), got[:, :width]
    wide = mm(reads.astype(bf16), before)
    return wide[:, :width].astype(bf16), got[:, :width] + wide[:, width:]


def kernel(
    n_seq,
    n_head,
    rounds,
    q_hbm,
    k_hbm,
    v_hbm,
    beta_hbm,
    gate_hbm,
    len_hbm,
    gain_hbm,
    w_hbm,
    out_ref,
    q_s,
    k_s,
    v_s,
    w_s,
    beta_s,
    gate_s,
    len_s,
    gain_s,
    row_s,
    col_s,
    tok_s,
    pair_s,
    read_s,
    crow_s,
    ctok_s,
    erow_s,
    eye_s,
    lev_s,
    write_s,
    norm_s,
    before_s,
    map_s,
    add_s,
    g_s,
    o_s,
    send_s,
    recv_s,
    up_s,
    own_s,
    enter_s,
    flat_s,
    part_s,
    relay_s,
    sum_s,
    got_s,
    in_sem,
    small_sem,
    w_sem,
    near_send,
    near_recv,
    ring_send,
    ring_recv,
    relay_send,
    relay_recv,
    x_send,
    x_recv,
):
    z = lax.axis_index("seq")
    x = lax.axis_index("head")
    heads, subs, width = k_s.shape
    tokens = q_s.shape[1]
    blocks = tokens // BLOCK
    n = 2 * BLOCK
    right, left = lax.rem(x + 1, n_head), lax.rem(x + n_head - 1, n_head)
    has_before, has_after = z > 0, z < n_seq - 1
    odd = lax.rem(z, 2) == 1
    even = jnp.logical_not(odd)
    pair_at = z // 2
    reach = rounds // 2
    passes = jnp.minimum(reach, pair_at + 1)
    last = jnp.maximum(jnp.minimum(reach, pair_at) - 1, 0)
    relays = odd & has_after

    smalls = [
        pltpu.make_async_copy(src, dst, small_sem.at[i])
        for i, (src, dst) in enumerate(
            ((len_hbm, len_s), (gate_hbm, gate_s), (beta_hbm, beta_s), (gain_hbm, gain_s))
        )
    ]
    for copy in smalls:
        copy.start()
    k_rows = k_hbm.reshape(subs, heads * width)
    v_rows = v_hbm.reshape(subs, heads * width)

    def loads(h):
        lanes = pl.ds(pl.multiple_of(h * width, width), width)
        return (
            pltpu.make_async_copy(k_rows.at[:, lanes], k_s.at[h], in_sem.at[0, h]),
            pltpu.make_async_copy(v_rows.at[:, lanes], v_s.at[h], in_sem.at[1, h]),
            pltpu.make_async_copy(q_hbm.at[:, lanes], q_s.at[h], in_sem.at[2, h]),
        )

    for h in range(heads):
        for copy in loads(h)[:2]:
            copy.start()
    for h in range(heads):
        loads(h)[2].start()
    w_copy = pltpu.make_async_copy(w_hbm, w_s, w_sem)
    w_copy.start()

    barrier = pltpu.get_barrier_semaphore()
    for side in (right, left):
        pl.semaphore_signal(barrier, inc=1, device_id={"head": side}, device_id_type=MESH)

    @pl.when(has_before)
    def _():
        pl.semaphore_signal(barrier, inc=1, device_id={"seq": z - 1}, device_id_type=MESH)

    @pl.when(odd & (z > 1))
    def _():
        pl.semaphore_signal(barrier, inc=1, device_id={"seq": z - 2}, device_id_type=MESH)

    eye_s[...] = (iota((n, n), 0) == iota((n, n), 1)).astype(f32)
    for level in range(levels_of(n)):
        lev_s[level] = level_mask(n, level)
    for copy in smalls:
        copy.wait()
    offset = z * tokens
    ends, run = [], 0
    for i in range(len_s.shape[0]):
        run = run + len_s[i]
        ends.append(run)
    rows, toks = vectors(gate_s[...], [beta_s[j] for j in range(2)])
    for b in range(blocks):
        cols = jnp.transpose(rows[b])
        t_cols = jnp.transpose(toks[b])
        for h in range(heads):
            row_s[h, b] = rows[b][h : h + 1]
            row_s[heads + h, b] = rows[b][heads + h : heads + h + 1]
            col_s[h, b] = cols[:, h : h + 1]
            tok_s[h, b] = t_cols[:BLOCK, h : h + 1]
        pair_s[b], read_s[b], crow_s[b], ctok_s[b], erow_s[b] = block_masks(offset, ends, b)

    @pl.when(jnp.logical_not(has_before))
    def _():
        enter_s[...] = jnp.zeros_like(enter_s)

    def to_next(what, src, dst, sem, h, step):
        return pltpu.make_async_remote_copy(
            src_ref=src,
            dst_ref=dst,
            send_sem=sem[0].at[what, h],
            recv_sem=sem[1].at[what, h],
            device_id={"seq": jnp.minimum(z + step, n_seq - 1)},
            device_id_type=MESH,
        )

    near = (near_send, near_recv)
    ring = (ring_send, ring_recv)

    def up_add(h):
        return to_next(0, send_s.at[0, h], up_s.at[0, h], near, h, 1)

    def up_map(h):
        return to_next(1, own_s.at[h], up_s.at[1, h], near, h, 1)

    def down(h):
        return to_next(2, send_s.at[passes - 1, h], enter_s.at[h], near, h, 1)

    def hop(r, h):
        return to_next(r, send_s.at[r, h], recv_s.at[r, h], ring, h, 2)

    def masks_of(b):
        return pair_s[b], read_s[b], crow_s[b], ctok_s[b], erow_s[b]

    def two_heads(pair, carry):
        hs = [2 * pair, 2 * pair + 1]
        units, masks = [], []
        for h in hs:
            for copy in loads(h)[:2]:
                copy.wait()
        for h in hs:
            for b in range(blocks):
                at = pl.ds(b * n, n)
                units.append(
                    (
                        k_s[h, at, :],
                        v_s[h, at, :],
                        row_s[h, b],
                        col_s[h, b],
                        row_s[heads + h, b],
                    )
                )
                masks.append(masks_of(b))
        outs = state_maps(units, masks, eye_s[...], lambda l: lev_s[l])

        totals = [
            compose([m[:2] for m in outs[i * blocks : (i + 1) * blocks]]) for i in range(len(hs))
        ]

        @pl.when(pair == 0)
        def _():
            pl.semaphore_wait(
                barrier, 2 + has_after.astype(jnp.int32) + relays.astype(jnp.int32)
            )

        for h, total in zip(hs, totals):
            send_s[0, h] = total[-1][:, width:].astype(bf16)

        @pl.when(even)
        def _():
            for h in hs:
                up_add(h).start()

        for i, h in enumerate(hs):
            for b in range(blocks):
                write_s[h, b] = outs[i * blocks + b][2]
                norm_s[h, b] = outs[i * blocks + b][3]
            for b in range(1, blocks):
                before_s[h, b - 1] = totals[i][b - 1].astype(bf16)
            hi, lo = split(totals[i][-1][:, :width])
            own_s[h] = hi
            map_s[h] = jnp.concatenate([hi, lo], axis=1)
            add_s[h] = totals[i][-1][:, width:]

        @pl.when(even)
        def _():
            for h in hs:
                up_map(h).start()

        return carry

    lax.fori_loop(0, heads // 2, two_heads, 0)

    def twice(a):
        return jnp.concatenate([a, a], axis=0)

    def join():
        for h in range(heads):
            up_add(h).wait_recv()
            add = add_s[h] + mm(map_s[h], twice(up_s[0, h]))
            send_s[0, h] = add.astype(bf16)
            add_s[h] = add

            @pl.when(has_after)
            def _():
                hop(0, h).start()

            @pl.when(pair_at == 0)
            def _():
                down(h).start()

        for h in range(heads):
            up_map(h).wait_recv()
            map_s[h] = jnp.concatenate(split(mm(map_s[h], twice(up_s[1, h]))), axis=1)

    def step(r):
        for h in range(heads):
            hop(r - 1, h).wait_recv()
            state = add_s[h] + mm(map_s[h], twice(recv_s[r - 1, h]))
            send_s[r, h] = state.astype(bf16)
            hop(r, h).start()

            @pl.when(r == passes - 1)
            def _():
                down(h).start()

    def reads_and_step(h, carry):
        loads(h)[2].wait()
        for b in range(blocks):
            at = pl.ds(b * BLOCK, BLOCK)
            g_s[h, at, :], o_s[h, at, :] = block_reads(
                q_s[h, at, :],
                k_s[h, pl.ds(b * n, n), :],
                write_s[h, b],
                norm_s[h, b],
                row_s[h, b],
                tok_s[h, b],
                masks_of(b),
                before_s[h, b - 1] if b else None,
            )

        @pl.when(odd & (h == 1))
        def _():
            join()

        @pl.when(relays & (h > 1) & (h - 1 < passes))
        def _():
            step(h - 1)

        return carry

    def just_step(r, carry):
        step(r)
        return carry

    lax.fori_loop(0, heads, reads_and_step, 0)
    lax.fori_loop(heads - 1, jnp.where(relays, passes, 0), just_step, 0)

    @pl.when(jnp.logical_not(has_after))
    def _():
        def skip(r, carry):
            for h in range(heads):
                hop(r, h).wait_recv()
            return carry

        lax.fori_loop(0, last, skip, 0)

    for h in range(heads):

        @pl.when(even & has_before)
        def _():
            down(h).wait_recv()

        @pl.when(odd & (pair_at == 0))
        def _():
            enter_s[h] = up_s[0, h]

        @pl.when(odd & (pair_at >= reach))
        def _():
            hop(last, h).wait_recv()

        @pl.when(odd & (pair_at > 0))
        def _():
            state = up_s[0, h].astype(f32) + mm(up_s[1, h], recv_s[last, h])
            enter_s[h] = state.astype(bf16)

        out = o_s[h] + mm(g_s[h], enter_s[h])
        mean = jnp.sum(out * out, axis=1, keepdims=True) * (1.0 / width)
        flat_s[:, h * width : (h + 1) * width] = (
            out * lax.rsqrt(mean + EPS) * gain_s[...]
        ).astype(bf16)

    chunks, _, chunk = part_s.shape
    share = out_ref.shape[0]
    lower = chunks // 2
    far = lax.rem(x + 2, n_head)

    def rows_for(dest):
        return pl.ds(pl.multiple_of(dest * share, share), share)

    def relay(c):
        return pltpu.make_async_remote_copy(
            src_ref=part_s.at[c, rows_for(far), :],
            dst_ref=relay_s.at[c],
            send_sem=relay_send.at[c],
            recv_sem=relay_recv.at[c],
            device_id={"head": right if c < lower else left},
            device_id_type=MESH,
        )

    def direct(c):
        to = left if c < lower else right
        return pltpu.make_async_remote_copy(
            src_ref=part_s.at[c, rows_for(to), :],
            dst_ref=got_s.at[0, c],
            send_sem=x_send.at[0, c],
            recv_sem=x_recv.at[0, c],
            device_id={"head": to},
            device_id_type=MESH,
        )

    def summed(c):
        to = right if c < lower else left
        return pltpu.make_async_remote_copy(
            src_ref=sum_s.at[c],
            dst_ref=got_s.at[1, c],
            send_sem=x_send.at[1, c],
            recv_sem=x_recv.at[1, c],
            device_id={"head": to},
            device_id_type=MESH,
        )

    order = [c for pair in zip(range(lower), range(lower, chunks)) for c in pair]
    w_copy.wait()
    flat = flat_s[...]
    for c in order:
        part_s[c] = mm(flat, w_s[:, c * chunk : (c + 1) * chunk]).astype(bf16)
        relay(c).start()
    for c in order:
        direct(c).start()
    for c in order:
        relay(c).wait_recv()
        to = right if c < lower else left
        sum_s[c] = (part_s[c, rows_for(to), :].astype(f32) + relay_s[c].astype(f32)).astype(bf16)
        summed(c).start()
    for c in order:
        direct(c).wait_recv()
        total = part_s[c, rows_for(x), :].astype(f32) + got_s[0, c].astype(f32)
        summed(c).wait_recv()
        out_ref[:, c * chunk : (c + 1) * chunk] = (total + got_s[1, c].astype(f32)).astype(bf16)

    def drain(r, carry):
        for h in range(heads):
            hop(r, h).wait_send()
        return carry

    lax.fori_loop(0, jnp.where(relays, passes, 0), drain, 0)

    @pl.when(relays)
    def _():
        for h in range(heads):
            down(h).wait_send()

    @pl.when(even)
    def _():
        for h in range(heads):
            up_add(h).wait_send()
            up_map(h).wait_send()

    for c in order:
        relay(c).wait_send()
        direct(c).wait_send()
        summed(c).wait_send()


def solution(mesh):
    n_seq, n_head = mesh.shape["seq"], mesh.shape["head"]

    def body(queries, keys, values, beta, gate, lengths, gain, weight):
        tokens, lanes = queries.shape[1:]
        refl, heads = beta.shape[2:]
        width = lanes // heads
        subs = tokens * refl
        blocks = tokens // BLOCK
        n = refl * BLOCK
        model = weight.shape[1]
        share = tokens // n_head
        rounds = -(-LONGEST // tokens)
        chunks = 4
        chunk = model // chunks
        hbm = pl.BlockSpec(memory_space=pltpu.HBM)
        vmem = pl.BlockSpec(memory_space=pltpu.VMEM)
        dma = pltpu.SemaphoreType.DMA
        out = pl.pallas_call(
            functools.partial(kernel, n_seq, n_head, rounds),
            out_shape=jax.ShapeDtypeStruct((share, model), bf16),
            in_specs=[hbm] * 8,
            out_specs=vmem,
            scratch_shapes=[
                pltpu.VMEM((heads, tokens, width), bf16),
                pltpu.VMEM((heads, subs, width), bf16),
                pltpu.VMEM((heads, subs, width), bf16),
                pltpu.VMEM((lanes, model), bf16),
                pltpu.VMEM((refl, heads, tokens), f32),
                pltpu.VMEM((heads, tokens), f32),
                pltpu.SMEM((lengths.shape[1],), jnp.int32),
                pltpu.VMEM((1, width), f32),
                pltpu.VMEM((2 * heads, blocks, 1, n), f32),
                pltpu.VMEM((heads, blocks, n, 1), f32),
                pltpu.VMEM((heads, blocks, BLOCK, 1), f32),
                pltpu.VMEM((blocks, n, n), f32),
                pltpu.VMEM((blocks, BLOCK, n), f32),
                pltpu.VMEM((blocks, 1, n), f32),
                pltpu.VMEM((blocks, BLOCK, 1), f32),
                pltpu.VMEM((blocks, 1, n), f32),
                pltpu.VMEM((n, n), f32),
                pltpu.VMEM((levels_of(n), n, n), bf16),
                pltpu.VMEM((heads, blocks, n, 2 * width), bf16),
                pltpu.VMEM((heads, blocks, 1, n), f32),
                pltpu.VMEM((heads, blocks - 1, width, 2 * width), bf16),
                pltpu.VMEM((heads, width, 2 * width), bf16),
                pltpu.VMEM((heads, width, width), f32),
                pltpu.VMEM((heads, tokens, width), bf16),
                pltpu.VMEM((heads, tokens, width), f32),
                pltpu.VMEM((rounds // 2, heads, width, width), bf16),
                pltpu.VMEM((rounds // 2, heads, width, width), bf16),
                pltpu.VMEM((2, heads, width, width), bf16),
                pltpu.VMEM((heads, width, width), bf16),
                pltpu.VMEM((heads, width, width), bf16),
                pltpu.VMEM((tokens, lanes), bf16),
                pltpu.VMEM((chunks, tokens, chunk), bf16),
                pltpu.VMEM((chunks, share, chunk), bf16),
                pltpu.VMEM((chunks, share, chunk), bf16),
                pltpu.VMEM((2, chunks, share, chunk), bf16),
                dma((3, heads)),
                dma((4,)),
                dma,
                dma((3, heads)),
                dma((3, heads)),
                dma((rounds // 2, heads)),
                dma((rounds // 2, heads)),
                dma((chunks,)),
                dma((chunks,)),
                dma((2, chunks)),
                dma((2, chunks)),
            ],
            compiler_params=pltpu.CompilerParams(
                collective_id=0, has_side_effects=True, vmem_limit_bytes=40 * 1024 * 1024
            ),
        )(
            *[
                pltpu.with_memory_space_constraint(a, pltpu.HBM)
                for a in (
            queries[0],
            keys[0],
            values[0],
            jnp.transpose(beta[0], (1, 2, 0)),
            jnp.transpose(gate[0], (1, 0)),
            lengths[0],
            gain[None, :],
            weight,
                )
            ]
        )
        return out[None]

    packs = ("parts", "rep")
    in_specs = (
        P(packs, "seq", "head"),
        P(packs, "seq", None, "head"),
        P(packs, "seq", None, "head"),
        P(packs, "seq", None, "head"),
        P(packs, "seq", "head"),
        P(packs, None),
        P(),
        P("head", None),
    )
    out_specs = P(packs, ("seq", "head"), None)
    return jax.shard_map(body, mesh=mesh, in_specs=in_specs, out_specs=out_specs, check_vma=False)
```

```python
import functools

import jax
import jax.numpy as jnp
from jax import lax
from jax.experimental import pallas as pl
from jax.experimental.pallas import tpu as pltpu
from jax.sharding import PartitionSpec as P

BLOCK = 64
LONGEST = 2048
EPS = 1e-06
FAR = -1e30
MESH = pl.DeviceIdType.MESH
f32 = jnp.float32
bf16 = jnp.bfloat16


def mm(a, b):
    return lax.dot_general(a, b, (((1,), (0,)), ((), ())), preferred_element_type=f32)


def mm_t(a, b):
    return lax.dot_general(a, b, (((1,), (1,)), ((), ())), preferred_element_type=f32)


def split(x):
    hi = x.astype(bf16)
    return hi, (x - hi.astype(f32)).astype(bf16)


def iota(shape, dim):
    return lax.broadcasted_iota(jnp.int32, shape, dim)


def split3(x):
    first = x.astype(bf16)
    rest = x - first.astype(f32)
    second = rest.astype(bf16)
    return first, second, (rest - second.astype(f32)).astype(bf16)


def seg_of(pos, ends):
    total = jnp.zeros_like(pos)
    for end in ends:
        total = total + (pos >= end).astype(jnp.int32)
    return total


def vectors(gate, beta):
    heads, tokens = gate.shape
    n = 2 * BLOCK
    blocks = tokens // BLOCK
    left = []
    for b in range(blocks):
        at = slice(b * BLOCK, (b + 1) * BLOCK)
        part = gate[:, at]
        left.append(jnp.concatenate([part, jnp.zeros_like(part)], axis=1))
        left.append(jnp.concatenate([beta[0][:, at], beta[1][:, at]], axis=1))
    left = jnp.concatenate(left, axis=0)
    count = left.shape[0]
    k, r = iota((n, n), 0), iota((n, n), 1)
    upto = ((k < BLOCK) & (k <= r // 2)).astype(f32)
    place = (r == 2 * (k % BLOCK) + k // BLOCK).astype(f32)
    token = ((k < BLOCK) & (k <= r)).astype(f32)
    table = jnp.concatenate([upto, place, token], axis=1).astype(bf16)
    got = mm(jnp.concatenate(split3(left), axis=0), table)
    got = got[:count] + got[count : 2 * count] + got[2 * count :]
    both = 2 * heads
    first = iota((both, n), 0) < heads
    rows, toks = [], []
    for b in range(blocks):
        mine = got[b * both : (b + 1) * both]
        rows.append(jnp.where(first, mine[:, :n], mine[:, n : 2 * n]))
        toks.append(mine[:, 2 * n :])
    return rows, toks


def block_masks(offset, ends, block):
    n = 2 * BLOCK
    start = offset + block * BLOCK
    before = sum((start - 1 >= e).astype(jnp.int32) for e in ends)
    before = jnp.where(start == 0, -1, before)
    last = sum((start + BLOCK - 1 >= e).astype(jnp.int32) for e in ends)
    seg_row = seg_of(start + iota((1, n), 1) // 2, ends)
    seg_col = seg_of(start + iota((n, 1), 0) // 2, ends)
    seg_tok = seg_of(start + iota((BLOCK, 1), 0), ends)
    i, j = iota((n, n), 0), iota((n, n), 1)
    pair = jnp.where((i >= j) & (seg_col == seg_row), 0.0, FAR)
    ti, tj = iota((BLOCK, n), 0), iota((BLOCK, n), 1)
    read = jnp.where((ti >= tj // 2) & (seg_tok == seg_row), 0.0, FAR)
    carry_row = jnp.where(seg_row == before, 0.0, FAR)
    carry_tok = jnp.where(seg_tok == before, 0.0, FAR)
    end_row = jnp.where(seg_row == last, 0.0, FAR)
    return pair, read, carry_row, carry_tok, end_row


def level_mask(n, level):
    i, j = iota((n, n), 0), iota((n, n), 1)
    return ((i > j) & (lax.shift_right_logical(i ^ j, level) == 1)).astype(f32).astype(bf16)


def levels_of(n):
    return n.bit_length() - 1


def as_cols(rows):
    cols = jnp.transpose(jnp.concatenate(rows, axis=0))
    return [cols[:, u : u + 1] for u in range(len(rows))]


def state_maps(units, masks, eye, levels):
    n = eye.shape[0]
    width = units[0][0].shape[1]
    eye16 = eye.astype(bf16)
    grams = [mm_t(k, k) for k, *_ in units]
    norms = [
        lax.rsqrt(jnp.sum(gram * eye, axis=0, keepdims=True) + EPS) for gram in grams
    ]
    beta_cols = as_cols([norm * unit[4] for norm, unit in zip(norms, units)])
    end_cols = as_cols(
        [
            jnp.exp((unit[2][:, n - 1 :] - unit[2]) + mask[4]) * norm
            for norm, unit, mask in zip(norms, units, masks)
        ]
    )
    lowers = []
    for gram, norm, beta_col, (k, v, c_row, c_col, b_row), mask in zip(
        grams, norms, beta_cols, units, masks
    ):
        ratio = jnp.exp((c_col - c_row) + mask[0])
        lower = (beta_col * ratio) * (norm * gram)
        lowers.append(split(lower - lower * eye))
    xs = [eye16 - low[0] * levels(0) for low in lowers]
    for level in range(1, levels_of(n)):
        mask = levels(level)
        ys = [mm(low[0] * mask, x).astype(bf16) for low, x in zip(lowers, xs)]
        xs = [x - mm(x, y).astype(bf16) for x, y in zip(xs, ys)]
    lefts = [
        mm(jnp.concatenate(low, axis=1), jnp.concatenate([x, x], axis=0))
        for low, x in zip(lowers, xs)
    ]
    rests = [((eye - x.astype(f32)) - left).astype(bf16) for x, left in zip(xs, lefts)]
    invs = [x.astype(f32) + mm(x, rest) for x, rest in zip(xs, rests)]
    writes = []
    for inv, norm, (k, v, c_row, c_col, b_row), mask in zip(invs, norms, units, masks):
        for_value = inv * b_row
        for_key = inv * (b_row * jnp.exp(c_row + mask[2]) * norm)
        wv = mm(jnp.concatenate(split(for_value), axis=1), jnp.concatenate([v, v], axis=0))
        wk = mm(jnp.concatenate(split(for_key), axis=1), jnp.concatenate([k, k], axis=0))
        writes.append(jnp.concatenate([wv, wk], axis=1))
    outs = []
    for write, end, norm, (k, v, c_row, c_col, b_row), mask in zip(
        writes, end_cols, norms, units, masks
    ):
        hi, lo = split(write * end)
        kt = jnp.transpose(k)
        ew = mm(jnp.concatenate([kt, kt], axis=1), jnp.concatenate([hi, lo], axis=0))
        carry_last = jnp.exp(c_row[:, n - 1 :] + mask[2][:, n - 1 :])
        outs.append((carry_last * eye - ew[:, width:], ew[:, :width], write.astype(bf16), norm))
    return outs


def compose(maps):
    width = maps[0][0].shape[1]
    totals = [jnp.concatenate(maps[0], axis=1)]
    for map_b, add_b in maps[1:]:
        hi, lo = split(totals[-1])
        m_hi, m_lo = split(map_b)
        total = mm(jnp.concatenate([m_hi, m_lo], axis=1), jnp.concatenate([hi, hi], axis=0))
        total = total + mm(m_hi, lo)
        totals.append(jnp.concatenate([total[:, :width], total[:, width:] + add_b], axis=1))
    return totals


def block_reads(q, k, write, norm, c_row, ct_col, mask, before):
    width = q.shape[1]
    qf = q.astype(f32)
    nq = lax.rsqrt(jnp.sum(qf * qf, axis=1, keepdims=True) + EPS) * width**-0.5
    weights = (jnp.exp((ct_col - c_row) + mask[1]) * nq) * (norm * mm_t(q, k))
    got = mm(weights.astype(bf16), write)
    reads = (jnp.exp(ct_col + mask[3]) * nq) * qf - got[:, width:]
    if before is None:
        return reads.astype(bf16), got[:, :width]
    wide = mm(reads.astype(bf16), before)
    return wide[:, :width].astype(bf16), got[:, :width] + wide[:, width:]


def kernel(
    n_seq,
    n_head,
    rounds,
    q_hbm,
    k_hbm,
    v_hbm,
    beta_hbm,
    gate_hbm,
    len_hbm,
    gain_hbm,
    w_hbm,
    out_ref,
    q_s,
    k_s,
    v_s,
    w_s,
    beta_s,
    gate_s,
    len_s,
    gain_s,
    row_s,
    col_s,
    tok_s,
    pair_s,
    read_s,
    crow_s,
    ctok_s,
    erow_s,
    eye_s,
    lev_s,
    write_s,
    norm_s,
    before_s,
    map_s,
    add_s,
    g_s,
    o_s,
    send_s,
    recv_s,
    up_s,
    own_s,
    enter_s,
    flat_s,
    part_s,
    relay_s,
    sum_s,
    got_s,
    in_sem,
    small_sem,
    w_sem,
    near_send,
    near_recv,
    ring_send,
    ring_recv,
    relay_send,
    relay_recv,
    x_send,
    x_recv,
):
    z = lax.axis_index("seq")
    x = lax.axis_index("head")
    heads, subs, width = k_s.shape
    tokens = q_s.shape[1]
    blocks = tokens // BLOCK
    n = 2 * BLOCK
    right, left = lax.rem(x + 1, n_head), lax.rem(x + n_head - 1, n_head)
    has_before, has_after = z > 0, z < n_seq - 1
    odd = lax.rem(z, 2) == 1
    even = jnp.logical_not(odd)
    pair_at = z // 2
    reach = rounds // 2
    relays = odd & has_after
    odd_pair = lax.rem(pair_at, 2)

    def incoming(pair):
        late = jnp.where(lax.rem(pair, 2) == 1, reach - 1, reach)
        return jnp.where(pair <= reach, pair - 1, late)

    last = jnp.maximum(incoming(pair_at), 0)
    down_at = incoming(pair_at + 1)
    starts = relays & ((odd_pair == 1) | (pair_at == 0))
    lead = relays & (pair_at < reach)

    smalls = [
        pltpu.make_async_copy(src, dst, small_sem.at[i])
        for i, (src, dst) in enumerate(
            ((len_hbm, len_s), (gate_hbm, gate_s), (beta_hbm, beta_s), (gain_hbm, gain_s))
        )
    ]
    for copy in smalls:
        copy.start()
    k_rows = k_hbm.reshape(subs, heads * width)
    v_rows = v_hbm.reshape(subs, heads * width)

    def loads(h):
        lanes = pl.ds(pl.multiple_of(h * width, width), width)
        return (
            pltpu.make_async_copy(k_rows.at[:, lanes], k_s.at[h], in_sem.at[0, h]),
            pltpu.make_async_copy(v_rows.at[:, lanes], v_s.at[h], in_sem.at[1, h]),
            pltpu.make_async_copy(q_hbm.at[:, lanes], q_s.at[h], in_sem.at[2, h]),
        )

    for h in range(heads):
        for copy in loads(h)[:2]:
            copy.start()
    for h in range(heads):
        loads(h)[2].start()
    w_copy = pltpu.make_async_copy(w_hbm, w_s, w_sem)
    w_copy.start()

    barrier = pltpu.get_barrier_semaphore()
    for side in (right, left):
        pl.semaphore_signal(barrier, inc=1, device_id={"head": side}, device_id_type=MESH)

    @pl.when(has_before)
    def _():
        pl.semaphore_signal(barrier, inc=1, device_id={"seq": z - 1}, device_id_type=MESH)

    @pl.when(odd & (z > 1))
    def _():
        pl.semaphore_signal(barrier, inc=1, device_id={"seq": z - 2}, device_id_type=MESH)

    eye_s[...] = (iota((n, n), 0) == iota((n, n), 1)).astype(f32)
    for level in range(levels_of(n)):
        lev_s[level] = level_mask(n, level)
    for copy in smalls:
        copy.wait()
    offset = z * tokens
    ends, run = [], 0
    for i in range(len_s.shape[0]):
        run = run + len_s[i]
        ends.append(run)
    rows, toks = vectors(gate_s[...], [beta_s[j] for j in range(2)])
    for b in range(blocks):
        cols = jnp.transpose(rows[b])
        t_cols = jnp.transpose(toks[b])
        for h in range(heads):
            row_s[h, b] = rows[b][h : h + 1]
            row_s[heads + h, b] = rows[b][heads + h : heads + h + 1]
            col_s[h, b] = cols[:, h : h + 1]
            tok_s[h, b] = t_cols[:BLOCK, h : h + 1]
        pair_s[b], read_s[b], crow_s[b], ctok_s[b], erow_s[b] = block_masks(offset, ends, b)

    @pl.when(jnp.logical_not(has_before))
    def _():
        enter_s[...] = jnp.zeros_like(enter_s)

    def to_next(what, src, dst, sem, h, step):
        return pltpu.make_async_remote_copy(
            src_ref=src,
            dst_ref=dst,
            send_sem=sem[0].at[what, h],
            recv_sem=sem[1].at[what, h],
            device_id={"seq": jnp.minimum(z + step, n_seq - 1)},
            device_id_type=MESH,
        )

    near = (near_send, near_recv)
    ring = (ring_send, ring_recv)

    def up_add(h):
        return to_next(0, send_s.at[0, h], up_s.at[0, h], near, h, 1)

    def up_map(h):
        return to_next(1, own_s.at[h], up_s.at[1, h], near, h, 1)

    def down(h):
        return to_next(2, send_s.at[down_at, h], enter_s.at[h], near, h, 1)

    def hop(r, h):
        return to_next(r, send_s.at[r, h], recv_s.at[r, h], ring, h, 2)

    def masks_of(b):
        return pair_s[b], read_s[b], crow_s[b], ctok_s[b], erow_s[b]

    def two_heads(pair, carry):
        hs = [2 * pair, 2 * pair + 1]
        units, masks = [], []
        for h in hs:
            for copy in loads(h)[:2]:
                copy.wait()
        for h in hs:
            for b in range(blocks):
                at = pl.ds(b * n, n)
                units.append(
                    (
                        k_s[h, at, :],
                        v_s[h, at, :],
                        row_s[h, b],
                        col_s[h, b],
                        row_s[heads + h, b],
                    )
                )
                masks.append(masks_of(b))
        outs = state_maps(units, masks, eye_s[...], lambda l: lev_s[l])

        totals = [
            compose([m[:2] for m in outs[i * blocks : (i + 1) * blocks]]) for i in range(len(hs))
        ]

        @pl.when(pair == 0)
        def _():
            pl.semaphore_wait(
                barrier, 2 + has_after.astype(jnp.int32) + relays.astype(jnp.int32)
            )

        for h, total in zip(hs, totals):
            send_s[0, h] = total[-1][:, width:].astype(bf16)

        @pl.when(even)
        def _():
            for h in hs:
                up_add(h).start()

        for i, h in enumerate(hs):
            for b in range(blocks):
                write_s[h, b] = outs[i * blocks + b][2]
                norm_s[h, b] = outs[i * blocks + b][3]
            for b in range(1, blocks):
                before_s[h, b - 1] = totals[i][b - 1].astype(bf16)
            hi, lo = split(totals[i][-1][:, :width])
            own_s[h] = hi
            map_s[h] = jnp.concatenate([hi, lo], axis=1)
            add_s[h] = totals[i][-1][:, width:]

        @pl.when(even)
        def _():
            for h in hs:
                up_map(h).start()

        return carry

    lax.fori_loop(0, heads // 2, two_heads, 0)

    def twice(a):
        return jnp.concatenate([a, a], axis=0)

    def join():
        for h in range(heads):
            up_add(h).wait_recv()
            add = add_s[h] + mm(map_s[h], twice(up_s[0, h]))
            send_s[0, h] = add.astype(bf16)
            add_s[h] = add

            @pl.when(starts)
            def _():
                hop(0, h).start()

            @pl.when(pair_at == 0)
            def _():
                down(h).start()

        for h in range(heads):
            up_map(h).wait_recv()
            map_s[h] = jnp.concatenate(split(mm(map_s[h], twice(up_s[1, h]))), axis=1)

    def step(r):
        for h in range(heads):
            hop(r - 1, h).wait_recv()
            state = add_s[h] + mm(map_s[h], twice(recv_s[r - 1, h]))
            send_s[r, h] = state.astype(bf16)
            hop(r, h).start()

            @pl.when(r == down_at)
            def _():
                down(h).start()

    def reads_and_step(h, carry):
        loads(h)[2].wait()
        for b in range(blocks):
            at = pl.ds(b * BLOCK, BLOCK)
            g_s[h, at, :], o_s[h, at, :] = block_reads(
                q_s[h, at, :],
                k_s[h, pl.ds(b * n, n), :],
                write_s[h, b],
                norm_s[h, b],
                row_s[h, b],
                tok_s[h, b],
                masks_of(b),
                before_s[h, b - 1] if b else None,
            )

        @pl.when(odd & (h == 1))
        def _():
            join()

        age = 1 - odd_pair + 2 * (h - 2 + odd_pair)

        @pl.when(relays & (h > 1) & (age <= jnp.minimum(reach, pair_at - 1)))
        def _():
            step(age)

        return carry

    lax.fori_loop(0, heads, reads_and_step, 0)

    @pl.when(lead & (pair_at > 0))
    def _():
        step(pair_at)

    @pl.when(jnp.logical_not(has_after))
    def _():
        def skip(i, carry):
            for h in range(heads):
                hop(1 + 2 * i, h).wait_recv()
            return carry

        lax.fori_loop(0, (reach - 1) // 2, skip, 0)

    waits = odd & (jnp.logical_not(has_after) | ((odd_pair == 0) & (pair_at >= reach)))
    for h in range(heads):

        @pl.when(even & has_before)
        def _():
            down(h).wait_recv()

        @pl.when(odd & (pair_at == 0))
        def _():
            enter_s[h] = up_s[0, h]

        @pl.when(waits)
        def _():
            hop(last, h).wait_recv()

        @pl.when(odd & (pair_at > 0))
        def _():
            state = up_s[0, h].astype(f32) + mm(up_s[1, h], recv_s[last, h])
            enter_s[h] = state.astype(bf16)

        out = o_s[h] + mm(g_s[h], enter_s[h])
        mean = jnp.sum(out * out, axis=1, keepdims=True) * (1.0 / width)
        flat_s[:, h * width : (h + 1) * width] = (
            out * lax.rsqrt(mean + EPS) * gain_s[...]
        ).astype(bf16)

    chunks, _, chunk = part_s.shape
    share = out_ref.shape[0]
    lower = chunks // 2
    far = lax.rem(x + 2, n_head)

    def rows_for(dest):
        return pl.ds(pl.multiple_of(dest * share, share), share)

    def relay(c):
        return pltpu.make_async_remote_copy(
            src_ref=part_s.at[c, rows_for(far), :],
            dst_ref=relay_s.at[c],
            send_sem=relay_send.at[c],
            recv_sem=relay_recv.at[c],
            device_id={"head": right if c < lower else left},
            device_id_type=MESH,
        )

    def direct(c):
        to = left if c < lower else right
        return pltpu.make_async_remote_copy(
            src_ref=part_s.at[c, rows_for(to), :],
            dst_ref=got_s.at[0, c],
            send_sem=x_send.at[0, c],
            recv_sem=x_recv.at[0, c],
            device_id={"head": to},
            device_id_type=MESH,
        )

    def summed(c):
        to = right if c < lower else left
        return pltpu.make_async_remote_copy(
            src_ref=sum_s.at[c],
            dst_ref=got_s.at[1, c],
            send_sem=x_send.at[1, c],
            recv_sem=x_recv.at[1, c],
            device_id={"head": to},
            device_id_type=MESH,
        )

    order = [c for pair in zip(range(lower), range(lower, chunks)) for c in pair]
    w_copy.wait()
    flat = flat_s[...]
    for c in order:
        part_s[c] = mm(flat, w_s[:, c * chunk : (c + 1) * chunk]).astype(bf16)
        relay(c).start()
    for c in order:
        direct(c).start()
    for c in order:
        relay(c).wait_recv()
        to = right if c < lower else left
        sum_s[c] = (part_s[c, rows_for(to), :].astype(f32) + relay_s[c].astype(f32)).astype(bf16)
        summed(c).start()
    for c in order:
        direct(c).wait_recv()
        total = part_s[c, rows_for(x), :].astype(f32) + got_s[0, c].astype(f32)
        summed(c).wait_recv()
        out_ref[:, c * chunk : (c + 1) * chunk] = (total + got_s[1, c].astype(f32)).astype(bf16)

    for r in range(reach + 1):
        sent = lax.rem(r + odd_pair, 2) == 1
        sent = sent & (r < pair_at)

        @pl.when(relays & (sent | (lead & (pair_at == r))))
        def _():
            for h in range(heads):
                hop(r, h).wait_send()

    @pl.when(relays)
    def _():
        for h in range(heads):
            down(h).wait_send()

    @pl.when(even)
    def _():
        for h in range(heads):
            up_add(h).wait_send()
            up_map(h).wait_send()

    for c in order:
        relay(c).wait_send()
        direct(c).wait_send()
        summed(c).wait_send()


def solution(mesh):
    n_seq, n_head = mesh.shape["seq"], mesh.shape["head"]

    def body(queries, keys, values, beta, gate, lengths, gain, weight):
        tokens, lanes = queries.shape[1:]
        refl, heads = beta.shape[2:]
        width = lanes // heads
        subs = tokens * refl
        blocks = tokens // BLOCK
        n = refl * BLOCK
        model = weight.shape[1]
        share = tokens // n_head
        rounds = -(-LONGEST // tokens)
        chunks = 4
        chunk = model // chunks
        hbm = pl.BlockSpec(memory_space=pltpu.HBM)
        vmem = pl.BlockSpec(memory_space=pltpu.VMEM)
        dma = pltpu.SemaphoreType.DMA
        out = pl.pallas_call(
            functools.partial(kernel, n_seq, n_head, rounds),
            out_shape=jax.ShapeDtypeStruct((share, model), bf16),
            in_specs=[hbm] * 8,
            out_specs=vmem,
            scratch_shapes=[
                pltpu.VMEM((heads, tokens, width), bf16),
                pltpu.VMEM((heads, subs, width), bf16),
                pltpu.VMEM((heads, subs, width), bf16),
                pltpu.VMEM((lanes, model), bf16),
                pltpu.VMEM((refl, heads, tokens), f32),
                pltpu.VMEM((heads, tokens), f32),
                pltpu.SMEM((lengths.shape[1],), jnp.int32),
                pltpu.VMEM((1, width), f32),
                pltpu.VMEM((2 * heads, blocks, 1, n), f32),
                pltpu.VMEM((heads, blocks, n, 1), f32),
                pltpu.VMEM((heads, blocks, BLOCK, 1), f32),
                pltpu.VMEM((blocks, n, n), f32),
                pltpu.VMEM((blocks, BLOCK, n), f32),
                pltpu.VMEM((blocks, 1, n), f32),
                pltpu.VMEM((blocks, BLOCK, 1), f32),
                pltpu.VMEM((blocks, 1, n), f32),
                pltpu.VMEM((n, n), f32),
                pltpu.VMEM((levels_of(n), n, n), bf16),
                pltpu.VMEM((heads, blocks, n, 2 * width), bf16),
                pltpu.VMEM((heads, blocks, 1, n), f32),
                pltpu.VMEM((heads, blocks - 1, width, 2 * width), bf16),
                pltpu.VMEM((heads, width, 2 * width), bf16),
                pltpu.VMEM((heads, width, width), f32),
                pltpu.VMEM((heads, tokens, width), bf16),
                pltpu.VMEM((heads, tokens, width), f32),
                pltpu.VMEM((rounds // 2 + 1, heads, width, width), bf16),
                pltpu.VMEM((rounds // 2 + 1, heads, width, width), bf16),
                pltpu.VMEM((2, heads, width, width), bf16),
                pltpu.VMEM((heads, width, width), bf16),
                pltpu.VMEM((heads, width, width), bf16),
                pltpu.VMEM((tokens, lanes), bf16),
                pltpu.VMEM((chunks, tokens, chunk), bf16),
                pltpu.VMEM((chunks, share, chunk), bf16),
                pltpu.VMEM((chunks, share, chunk), bf16),
                pltpu.VMEM((2, chunks, share, chunk), bf16),
                dma((3, heads)),
                dma((4,)),
                dma,
                dma((3, heads)),
                dma((3, heads)),
                dma((rounds // 2 + 1, heads)),
                dma((rounds // 2 + 1, heads)),
                dma((chunks,)),
                dma((chunks,)),
                dma((2, chunks)),
                dma((2, chunks)),
            ],
            compiler_params=pltpu.CompilerParams(
                collective_id=0, has_side_effects=True, vmem_limit_bytes=40 * 1024 * 1024
            ),
        )(
            *[
                pltpu.with_memory_space_constraint(a, pltpu.HBM)
                for a in (
            queries[0],
            keys[0],
            values[0],
            jnp.transpose(beta[0], (1, 2, 0)),
            jnp.transpose(gate[0], (1, 0)),
            lengths[0],
            gain[None, :],
            weight,
                )
            ]
        )
        return out[None]

    packs = ("parts", "rep")
    in_specs = (
        P(packs, "seq", "head"),
        P(packs, "seq", None, "head"),
        P(packs, "seq", None, "head"),
        P(packs, "seq", None, "head"),
        P(packs, "seq", "head"),
        P(packs, None),
        P(),
        P("head", None),
    )
    out_specs = P(packs, ("seq", "head"), None)
    return jax.shard_map(body, mesh=mesh, in_specs=in_specs, out_specs=out_specs, check_vma=False)
```

```python
import functools

import jax
import jax.numpy as jnp
from jax import lax
from jax.experimental import pallas as pl
from jax.experimental.pallas import tpu as pltpu
from jax.sharding import PartitionSpec as P

BLOCK = 64
LONGEST = 2048
EPS = 1e-06
FAR = -1e30
MESH = pl.DeviceIdType.MESH
f32 = jnp.float32
bf16 = jnp.bfloat16


def mm(a, b):
    return lax.dot_general(a, b, (((1,), (0,)), ((), ())), preferred_element_type=f32)


def mm_t(a, b):
    return lax.dot_general(a, b, (((1,), (1,)), ((), ())), preferred_element_type=f32)


def split(x):
    hi = x.astype(bf16)
    return hi, (x - hi.astype(f32)).astype(bf16)


def iota(shape, dim):
    return lax.broadcasted_iota(jnp.int32, shape, dim)


def split3(x):
    first = x.astype(bf16)
    rest = x - first.astype(f32)
    second = rest.astype(bf16)
    return first, second, (rest - second.astype(f32)).astype(bf16)


def seg_of(pos, ends):
    total = jnp.zeros_like(pos)
    for end in ends:
        total = total + (pos >= end).astype(jnp.int32)
    return total


def vectors(gate, beta):
    heads, tokens = gate.shape
    n = 2 * BLOCK
    blocks = tokens // BLOCK
    left = []
    for b in range(blocks):
        at = slice(b * BLOCK, (b + 1) * BLOCK)
        part = gate[:, at]
        left.append(jnp.concatenate([part, jnp.zeros_like(part)], axis=1))
        left.append(jnp.concatenate([beta[0][:, at], beta[1][:, at]], axis=1))
    left = jnp.concatenate(left, axis=0)
    count = left.shape[0]
    k, r = iota((n, n), 0), iota((n, n), 1)
    upto = ((k < BLOCK) & (k <= r // 2)).astype(f32)
    place = (r == 2 * (k % BLOCK) + k // BLOCK).astype(f32)
    token = ((k < BLOCK) & (k <= r)).astype(f32)
    table = jnp.concatenate([upto, place, token], axis=1).astype(bf16)
    got = mm(jnp.concatenate(split3(left), axis=0), table)
    got = got[:count] + got[count : 2 * count] + got[2 * count :]
    both = 2 * heads
    first = iota((both, n), 0) < heads
    rows, toks = [], []
    for b in range(blocks):
        mine = got[b * both : (b + 1) * both]
        rows.append(jnp.where(first, mine[:, :n], mine[:, n : 2 * n]))
        toks.append(mine[:, 2 * n :])
    return rows, toks


def block_masks(offset, ends, block):
    n = 2 * BLOCK
    start = offset + block * BLOCK
    before = sum((start - 1 >= e).astype(jnp.int32) for e in ends)
    before = jnp.where(start == 0, -1, before)
    last = sum((start + BLOCK - 1 >= e).astype(jnp.int32) for e in ends)
    seg_row = seg_of(start + iota((1, n), 1) // 2, ends)
    seg_col = seg_of(start + iota((n, 1), 0) // 2, ends)
    seg_tok = seg_of(start + iota((BLOCK, 1), 0), ends)
    i, j = iota((n, n), 0), iota((n, n), 1)
    pair = jnp.where((i >= j) & (seg_col == seg_row), 0.0, FAR)
    ti, tj = iota((BLOCK, n), 0), iota((BLOCK, n), 1)
    read = jnp.where((ti >= tj // 2) & (seg_tok == seg_row), 0.0, FAR)
    carry_row = jnp.where(seg_row == before, 0.0, FAR)
    carry_tok = jnp.where(seg_tok == before, 0.0, FAR)
    end_row = jnp.where(seg_row == last, 0.0, FAR)
    return pair, read, carry_row, carry_tok, end_row


def level_mask(n, level):
    i, j = iota((n, n), 0), iota((n, n), 1)
    return ((i > j) & (lax.shift_right_logical(i ^ j, level) == 1)).astype(f32).astype(bf16)


def levels_of(n):
    return n.bit_length() - 1


def as_cols(rows):
    cols = jnp.transpose(jnp.concatenate(rows, axis=0))
    return [cols[:, u : u + 1] for u in range(len(rows))]


def state_maps(units, masks, eye, levels):
    n = eye.shape[0]
    width = units[0][0].shape[1]
    eye16 = eye.astype(bf16)
    grams = [mm_t(k, k) for k, *_ in units]
    norms = [
        lax.rsqrt(jnp.sum(gram * eye, axis=0, keepdims=True) + EPS) for gram in grams
    ]
    beta_cols = as_cols([norm * unit[4] for norm, unit in zip(norms, units)])
    end_cols = as_cols(
        [
            jnp.exp((unit[2][:, n - 1 :] - unit[2]) + mask[4]) * norm
            for norm, unit, mask in zip(norms, units, masks)
        ]
    )
    lowers = []
    for gram, norm, beta_col, (k, v, c_row, c_col, b_row), mask in zip(
        grams, norms, beta_cols, units, masks
    ):
        ratio = jnp.exp((c_col - c_row) + mask[0])
        lower = (beta_col * ratio) * (norm * gram)
        lowers.append(split(lower - lower * eye))
    xs = [eye16 - low[0] * levels(0) for low in lowers]
    for level in range(1, levels_of(n)):
        mask = levels(level)
        ys = [mm(low[0] * mask, x).astype(bf16) for low, x in zip(lowers, xs)]
        xs = [x - mm(x, y).astype(bf16) for x, y in zip(xs, ys)]
    lefts = [
        mm(jnp.concatenate(low, axis=1), jnp.concatenate([x, x], axis=0))
        for low, x in zip(lowers, xs)
    ]
    rests = [((eye - x.astype(f32)) - left).astype(bf16) for x, left in zip(xs, lefts)]
    invs = [x.astype(f32) + mm(x, rest) for x, rest in zip(xs, rests)]
    writes = []
    for inv, norm, (k, v, c_row, c_col, b_row), mask in zip(invs, norms, units, masks):
        for_value = inv * b_row
        for_key = inv * (b_row * jnp.exp(c_row + mask[2]) * norm)
        wv = mm(jnp.concatenate(split(for_value), axis=1), jnp.concatenate([v, v], axis=0))
        wk = mm(jnp.concatenate(split(for_key), axis=1), jnp.concatenate([k, k], axis=0))
        writes.append(jnp.concatenate([wv, wk], axis=1))
    outs = []
    for write, end, norm, (k, v, c_row, c_col, b_row), mask in zip(
        writes, end_cols, norms, units, masks
    ):
        hi, lo = split(write * end)
        kt = jnp.transpose(k)
        ew = mm(jnp.concatenate([kt, kt], axis=1), jnp.concatenate([hi, lo], axis=0))
        carry_last = jnp.exp(c_row[:, n - 1 :] + mask[2][:, n - 1 :])
        outs.append((carry_last * eye - ew[:, width:], ew[:, :width], write.astype(bf16), norm))
    return outs


def compose(maps):
    width = maps[0][0].shape[1]
    totals = [jnp.concatenate(maps[0], axis=1)]
    for map_b, add_b in maps[1:]:
        hi, lo = split(totals[-1])
        m_hi, m_lo = split(map_b)
        total = mm(jnp.concatenate([m_hi, m_lo], axis=1), jnp.concatenate([hi, hi], axis=0))
        total = total + mm(m_hi, lo)
        totals.append(jnp.concatenate([total[:, :width], total[:, width:] + add_b], axis=1))
    return totals


def block_reads(q, k, write, norm, c_row, ct_col, mask, before):
    width = q.shape[1]
    qf = q.astype(f32)
    nq = lax.rsqrt(jnp.sum(qf * qf, axis=1, keepdims=True) + EPS) * width**-0.5
    weights = (jnp.exp((ct_col - c_row) + mask[1]) * nq) * (norm * mm_t(q, k))
    got = mm(weights.astype(bf16), write)
    reads = (jnp.exp(ct_col + mask[3]) * nq) * qf - got[:, width:]
    if before is None:
        return reads.astype(bf16), got[:, :width]
    wide = mm(reads.astype(bf16), before)
    return wide[:, :width].astype(bf16), got[:, :width] + wide[:, width:]


def kernel(
    n_seq,
    n_head,
    rounds,
    q_hbm,
    k_hbm,
    v_hbm,
    beta_hbm,
    gate_hbm,
    len_hbm,
    gain_hbm,
    w_hbm,
    out_ref,
    q_s,
    k_s,
    v_s,
    w_s,
    beta_s,
    gate_s,
    len_s,
    gain_s,
    row_s,
    col_s,
    tok_s,
    pair_s,
    read_s,
    crow_s,
    ctok_s,
    erow_s,
    eye_s,
    lev_s,
    write_s,
    norm_s,
    before_s,
    map_s,
    add_s,
    g_s,
    o_s,
    send_s,
    recv_s,
    up_s,
    own_s,
    enter_s,
    flat_s,
    part_s,
    relay_s,
    sum_s,
    got_s,
    in_sem,
    small_sem,
    w_sem,
    near_send,
    near_recv,
    ring_send,
    ring_recv,
    relay_send,
    relay_recv,
    x_send,
    x_recv,
):
    z = lax.axis_index("seq")
    x = lax.axis_index("head")
    heads, subs, width = k_s.shape
    tokens = q_s.shape[1]
    blocks = tokens // BLOCK
    n = 2 * BLOCK
    right, left = lax.rem(x + 1, n_head), lax.rem(x + n_head - 1, n_head)
    has_before, has_after = z > 0, z < n_seq - 1
    odd = lax.rem(z, 2) == 1
    even = jnp.logical_not(odd)
    pair_at = z // 2
    reach = rounds // 2
    relays = odd & has_after
    odd_pair = lax.rem(pair_at, 2)

    def incoming(pair):
        late = jnp.where(lax.rem(pair, 2) == 1, reach - 1, reach)
        return jnp.where(pair <= reach, pair - 1, late)

    last = jnp.maximum(incoming(pair_at), 0)
    down_at = incoming(pair_at + 1)
    starts = relays & ((odd_pair == 1) | (pair_at == 0))
    lead = relays & (pair_at < reach)

    smalls = [
        pltpu.make_async_copy(src, dst, small_sem.at[i])
        for i, (src, dst) in enumerate(
            ((len_hbm, len_s), (gate_hbm, gate_s), (beta_hbm, beta_s), (gain_hbm, gain_s))
        )
    ]
    for copy in smalls:
        copy.start()
    k_rows = k_hbm.reshape(subs, heads * width)
    v_rows = v_hbm.reshape(subs, heads * width)

    def loads(h):
        lanes = pl.ds(pl.multiple_of(h * width, width), width)
        return (
            pltpu.make_async_copy(k_rows.at[:, lanes], k_s.at[h], in_sem.at[0, h]),
            pltpu.make_async_copy(v_rows.at[:, lanes], v_s.at[h], in_sem.at[1, h]),
            pltpu.make_async_copy(q_hbm.at[:, lanes], q_s.at[h], in_sem.at[2, h]),
        )

    for h in range(heads):
        for copy in loads(h)[:2]:
            copy.start()
    for h in range(heads):
        loads(h)[2].start()
    w_copy = pltpu.make_async_copy(w_hbm, w_s, w_sem)
    w_copy.start()

    barrier = pltpu.get_barrier_semaphore()
    for side in (right, left):
        pl.semaphore_signal(barrier, inc=1, device_id={"head": side}, device_id_type=MESH)

    @pl.when(has_before)
    def _():
        pl.semaphore_signal(barrier, inc=1, device_id={"seq": z - 1}, device_id_type=MESH)

    @pl.when(odd & (z > 1))
    def _():
        pl.semaphore_signal(barrier, inc=1, device_id={"seq": z - 2}, device_id_type=MESH)

    eye_s[...] = (iota((n, n), 0) == iota((n, n), 1)).astype(f32)
    for level in range(levels_of(n)):
        lev_s[level] = level_mask(n, level)
    for copy in smalls:
        copy.wait()
    offset = z * tokens
    ends, run = [], 0
    for i in range(len_s.shape[0]):
        run = run + len_s[i]
        ends.append(run)
    rows, toks = vectors(gate_s[...], [beta_s[j] for j in range(2)])
    for b in range(blocks):
        cols = jnp.transpose(rows[b])
        t_cols = jnp.transpose(toks[b])
        for h in range(heads):
            row_s[h, b] = rows[b][h : h + 1]
            row_s[heads + h, b] = rows[b][heads + h : heads + h + 1]
            col_s[h, b] = cols[:, h : h + 1]
            tok_s[h, b] = t_cols[:BLOCK, h : h + 1]
        pair_s[b], read_s[b], crow_s[b], ctok_s[b], erow_s[b] = block_masks(offset, ends, b)

    @pl.when(jnp.logical_not(has_before))
    def _():
        enter_s[...] = jnp.zeros_like(enter_s)

    def to_next(what, src, dst, sem, h, step):
        return pltpu.make_async_remote_copy(
            src_ref=src,
            dst_ref=dst,
            send_sem=sem[0].at[what, h],
            recv_sem=sem[1].at[what, h],
            device_id={"seq": jnp.minimum(z + step, n_seq - 1)},
            device_id_type=MESH,
        )

    near = (near_send, near_recv)
    ring = (ring_send, ring_recv)

    def up_add(h):
        return to_next(0, send_s.at[0, h], up_s.at[0, h], near, h, 1)

    def up_map(h):
        return to_next(1, own_s.at[h], up_s.at[1, h], near, h, 1)

    def down(h):
        return to_next(2, send_s.at[down_at, h], enter_s.at[h], near, h, 1)

    def hop(r, h):
        return to_next(r, send_s.at[r, h], recv_s.at[r, h], ring, h, 2)

    def masks_of(b):
        return pair_s[b], read_s[b], crow_s[b], ctok_s[b], erow_s[b]

    units, masks = [], []
    for h in range(heads):
        for copy in loads(h)[:2]:
            copy.wait()
    for h in range(heads):
        for b in range(blocks):
            at = pl.ds(b * n, n)
            units.append(
                (k_s[h, at, :], v_s[h, at, :], row_s[h, b], col_s[h, b], row_s[heads + h, b])
            )
            masks.append(masks_of(b))
    outs = state_maps(units, masks, eye_s[...], lambda l: lev_s[l])
    totals = [compose([m[:2] for m in outs[h * blocks : (h + 1) * blocks]]) for h in range(heads)]
    for h in range(heads):
        send_s[0, h] = totals[h][-1][:, width:].astype(bf16)
        hi, lo = split(totals[h][-1][:, :width])
        own_s[h] = hi
        map_s[h] = jnp.concatenate([hi, lo], axis=1)

    pl.semaphore_wait(barrier, 2 + has_after.astype(jnp.int32) + relays.astype(jnp.int32))

    @pl.when(even)
    def _():
        for h in range(heads):
            up_add(h).start()
        for h in range(heads):
            up_map(h).start()

    for h in range(heads):
        add_s[h] = totals[h][-1][:, width:]
        for b in range(blocks):
            write_s[h, b] = outs[h * blocks + b][2]
            norm_s[h, b] = outs[h * blocks + b][3]
        for b in range(1, blocks):
            before_s[h, b - 1] = totals[h][b - 1].astype(bf16)

    def twice(a):
        return jnp.concatenate([a, a], axis=0)

    def join():
        for h in range(heads):
            up_add(h).wait_recv()
            add = add_s[h] + mm(map_s[h], twice(up_s[0, h]))
            send_s[0, h] = add.astype(bf16)
            add_s[h] = add

            @pl.when(starts)
            def _():
                hop(0, h).start()

            @pl.when(pair_at == 0)
            def _():
                down(h).start()

        for h in range(heads):
            up_map(h).wait_recv()
            map_s[h] = jnp.concatenate(split(mm(map_s[h], twice(up_s[1, h]))), axis=1)

    def step(r):
        for h in range(heads):
            hop(r - 1, h).wait_recv()
            state = add_s[h] + mm(map_s[h], twice(recv_s[r - 1, h]))
            send_s[r, h] = state.astype(bf16)
            hop(r, h).start()

            @pl.when(r == down_at)
            def _():
                down(h).start()

    def reads_and_join(i, carry):
        for h in (2 * i, 2 * i + 1):
            loads(h)[2].wait()
        for h in (2 * i, 2 * i + 1):
            for b in range(blocks):
                at = pl.ds(b * BLOCK, BLOCK)
                g_s[h, at, :], o_s[h, at, :] = block_reads(
                    q_s[h, at, :],
                    k_s[h, pl.ds(b * n, n), :],
                    write_s[h, b],
                    norm_s[h, b],
                    row_s[h, b],
                    tok_s[h, b],
                    masks_of(b),
                    before_s[h, b - 1] if b else None,
                )

        @pl.when(odd & (i == (pair_at == 0).astype(jnp.int32)))
        def _():
            join()

        return carry

    lax.fori_loop(0, heads // 2, reads_and_join, 0)

    def next_age(i, carry):
        age = 1 - odd_pair + 2 * (i + odd_pair)

        @pl.when(relays & (age <= jnp.minimum(reach, pair_at - 1)))
        def _():
            step(age)

        return carry

    lax.fori_loop(0, reach // 2, next_age, 0)

    @pl.when(lead & (pair_at > 0))
    def _():
        step(pair_at)

    @pl.when(jnp.logical_not(has_after))
    def _():
        def skip(i, carry):
            for h in range(heads):
                hop(1 + 2 * i, h).wait_recv()
            return carry

        lax.fori_loop(0, (reach - 1) // 2, skip, 0)

    waits = odd & (jnp.logical_not(has_after) | ((odd_pair == 0) & (pair_at >= reach)))
    for h in range(heads):

        @pl.when(even & has_before)
        def _():
            down(h).wait_recv()

        @pl.when(odd & (pair_at == 0))
        def _():
            enter_s[h] = up_s[0, h]

        @pl.when(waits)
        def _():
            hop(last, h).wait_recv()

        @pl.when(odd & (pair_at > 0))
        def _():
            state = up_s[0, h].astype(f32) + mm(up_s[1, h], recv_s[last, h])
            enter_s[h] = state.astype(bf16)

        out = o_s[h] + mm(g_s[h], enter_s[h])
        mean = jnp.sum(out * out, axis=1, keepdims=True) * (1.0 / width)
        flat_s[:, h * width : (h + 1) * width] = (
            out * lax.rsqrt(mean + EPS) * gain_s[...]
        ).astype(bf16)

    chunks, _, chunk = part_s.shape
    share = out_ref.shape[0]
    lower = chunks // 2
    far = lax.rem(x + 2, n_head)

    def rows_for(dest):
        return pl.ds(pl.multiple_of(dest * share, share), share)

    def relay(c):
        return pltpu.make_async_remote_copy(
            src_ref=part_s.at[c, rows_for(far), :],
            dst_ref=relay_s.at[c],
            send_sem=relay_send.at[c],
            recv_sem=relay_recv.at[c],
            device_id={"head": right if c < lower else left},
            device_id_type=MESH,
        )

    def direct(c):
        to = left if c < lower else right
        return pltpu.make_async_remote_copy(
            src_ref=part_s.at[c, rows_for(to), :],
            dst_ref=got_s.at[0, c],
            send_sem=x_send.at[0, c],
            recv_sem=x_recv.at[0, c],
            device_id={"head": to},
            device_id_type=MESH,
        )

    def summed(c):
        to = right if c < lower else left
        return pltpu.make_async_remote_copy(
            src_ref=sum_s.at[c],
            dst_ref=got_s.at[1, c],
            send_sem=x_send.at[1, c],
            recv_sem=x_recv.at[1, c],
            device_id={"head": to},
            device_id_type=MESH,
        )

    order = [c for pair in zip(range(lower), range(lower, chunks)) for c in pair]
    w_copy.wait()
    flat = flat_s[...]
    for c in order:
        part_s[c] = mm(flat, w_s[:, c * chunk : (c + 1) * chunk]).astype(bf16)
        relay(c).start()
    for c in order:
        direct(c).start()
    for c in order:
        relay(c).wait_recv()
        to = right if c < lower else left
        sum_s[c] = (part_s[c, rows_for(to), :].astype(f32) + relay_s[c].astype(f32)).astype(bf16)
        summed(c).start()
    for c in order:
        direct(c).wait_recv()
        total = part_s[c, rows_for(x), :].astype(f32) + got_s[0, c].astype(f32)
        summed(c).wait_recv()
        out_ref[:, c * chunk : (c + 1) * chunk] = (total + got_s[1, c].astype(f32)).astype(bf16)

    for r in range(reach + 1):
        sent = lax.rem(r + odd_pair, 2) == 1
        sent = sent & (r < pair_at)

        @pl.when(relays & (sent | (lead & (pair_at == r))))
        def _():
            for h in range(heads):
                hop(r, h).wait_send()

    @pl.when(relays)
    def _():
        for h in range(heads):
            down(h).wait_send()

    @pl.when(even)
    def _():
        for h in range(heads):
            up_add(h).wait_send()
            up_map(h).wait_send()

    for c in order:
        relay(c).wait_send()
        direct(c).wait_send()
        summed(c).wait_send()


def solution(mesh):
    n_seq, n_head = mesh.shape["seq"], mesh.shape["head"]

    def body(queries, keys, values, beta, gate, lengths, gain, weight):
        tokens, lanes = queries.shape[1:]
        refl, heads = beta.shape[2:]
        width = lanes // heads
        subs = tokens * refl
        blocks = tokens // BLOCK
        n = refl * BLOCK
        model = weight.shape[1]
        share = tokens // n_head
        rounds = -(-LONGEST // tokens)
        chunks = 4
        chunk = model // chunks
        hbm = pl.BlockSpec(memory_space=pltpu.HBM)
        vmem = pl.BlockSpec(memory_space=pltpu.VMEM)
        dma = pltpu.SemaphoreType.DMA
        out = pl.pallas_call(
            functools.partial(kernel, n_seq, n_head, rounds),
            out_shape=jax.ShapeDtypeStruct((share, model), bf16),
            in_specs=[hbm] * 8,
            out_specs=vmem,
            scratch_shapes=[
                pltpu.VMEM((heads, tokens, width), bf16),
                pltpu.VMEM((heads, subs, width), bf16),
                pltpu.VMEM((heads, subs, width), bf16),
                pltpu.VMEM((lanes, model), bf16),
                pltpu.VMEM((refl, heads, tokens), f32),
                pltpu.VMEM((heads, tokens), f32),
                pltpu.SMEM((lengths.shape[1],), jnp.int32),
                pltpu.VMEM((1, width), f32),
                pltpu.VMEM((2 * heads, blocks, 1, n), f32),
                pltpu.VMEM((heads, blocks, n, 1), f32),
                pltpu.VMEM((heads, blocks, BLOCK, 1), f32),
                pltpu.VMEM((blocks, n, n), f32),
                pltpu.VMEM((blocks, BLOCK, n), f32),
                pltpu.VMEM((blocks, 1, n), f32),
                pltpu.VMEM((blocks, BLOCK, 1), f32),
                pltpu.VMEM((blocks, 1, n), f32),
                pltpu.VMEM((n, n), f32),
                pltpu.VMEM((levels_of(n), n, n), bf16),
                pltpu.VMEM((heads, blocks, n, 2 * width), bf16),
                pltpu.VMEM((heads, blocks, 1, n), f32),
                pltpu.VMEM((heads, blocks - 1, width, 2 * width), bf16),
                pltpu.VMEM((heads, width, 2 * width), bf16),
                pltpu.VMEM((heads, width, width), f32),
                pltpu.VMEM((heads, tokens, width), bf16),
                pltpu.VMEM((heads, tokens, width), f32),
                pltpu.VMEM((rounds // 2 + 1, heads, width, width), bf16),
                pltpu.VMEM((rounds // 2 + 1, heads, width, width), bf16),
                pltpu.VMEM((2, heads, width, width), bf16),
                pltpu.VMEM((heads, width, width), bf16),
                pltpu.VMEM((heads, width, width), bf16),
                pltpu.VMEM((tokens, lanes), bf16),
                pltpu.VMEM((chunks, tokens, chunk), bf16),
                pltpu.VMEM((chunks, share, chunk), bf16),
                pltpu.VMEM((chunks, share, chunk), bf16),
                pltpu.VMEM((2, chunks, share, chunk), bf16),
                dma((3, heads)),
                dma((4,)),
                dma,
                dma((3, heads)),
                dma((3, heads)),
                dma((rounds // 2 + 1, heads)),
                dma((rounds // 2 + 1, heads)),
                dma((chunks,)),
                dma((chunks,)),
                dma((2, chunks)),
                dma((2, chunks)),
            ],
            compiler_params=pltpu.CompilerParams(
                collective_id=0, has_side_effects=True, vmem_limit_bytes=40 * 1024 * 1024
            ),
        )(
            *[
                pltpu.with_memory_space_constraint(a, pltpu.HBM)
                for a in (
            queries[0],
            keys[0],
            values[0],
            jnp.transpose(beta[0], (1, 2, 0)),
            jnp.transpose(gate[0], (1, 0)),
            lengths[0],
            gain[None, :],
            weight,
                )
            ]
        )
        return out[None]

    packs = ("parts", "rep")
    in_specs = (
        P(packs, "seq", "head"),
        P(packs, "seq", None, "head"),
        P(packs, "seq", None, "head"),
        P(packs, "seq", None, "head"),
        P(packs, "seq", "head"),
        P(packs, None),
        P(),
        P("head", None),
    )
    out_specs = P(packs, ("seq", "head"), None)
    return jax.shard_map(body, mesh=mesh, in_specs=in_specs, out_specs=out_specs, check_vma=False)
```

```python
import functools

import jax
import jax.numpy as jnp
from jax import lax
from jax.experimental import pallas as pl
from jax.experimental.pallas import tpu as pltpu
from jax.sharding import PartitionSpec as P

BLOCK = 64
LONGEST = 2048
EPS = 1e-06
FAR = -1e30
MESH = pl.DeviceIdType.MESH
f32 = jnp.float32
bf16 = jnp.bfloat16


def mm(a, b):
    return lax.dot_general(a, b, (((1,), (0,)), ((), ())), preferred_element_type=f32)


def mm_t(a, b):
    return lax.dot_general(a, b, (((1,), (1,)), ((), ())), preferred_element_type=f32)


def split(x):
    hi = x.astype(bf16)
    return hi, (x - hi.astype(f32)).astype(bf16)


def iota(shape, dim):
    return lax.broadcasted_iota(jnp.int32, shape, dim)


def split3(x):
    first = x.astype(bf16)
    rest = x - first.astype(f32)
    second = rest.astype(bf16)
    return first, second, (rest - second.astype(f32)).astype(bf16)


def seg_of(pos, ends):
    total = jnp.zeros_like(pos)
    for end in ends:
        total = total + (pos >= end).astype(jnp.int32)
    return total


def vectors(gate, beta):
    heads, tokens = gate.shape
    n = 2 * BLOCK
    blocks = tokens // BLOCK
    left = []
    for b in range(blocks):
        at = slice(b * BLOCK, (b + 1) * BLOCK)
        part = gate[:, at]
        left.append(jnp.concatenate([part, jnp.zeros_like(part)], axis=1))
        left.append(jnp.concatenate([beta[0][:, at], beta[1][:, at]], axis=1))
    left = jnp.concatenate(left, axis=0)
    count = left.shape[0]
    k, r = iota((n, n), 0), iota((n, n), 1)
    upto = ((k < BLOCK) & (k <= r // 2)).astype(f32)
    place = (r == 2 * (k % BLOCK) + k // BLOCK).astype(f32)
    token = ((k < BLOCK) & (k <= r)).astype(f32)
    table = jnp.concatenate([upto, place, token], axis=1).astype(bf16)
    got = mm(jnp.concatenate(split3(left), axis=0), table)
    got = got[:count] + got[count : 2 * count] + got[2 * count :]
    both = 2 * heads
    first = iota((both, n), 0) < heads
    rows, toks = [], []
    for b in range(blocks):
        mine = got[b * both : (b + 1) * both]
        rows.append(jnp.where(first, mine[:, :n], mine[:, n : 2 * n]))
        toks.append(mine[:, 2 * n :])
    return rows, toks


def block_masks(offset, ends, block):
    n = 2 * BLOCK
    start = offset + block * BLOCK
    before = sum((start - 1 >= e).astype(jnp.int32) for e in ends)
    before = jnp.where(start == 0, -1, before)
    last = sum((start + BLOCK - 1 >= e).astype(jnp.int32) for e in ends)
    seg_row = seg_of(start + iota((1, n), 1) // 2, ends)
    seg_col = seg_of(start + iota((n, 1), 0) // 2, ends)
    seg_tok = seg_of(start + iota((BLOCK, 1), 0), ends)
    i, j = iota((n, n), 0), iota((n, n), 1)
    pair = jnp.where((i >= j) & (seg_col == seg_row), 0.0, FAR)
    ti, tj = iota((BLOCK, n), 0), iota((BLOCK, n), 1)
    read = jnp.where((ti >= tj // 2) & (seg_tok == seg_row), 0.0, FAR)
    carry_row = jnp.where(seg_row == before, 0.0, FAR)
    carry_tok = jnp.where(seg_tok == before, 0.0, FAR)
    end_row = jnp.where(seg_row == last, 0.0, FAR)
    return pair, read, carry_row, carry_tok, end_row


def level_mask(n, level):
    i, j = iota((n, n), 0), iota((n, n), 1)
    return ((i > j) & (lax.shift_right_logical(i ^ j, level) == 1)).astype(f32).astype(bf16)


def levels_of(n):
    return n.bit_length() - 1


def as_cols(rows):
    cols = jnp.transpose(jnp.concatenate(rows, axis=0))
    return [cols[:, u : u + 1] for u in range(len(rows))]


def state_maps(units, masks, eye, levels):
    n = eye.shape[0]
    width = units[0][0].shape[1]
    eye16 = eye.astype(bf16)
    grams = [mm_t(k, k) for k, *_ in units]
    norms = [
        lax.rsqrt(jnp.sum(gram * eye, axis=0, keepdims=True) + EPS) for gram in grams
    ]
    beta_cols = as_cols([norm * unit[4] for norm, unit in zip(norms, units)])
    end_cols = as_cols(
        [
            jnp.exp((unit[2][:, n - 1 :] - unit[2]) + mask[4]) * norm
            for norm, unit, mask in zip(norms, units, masks)
        ]
    )
    lowers = []
    for gram, norm, beta_col, (k, v, c_row, c_col, b_row), mask in zip(
        grams, norms, beta_cols, units, masks
    ):
        ratio = jnp.exp((c_col - c_row) + mask[0])
        lower = (beta_col * ratio) * (norm * gram)
        lowers.append(split(lower - lower * eye))
    xs = [eye16 - low[0] * levels(0) for low in lowers]
    for level in range(1, levels_of(n)):
        mask = levels(level)
        ys = [mm(low[0] * mask, x).astype(bf16) for low, x in zip(lowers, xs)]
        xs = [x - mm(x, y).astype(bf16) for x, y in zip(xs, ys)]
    lefts = [
        mm(jnp.concatenate(low, axis=1), jnp.concatenate([x, x], axis=0))
        for low, x in zip(lowers, xs)
    ]
    rests = [((eye - x.astype(f32)) - left).astype(bf16) for x, left in zip(xs, lefts)]
    invs = [x.astype(f32) + mm(x, rest) for x, rest in zip(xs, rests)]
    writes = []
    for inv, norm, (k, v, c_row, c_col, b_row), mask in zip(invs, norms, units, masks):
        for_value = inv * b_row
        for_key = inv * (b_row * jnp.exp(c_row + mask[2]) * norm)
        wv = mm(jnp.concatenate(split(for_value), axis=1), jnp.concatenate([v, v], axis=0))
        wk = mm(jnp.concatenate(split(for_key), axis=1), jnp.concatenate([k, k], axis=0))
        writes.append(jnp.concatenate([wv, wk], axis=1))
    outs = []
    for write, end, norm, (k, v, c_row, c_col, b_row), mask in zip(
        writes, end_cols, norms, units, masks
    ):
        hi, lo = split(write * end)
        kt = jnp.transpose(k)
        ew = mm(jnp.concatenate([kt, kt], axis=1), jnp.concatenate([hi, lo], axis=0))
        carry_last = jnp.exp(c_row[:, n - 1 :] + mask[2][:, n - 1 :])
        outs.append((carry_last * eye - ew[:, width:], ew[:, :width], write.astype(bf16), norm))
    return outs


def compose(maps):
    width = maps[0][0].shape[1]
    totals = [jnp.concatenate(maps[0], axis=1)]
    for map_b, add_b in maps[1:]:
        hi, lo = split(totals[-1])
        m_hi, m_lo = split(map_b)
        total = mm(jnp.concatenate([m_hi, m_lo], axis=1), jnp.concatenate([hi, hi], axis=0))
        total = total + mm(m_hi, lo)
        totals.append(jnp.concatenate([total[:, :width], total[:, width:] + add_b], axis=1))
    return totals


def block_reads(q, k, write, norm, c_row, ct_col, mask, before):
    width = q.shape[1]
    qf = q.astype(f32)
    nq = lax.rsqrt(jnp.sum(qf * qf, axis=1, keepdims=True) + EPS) * width**-0.5
    weights = (jnp.exp((ct_col - c_row) + mask[1]) * nq) * (norm * mm_t(q, k))
    got = mm(weights.astype(bf16), write)
    reads = (jnp.exp(ct_col + mask[3]) * nq) * qf - got[:, width:]
    if before is None:
        return reads.astype(bf16), got[:, :width]
    wide = mm(reads.astype(bf16), before)
    return wide[:, :width].astype(bf16), got[:, :width] + wide[:, width:]


def kernel(
    n_seq,
    n_head,
    rounds,
    q_hbm,
    k_hbm,
    v_hbm,
    beta_hbm,
    gate_hbm,
    len_hbm,
    gain_hbm,
    w_hbm,
    out_ref,
    q_s,
    k_s,
    v_s,
    w_s,
    beta_s,
    gate_s,
    len_s,
    gain_s,
    row_s,
    col_s,
    tok_s,
    pair_s,
    read_s,
    crow_s,
    ctok_s,
    erow_s,
    eye_s,
    lev_s,
    write_s,
    norm_s,
    before_s,
    map_s,
    add_s,
    g_s,
    o_s,
    send_s,
    recv_s,
    up_s,
    own_s,
    enter_s,
    flat_s,
    part_s,
    relay_s,
    sum_s,
    got_s,
    in_sem,
    small_sem,
    w_sem,
    near_send,
    near_recv,
    ring_send,
    ring_recv,
    relay_send,
    relay_recv,
    x_send,
    x_recv,
):
    z = lax.axis_index("seq")
    x = lax.axis_index("head")
    heads, subs, width = k_s.shape
    tokens = q_s.shape[1]
    blocks = tokens // BLOCK
    n = 2 * BLOCK
    right, left = lax.rem(x + 1, n_head), lax.rem(x + n_head - 1, n_head)
    has_before, has_after = z > 0, z < n_seq - 1
    odd = lax.rem(z, 2) == 1
    even = jnp.logical_not(odd)
    pair_at = z // 2
    reach = rounds // 2
    relays = odd & has_after
    last = (pair_at > reach).astype(jnp.int32)
    down_at = (pair_at + 1 > reach).astype(jnp.int32)
    sends = (relays & (pair_at < reach), relays & (pair_at > 0))

    smalls = [
        pltpu.make_async_copy(src, dst, small_sem.at[i])
        for i, (src, dst) in enumerate(
            ((len_hbm, len_s), (gate_hbm, gate_s), (beta_hbm, beta_s), (gain_hbm, gain_s))
        )
    ]
    for copy in smalls:
        copy.start()
    k_rows = k_hbm.reshape(subs, heads * width)
    v_rows = v_hbm.reshape(subs, heads * width)

    def loads(h):
        lanes = pl.ds(pl.multiple_of(h * width, width), width)
        return (
            pltpu.make_async_copy(k_rows.at[:, lanes], k_s.at[h], in_sem.at[0, h]),
            pltpu.make_async_copy(v_rows.at[:, lanes], v_s.at[h], in_sem.at[1, h]),
            pltpu.make_async_copy(q_hbm.at[:, lanes], q_s.at[h], in_sem.at[2, h]),
        )

    for h in range(heads):
        for copy in loads(h)[:2]:
            copy.start()
    for h in range(heads):
        loads(h)[2].start()
    w_copy = pltpu.make_async_copy(w_hbm, w_s, w_sem)
    w_copy.start()

    barrier = pltpu.get_barrier_semaphore()
    for side in (right, left):
        pl.semaphore_signal(barrier, inc=1, device_id={"head": side}, device_id_type=MESH)

    @pl.when(has_before)
    def _():
        pl.semaphore_signal(barrier, inc=1, device_id={"seq": z - 1}, device_id_type=MESH)

    @pl.when(odd & (z > 1))
    def _():
        pl.semaphore_signal(barrier, inc=1, device_id={"seq": z - 2}, device_id_type=MESH)

    eye_s[...] = (iota((n, n), 0) == iota((n, n), 1)).astype(f32)
    for level in range(levels_of(n)):
        lev_s[level] = level_mask(n, level)
    for copy in smalls:
        copy.wait()
    offset = z * tokens
    ends, run = [], 0
    for i in range(len_s.shape[0]):
        run = run + len_s[i]
        ends.append(run)
    rows, toks = vectors(gate_s[...], [beta_s[j] for j in range(2)])
    for b in range(blocks):
        cols = jnp.transpose(rows[b])
        t_cols = jnp.transpose(toks[b])
        for h in range(heads):
            row_s[h, b] = rows[b][h : h + 1]
            row_s[heads + h, b] = rows[b][heads + h : heads + h + 1]
            col_s[h, b] = cols[:, h : h + 1]
            tok_s[h, b] = t_cols[:BLOCK, h : h + 1]
        pair_s[b], read_s[b], crow_s[b], ctok_s[b], erow_s[b] = block_masks(offset, ends, b)

    @pl.when(jnp.logical_not(has_before))
    def _():
        enter_s[...] = jnp.zeros_like(enter_s)

    def to_next(what, src, dst, sem, h, step):
        return pltpu.make_async_remote_copy(
            src_ref=src,
            dst_ref=dst,
            send_sem=sem[0].at[what, h],
            recv_sem=sem[1].at[what, h],
            device_id={"seq": jnp.minimum(z + step, n_seq - 1)},
            device_id_type=MESH,
        )

    near = (near_send, near_recv)
    ring = (ring_send, ring_recv)

    def up_add(h):
        return to_next(0, send_s.at[0, h], up_s.at[0, h], near, h, 1)

    def up_map(h):
        return to_next(1, own_s.at[h], up_s.at[1, h], near, h, 1)

    def down(h):
        return to_next(2, send_s.at[down_at, h], enter_s.at[h], near, h, 1)

    def hop(r, h):
        return to_next(r, send_s.at[r, h], recv_s.at[r, h], ring, h, 2)

    def masks_of(b):
        return pair_s[b], read_s[b], crow_s[b], ctok_s[b], erow_s[b]

    units, masks = [], []
    for h in range(heads):
        for copy in loads(h)[:2]:
            copy.wait()
    for h in range(heads):
        for b in range(blocks):
            at = pl.ds(b * n, n)
            units.append(
                (k_s[h, at, :], v_s[h, at, :], row_s[h, b], col_s[h, b], row_s[heads + h, b])
            )
            masks.append(masks_of(b))
    outs = state_maps(units, masks, eye_s[...], lambda l: lev_s[l])
    totals = [compose([m[:2] for m in outs[h * blocks : (h + 1) * blocks]]) for h in range(heads)]
    for h in range(heads):
        send_s[0, h] = totals[h][-1][:, width:].astype(bf16)
        hi, lo = split(totals[h][-1][:, :width])
        own_s[h] = hi
        map_s[h] = jnp.concatenate([hi, lo], axis=1)

    pl.semaphore_wait(barrier, 2 + has_after.astype(jnp.int32) + relays.astype(jnp.int32))

    @pl.when(even)
    def _():
        for h in range(heads):
            up_add(h).start()
        for h in range(heads):
            up_map(h).start()

    for h in range(heads):
        add_s[h] = totals[h][-1][:, width:]
        for b in range(blocks):
            write_s[h, b] = outs[h * blocks + b][2]
            norm_s[h, b] = outs[h * blocks + b][3]
        for b in range(1, blocks):
            before_s[h, b - 1] = totals[h][b - 1].astype(bf16)

    def twice(a):
        return jnp.concatenate([a, a], axis=0)

    def join():
        for h in range(heads):
            up_add(h).wait_recv()
            add = add_s[h] + mm(map_s[h], twice(up_s[0, h]))
            add_s[h] = add

            @pl.when(relays & (pair_at < 2))
            def _():
                send_s[pair_at, h] = add.astype(bf16)
                hop(pair_at, h).start()

            @pl.when(pair_at == 0)
            def _():
                down(h).start()

        for h in range(heads):
            up_map(h).wait_recv()
            map_s[h] = jnp.concatenate(split(mm(map_s[h], twice(up_s[1, h]))), axis=1)

    def step(r):
        for h in range(heads):
            hop(r, h).wait_recv()
            state = add_s[h] + mm(map_s[h], twice(recv_s[r, h]))
            send_s[r, h] = state.astype(bf16)
            hop(r, h).start()

            @pl.when(r == down_at)
            def _():
                down(h).start()

    def reads_and_join(i, carry):
        for h in (2 * i, 2 * i + 1):
            loads(h)[2].wait()
        for h in (2 * i, 2 * i + 1):
            for b in range(blocks):
                at = pl.ds(b * BLOCK, BLOCK)
                g_s[h, at, :], o_s[h, at, :] = block_reads(
                    q_s[h, at, :],
                    k_s[h, pl.ds(b * n, n), :],
                    write_s[h, b],
                    norm_s[h, b],
                    row_s[h, b],
                    tok_s[h, b],
                    masks_of(b),
                    before_s[h, b - 1] if b else None,
                )

        @pl.when(odd & (i == (pair_at == 0).astype(jnp.int32)))
        def _():
            join()

        return carry

    lax.fori_loop(0, heads // 2, reads_and_join, 0)

    def next_chain(i, carry):
        r = 1 - i

        @pl.when((sends[1] & (r == 1) & (pair_at > 1)) | (sends[0] & (r == 0) & (pair_at > 0)))
        def _():
            step(r)

        return carry

    lax.fori_loop(0, 2, next_chain, 0)
    waits = odd & (jnp.logical_not(has_after) | (pair_at == reach))
    for h in range(heads):

        @pl.when(even & has_before)
        def _():
            down(h).wait_recv()

        @pl.when(odd & (pair_at == 0))
        def _():
            enter_s[h] = up_s[0, h]

        @pl.when(waits)
        def _():
            hop(last, h).wait_recv()

        @pl.when(odd & (pair_at > 0))
        def _():
            state = up_s[0, h].astype(f32) + mm(up_s[1, h], recv_s[last, h])
            enter_s[h] = state.astype(bf16)

        out = o_s[h] + mm(g_s[h], enter_s[h])
        mean = jnp.sum(out * out, axis=1, keepdims=True) * (1.0 / width)
        flat_s[:, h * width : (h + 1) * width] = (
            out * lax.rsqrt(mean + EPS) * gain_s[...]
        ).astype(bf16)

    chunks, _, chunk = part_s.shape
    share = out_ref.shape[0]
    lower = chunks // 2
    far = lax.rem(x + 2, n_head)

    def rows_for(dest):
        return pl.ds(pl.multiple_of(dest * share, share), share)

    def relay(c):
        return pltpu.make_async_remote_copy(
            src_ref=part_s.at[c, rows_for(far), :],
            dst_ref=relay_s.at[c],
            send_sem=relay_send.at[c],
            recv_sem=relay_recv.at[c],
            device_id={"head": right if c < lower else left},
            device_id_type=MESH,
        )

    def direct(c):
        to = left if c < lower else right
        return pltpu.make_async_remote_copy(
            src_ref=part_s.at[c, rows_for(to), :],
            dst_ref=got_s.at[0, c],
            send_sem=x_send.at[0, c],
            recv_sem=x_recv.at[0, c],
            device_id={"head": to},
            device_id_type=MESH,
        )

    def summed(c):
        to = right if c < lower else left
        return pltpu.make_async_remote_copy(
            src_ref=sum_s.at[c],
            dst_ref=got_s.at[1, c],
            send_sem=x_send.at[1, c],
            recv_sem=x_recv.at[1, c],
            device_id={"head": to},
            device_id_type=MESH,
        )

    order = [c for pair in zip(range(lower), range(lower, chunks)) for c in pair]
    w_copy.wait()
    flat = flat_s[...]
    for c in order:
        part_s[c] = mm(flat, w_s[:, c * chunk : (c + 1) * chunk]).astype(bf16)
        relay(c).start()
    for c in order:
        direct(c).start()
    for c in order:
        relay(c).wait_recv()
        to = right if c < lower else left
        sum_s[c] = (part_s[c, rows_for(to), :].astype(f32) + relay_s[c].astype(f32)).astype(bf16)
        summed(c).start()
    for c in order:
        direct(c).wait_recv()
        total = part_s[c, rows_for(x), :].astype(f32) + got_s[0, c].astype(f32)
        summed(c).wait_recv()
        out_ref[:, c * chunk : (c + 1) * chunk] = (total + got_s[1, c].astype(f32)).astype(bf16)

    for r in range(2):

        @pl.when(sends[r])
        def _():
            for h in range(heads):
                hop(r, h).wait_send()

    @pl.when(relays)
    def _():
        for h in range(heads):
            down(h).wait_send()

    @pl.when(even)
    def _():
        for h in range(heads):
            up_add(h).wait_send()
            up_map(h).wait_send()

    for c in order:
        relay(c).wait_send()
        direct(c).wait_send()
        summed(c).wait_send()


def solution(mesh):
    n_seq, n_head = mesh.shape["seq"], mesh.shape["head"]

    def body(queries, keys, values, beta, gate, lengths, gain, weight):
        tokens, lanes = queries.shape[1:]
        refl, heads = beta.shape[2:]
        width = lanes // heads
        subs = tokens * refl
        blocks = tokens // BLOCK
        n = refl * BLOCK
        model = weight.shape[1]
        share = tokens // n_head
        rounds = -(-LONGEST // tokens)
        assert rounds % 2 == 0 and n_seq % 2 == 0 and n_seq // 2 > rounds // 2 + 1
        chunks = 4
        chunk = model // chunks
        hbm = pl.BlockSpec(memory_space=pltpu.HBM)
        vmem = pl.BlockSpec(memory_space=pltpu.VMEM)
        dma = pltpu.SemaphoreType.DMA
        out = pl.pallas_call(
            functools.partial(kernel, n_seq, n_head, rounds),
            out_shape=jax.ShapeDtypeStruct((share, model), bf16),
            in_specs=[hbm] * 8,
            out_specs=vmem,
            scratch_shapes=[
                pltpu.VMEM((heads, tokens, width), bf16),
                pltpu.VMEM((heads, subs, width), bf16),
                pltpu.VMEM((heads, subs, width), bf16),
                pltpu.VMEM((lanes, model), bf16),
                pltpu.VMEM((refl, heads, tokens), f32),
                pltpu.VMEM((heads, tokens), f32),
                pltpu.SMEM((lengths.shape[1],), jnp.int32),
                pltpu.VMEM((1, width), f32),
                pltpu.VMEM((2 * heads, blocks, 1, n), f32),
                pltpu.VMEM((heads, blocks, n, 1), f32),
                pltpu.VMEM((heads, blocks, BLOCK, 1), f32),
                pltpu.VMEM((blocks, n, n), f32),
                pltpu.VMEM((blocks, BLOCK, n), f32),
                pltpu.VMEM((blocks, 1, n), f32),
                pltpu.VMEM((blocks, BLOCK, 1), f32),
                pltpu.VMEM((blocks, 1, n), f32),
                pltpu.VMEM((n, n), f32),
                pltpu.VMEM((levels_of(n), n, n), bf16),
                pltpu.VMEM((heads, blocks, n, 2 * width), bf16),
                pltpu.VMEM((heads, blocks, 1, n), f32),
                pltpu.VMEM((heads, blocks - 1, width, 2 * width), bf16),
                pltpu.VMEM((heads, width, 2 * width), bf16),
                pltpu.VMEM((heads, width, width), f32),
                pltpu.VMEM((heads, tokens, width), bf16),
                pltpu.VMEM((heads, tokens, width), f32),
                pltpu.VMEM((2, heads, width, width), bf16),
                pltpu.VMEM((2, heads, width, width), bf16),
                pltpu.VMEM((2, heads, width, width), bf16),
                pltpu.VMEM((heads, width, width), bf16),
                pltpu.VMEM((heads, width, width), bf16),
                pltpu.VMEM((tokens, lanes), bf16),
                pltpu.VMEM((chunks, tokens, chunk), bf16),
                pltpu.VMEM((chunks, share, chunk), bf16),
                pltpu.VMEM((chunks, share, chunk), bf16),
                pltpu.VMEM((2, chunks, share, chunk), bf16),
                dma((3, heads)),
                dma((4,)),
                dma,
                dma((3, heads)),
                dma((3, heads)),
                dma((2, heads)),
                dma((2, heads)),
                dma((chunks,)),
                dma((chunks,)),
                dma((2, chunks)),
                dma((2, chunks)),
            ],
            compiler_params=pltpu.CompilerParams(
                collective_id=0, has_side_effects=True, vmem_limit_bytes=40 * 1024 * 1024
            ),
        )(
            *[
                pltpu.with_memory_space_constraint(a, pltpu.HBM)
                for a in (
            queries[0],
            keys[0],
            values[0],
            jnp.transpose(beta[0], (1, 2, 0)),
            jnp.transpose(gate[0], (1, 0)),
            lengths[0],
            gain[None, :],
            weight,
                )
            ]
        )
        return out[None]

    packs = ("parts", "rep")
    in_specs = (
        P(packs, "seq", "head"),
        P(packs, "seq", None, "head"),
        P(packs, "seq", None, "head"),
        P(packs, "seq", None, "head"),
        P(packs, "seq", "head"),
        P(packs, None),
        P(),
        P("head", None),
    )
    out_specs = P(packs, ("seq", "head"), None)
    return jax.shard_map(body, mesh=mesh, in_specs=in_specs, out_specs=out_specs, check_vma=False)
```

```python
import functools

import jax
import jax.numpy as jnp
from jax import lax
from jax.experimental import pallas as pl
from jax.experimental.pallas import tpu as pltpu
from jax.sharding import PartitionSpec as P

BLOCK = 64
LONGEST = 2048
EPS = 1e-06
FAR = -1e30
MESH = pl.DeviceIdType.MESH
f32 = jnp.float32
bf16 = jnp.bfloat16


def mm(a, b):
    return lax.dot_general(a, b, (((1,), (0,)), ((), ())), preferred_element_type=f32)


def mm_t(a, b):
    return lax.dot_general(a, b, (((1,), (1,)), ((), ())), preferred_element_type=f32)


def split(x):
    hi = x.astype(bf16)
    return hi, (x - hi.astype(f32)).astype(bf16)


def iota(shape, dim):
    return lax.broadcasted_iota(jnp.int32, shape, dim)


def split3(x):
    first = x.astype(bf16)
    rest = x - first.astype(f32)
    second = rest.astype(bf16)
    return first, second, (rest - second.astype(f32)).astype(bf16)


def seg_of(pos, ends):
    total = jnp.zeros_like(pos)
    for end in ends:
        total = total + (pos >= end).astype(jnp.int32)
    return total


def vectors(gate, beta):
    heads, tokens = gate.shape
    n = 2 * BLOCK
    blocks = tokens // BLOCK
    left = []
    for b in range(blocks):
        at = slice(b * BLOCK, (b + 1) * BLOCK)
        part = gate[:, at]
        left.append(jnp.concatenate([part, jnp.zeros_like(part)], axis=1))
        left.append(jnp.concatenate([beta[0][:, at], beta[1][:, at]], axis=1))
    left = jnp.concatenate(left, axis=0)
    count = left.shape[0]
    k, r = iota((n, n), 0), iota((n, n), 1)
    upto = ((k < BLOCK) & (k <= r // 2)).astype(f32)
    place = (r == 2 * (k % BLOCK) + k // BLOCK).astype(f32)
    token = ((k < BLOCK) & (k <= r)).astype(f32)
    table = jnp.concatenate([upto, place, token], axis=1).astype(bf16)
    got = mm(jnp.concatenate(split3(left), axis=0), table)
    got = got[:count] + got[count : 2 * count] + got[2 * count :]
    both = 2 * heads
    first = iota((both, n), 0) < heads
    rows, toks = [], []
    for b in range(blocks):
        mine = got[b * both : (b + 1) * both]
        rows.append(jnp.where(first, mine[:, :n], mine[:, n : 2 * n]))
        toks.append(mine[:, 2 * n :])
    return rows, toks


def block_masks(offset, ends, block):
    n = 2 * BLOCK
    start = offset + block * BLOCK
    before = sum((start - 1 >= e).astype(jnp.int32) for e in ends)
    before = jnp.where(start == 0, -1, before)
    last = sum((start + BLOCK - 1 >= e).astype(jnp.int32) for e in ends)
    seg_row = seg_of(start + iota((1, n), 1) // 2, ends)
    seg_col = seg_of(start + iota((n, 1), 0) // 2, ends)
    seg_tok = seg_of(start + iota((BLOCK, 1), 0), ends)
    i, j = iota((n, n), 0), iota((n, n), 1)
    pair = jnp.where((i >= j) & (seg_col == seg_row), 0.0, FAR)
    ti, tj = iota((BLOCK, n), 0), iota((BLOCK, n), 1)
    read = jnp.where((ti >= tj // 2) & (seg_tok == seg_row), 0.0, FAR)
    carry_row = jnp.where(seg_row == before, 0.0, FAR)
    carry_tok = jnp.where(seg_tok == before, 0.0, FAR)
    end_row = jnp.where(seg_row == last, 0.0, FAR)
    return pair, read, carry_row, carry_tok, end_row


def level_mask(n, level):
    i, j = iota((n, n), 0), iota((n, n), 1)
    return ((i > j) & (lax.shift_right_logical(i ^ j, level) == 1)).astype(f32).astype(bf16)


def levels_of(n):
    return n.bit_length() - 1


def as_cols(rows):
    cols = jnp.transpose(jnp.concatenate(rows, axis=0))
    return [cols[:, u : u + 1] for u in range(len(rows))]


def state_maps(units, masks, eye, levels):
    n = eye.shape[0]
    width = units[0][0].shape[1]
    eye16 = eye.astype(bf16)
    grams = [mm_t(k, k) for k, *_ in units]
    norms = [
        lax.rsqrt(jnp.sum(gram * eye, axis=0, keepdims=True) + EPS) for gram in grams
    ]
    beta_cols = as_cols([norm * unit[4] for norm, unit in zip(norms, units)])
    end_cols = as_cols(
        [
            jnp.exp((unit[2][:, n - 1 :] - unit[2]) + mask[4]) * norm
            for norm, unit, mask in zip(norms, units, masks)
        ]
    )
    lowers = []
    for gram, norm, beta_col, (k, v, c_row, c_col, b_row), mask in zip(
        grams, norms, beta_cols, units, masks
    ):
        ratio = jnp.exp((c_col - c_row) + mask[0])
        lower = (beta_col * ratio) * (norm * gram)
        lowers.append(split(lower - lower * eye))
    xs = [eye16 - low[0] * levels(0) for low in lowers]
    for level in range(1, levels_of(n)):
        mask = levels(level)
        ys = [mm(low[0] * mask, x).astype(bf16) for low, x in zip(lowers, xs)]
        xs = [x - mm(x, y).astype(bf16) for x, y in zip(xs, ys)]
    lefts = [
        mm(jnp.concatenate(low, axis=1), jnp.concatenate([x, x], axis=0))
        for low, x in zip(lowers, xs)
    ]
    rests = [((eye - x.astype(f32)) - left).astype(bf16) for x, left in zip(xs, lefts)]
    invs = [x.astype(f32) + mm(x, rest) for x, rest in zip(xs, rests)]
    writes = []
    for inv, norm, (k, v, c_row, c_col, b_row), mask in zip(invs, norms, units, masks):
        for_value = inv * b_row
        for_key = inv * (b_row * jnp.exp(c_row + mask[2]) * norm)
        wv = mm(jnp.concatenate(split(for_value), axis=1), jnp.concatenate([v, v], axis=0))
        wk = mm(jnp.concatenate(split(for_key), axis=1), jnp.concatenate([k, k], axis=0))
        writes.append(jnp.concatenate([wv, wk], axis=1))
    outs = []
    for write, end, norm, (k, v, c_row, c_col, b_row), mask in zip(
        writes, end_cols, norms, units, masks
    ):
        hi, lo = split(write * end)
        kt = jnp.transpose(k)
        ew = mm(jnp.concatenate([kt, kt], axis=1), jnp.concatenate([hi, lo], axis=0))
        carry_last = jnp.exp(c_row[:, n - 1 :] + mask[2][:, n - 1 :])
        outs.append((carry_last * eye - ew[:, width:], ew[:, :width], write.astype(bf16), norm))
    return outs


def after(later, earlier):
    width = later.shape[0]
    hi, lo = split(earlier)
    m_hi, m_lo = split(later[:, :width])
    total = mm(jnp.concatenate([m_hi, m_lo], axis=1), jnp.concatenate([hi, hi], axis=0))
    total = total + mm(m_hi, lo)
    return jnp.concatenate([total[:, :width], total[:, width:] + later[:, width:]], axis=1)


def compose(maps):
    first, second, third, fourth = (jnp.concatenate(m, axis=1) for m in maps)
    width = third.shape[0]
    early = after(second, first)
    whole = after(after(fourth, third), early)
    early16 = early.astype(bf16)
    three = mm(third[:, :width].astype(bf16), early16)
    three = jnp.concatenate([three[:, :width], three[:, width:] + third[:, width:]], axis=1)
    return first.astype(bf16), early16, three.astype(bf16), whole


def block_reads(q, k, write, norm, c_row, ct_col, mask, before):
    width = q.shape[1]
    qf = q.astype(f32)
    nq = lax.rsqrt(jnp.sum(qf * qf, axis=1, keepdims=True) + EPS) * width**-0.5
    weights = (jnp.exp((ct_col - c_row) + mask[1]) * nq) * (norm * mm_t(q, k))
    got = mm(weights.astype(bf16), write)
    reads = (jnp.exp(ct_col + mask[3]) * nq) * qf - got[:, width:]
    if before is None:
        return reads.astype(bf16), got[:, :width]
    wide = mm(reads.astype(bf16), before)
    return wide[:, :width].astype(bf16), got[:, :width] + wide[:, width:]


def kernel(
    n_seq,
    n_head,
    rounds,
    q_hbm,
    k_hbm,
    v_hbm,
    beta_hbm,
    gate_hbm,
    len_hbm,
    gain_hbm,
    w_hbm,
    out_ref,
    q_s,
    k_s,
    v_s,
    w_s,
    beta_s,
    gate_s,
    len_s,
    gain_s,
    row_s,
    col_s,
    tok_s,
    pair_s,
    read_s,
    crow_s,
    ctok_s,
    erow_s,
    eye_s,
    lev_s,
    write_s,
    norm_s,
    before_s,
    map_s,
    add_s,
    g_s,
    o_s,
    send_s,
    recv_s,
    up_s,
    own_s,
    enter_s,
    flat_s,
    part_s,
    relay_s,
    sum_s,
    got_s,
    in_sem,
    small_sem,
    w_sem,
    near_send,
    near_recv,
    ring_send,
    ring_recv,
    relay_send,
    relay_recv,
    x_send,
    x_recv,
):
    z = lax.axis_index("seq")
    x = lax.axis_index("head")
    heads, subs, width = k_s.shape
    tokens = q_s.shape[1]
    blocks = tokens // BLOCK
    n = 2 * BLOCK
    right, left = lax.rem(x + 1, n_head), lax.rem(x + n_head - 1, n_head)
    has_before, has_after = z > 0, z < n_seq - 1
    odd = lax.rem(z, 2) == 1
    even = jnp.logical_not(odd)
    pair_at = z // 2
    reach = rounds // 2
    relays = odd & has_after
    last = (pair_at > reach).astype(jnp.int32)
    down_at = (pair_at + 1 > reach).astype(jnp.int32)
    sends = (relays & (pair_at < reach), relays & (pair_at > 0))

    smalls = [
        pltpu.make_async_copy(src, dst, small_sem.at[i])
        for i, (src, dst) in enumerate(
            ((len_hbm, len_s), (gate_hbm, gate_s), (beta_hbm, beta_s), (gain_hbm, gain_s))
        )
    ]
    for copy in smalls:
        copy.start()
    k_rows = k_hbm.reshape(subs, heads * width)
    v_rows = v_hbm.reshape(subs, heads * width)

    def loads(h):
        lanes = pl.ds(pl.multiple_of(h * width, width), width)
        return (
            pltpu.make_async_copy(k_rows.at[:, lanes], k_s.at[h], in_sem.at[0, h]),
            pltpu.make_async_copy(v_rows.at[:, lanes], v_s.at[h], in_sem.at[1, h]),
            pltpu.make_async_copy(q_hbm.at[:, lanes], q_s.at[h], in_sem.at[2, h]),
        )

    for h in range(heads):
        for copy in loads(h)[:2]:
            copy.start()
    for h in range(heads):
        loads(h)[2].start()
    w_copy = pltpu.make_async_copy(w_hbm, w_s, w_sem)
    w_copy.start()

    barrier = pltpu.get_barrier_semaphore()
    for side in (right, left):
        pl.semaphore_signal(barrier, inc=1, device_id={"head": side}, device_id_type=MESH)

    @pl.when(has_before)
    def _():
        pl.semaphore_signal(barrier, inc=1, device_id={"seq": z - 1}, device_id_type=MESH)

    @pl.when(odd & (z > 1))
    def _():
        pl.semaphore_signal(barrier, inc=1, device_id={"seq": z - 2}, device_id_type=MESH)

    eye_s[...] = (iota((n, n), 0) == iota((n, n), 1)).astype(f32)
    for level in range(levels_of(n)):
        lev_s[level] = level_mask(n, level)
    for copy in smalls:
        copy.wait()
    offset = z * tokens
    ends, run = [], 0
    for i in range(len_s.shape[0]):
        run = run + len_s[i]
        ends.append(run)
    rows, toks = vectors(gate_s[...], [beta_s[j] for j in range(2)])
    for b in range(blocks):
        cols = jnp.transpose(rows[b])
        t_cols = jnp.transpose(toks[b])
        for h in range(heads):
            row_s[h, b] = rows[b][h : h + 1]
            row_s[heads + h, b] = rows[b][heads + h : heads + h + 1]
            col_s[h, b] = cols[:, h : h + 1]
            tok_s[h, b] = t_cols[:BLOCK, h : h + 1]
        pair_s[b], read_s[b], crow_s[b], ctok_s[b], erow_s[b] = block_masks(offset, ends, b)

    @pl.when(jnp.logical_not(has_before))
    def _():
        enter_s[...] = jnp.zeros_like(enter_s)

    def to_next(what, src, dst, sem, h, step):
        return pltpu.make_async_remote_copy(
            src_ref=src,
            dst_ref=dst,
            send_sem=sem[0].at[what, h],
            recv_sem=sem[1].at[what, h],
            device_id={"seq": jnp.minimum(z + step, n_seq - 1)},
            device_id_type=MESH,
        )

    near = (near_send, near_recv)
    ring = (ring_send, ring_recv)

    def up_add(h):
        return to_next(0, send_s.at[0, h], up_s.at[0, h], near, h, 1)

    def up_map(h):
        return to_next(1, own_s.at[h], up_s.at[1, h], near, h, 1)

    def down(h):
        return to_next(2, send_s.at[down_at, h], enter_s.at[h], near, h, 1)

    def hop(r, h):
        return to_next(r, send_s.at[r, h], recv_s.at[r, h], ring, h, 2)

    def masks_of(b):
        return pair_s[b], read_s[b], crow_s[b], ctok_s[b], erow_s[b]

    units, masks = [], []
    for h in range(heads):
        for copy in loads(h)[:2]:
            copy.wait()
    for h in range(heads):
        for b in range(blocks):
            at = pl.ds(b * n, n)
            units.append(
                (k_s[h, at, :], v_s[h, at, :], row_s[h, b], col_s[h, b], row_s[heads + h, b])
            )
            masks.append(masks_of(b))
    outs = state_maps(units, masks, eye_s[...], lambda l: lev_s[l])
    totals = [compose([m[:2] for m in outs[h * blocks : (h + 1) * blocks]]) for h in range(heads)]
    for h in range(heads):
        send_s[0, h] = totals[h][-1][:, width:].astype(bf16)
        hi, lo = split(totals[h][-1][:, :width])
        own_s[h] = hi
        map_s[h] = jnp.concatenate([hi, lo], axis=1)

    pl.semaphore_wait(barrier, 2 + has_after.astype(jnp.int32) + relays.astype(jnp.int32))

    @pl.when(even)
    def _():
        for h in range(heads):
            up_add(h).start()
        for h in range(heads):
            up_map(h).start()

    for h in range(heads):
        add_s[h] = totals[h][-1][:, width:]
        for b in range(blocks):
            write_s[h, b] = outs[h * blocks + b][2]
            norm_s[h, b] = outs[h * blocks + b][3]
        for b in range(1, blocks):
            before_s[h, b - 1] = totals[h][b - 1]

    def twice(a):
        return jnp.concatenate([a, a], axis=0)

    def join():
        for h in range(heads):
            up_add(h).wait_recv()
            add = add_s[h] + mm(map_s[h], twice(up_s[0, h]))
            add_s[h] = add

            @pl.when(relays & (pair_at < 2))
            def _():
                send_s[pair_at, h] = add.astype(bf16)
                hop(pair_at, h).start()

            @pl.when(pair_at == 0)
            def _():
                down(h).start()

        @pl.when(pair_at > 0)
        def _():
            for h in range(heads):
                up_map(h).wait_recv()
                map_s[h] = jnp.concatenate(split(mm(map_s[h], twice(up_s[1, h]))), axis=1)

    def step(r):
        for h in range(heads):
            hop(r, h).wait_recv()
            state = add_s[h] + mm(map_s[h], twice(recv_s[r, h]))
            send_s[r, h] = state.astype(bf16)
            hop(r, h).start()

            @pl.when(r == down_at)
            def _():
                down(h).start()

    def reads_and_join(i, carry):
        for h in (2 * i, 2 * i + 1):
            loads(h)[2].wait()
        for h in (2 * i, 2 * i + 1):
            for b in range(blocks):
                at = pl.ds(b * BLOCK, BLOCK)
                g_s[h, at, :], o_s[h, at, :] = block_reads(
                    q_s[h, at, :],
                    k_s[h, pl.ds(b * n, n), :],
                    write_s[h, b],
                    norm_s[h, b],
                    row_s[h, b],
                    tok_s[h, b],
                    masks_of(b),
                    before_s[h, b - 1] if b else None,
                )

        @pl.when(odd & (i == (pair_at == 0).astype(jnp.int32)))
        def _():
            join()

        return carry

    lax.fori_loop(0, heads // 2, reads_and_join, 0)

    def next_chain(i, carry):
        r = 1 - i

        @pl.when((sends[1] & (r == 1) & (pair_at > 1)) | (sends[0] & (r == 0) & (pair_at > 0)))
        def _():
            step(r)

        return carry

    lax.fori_loop(0, 2, next_chain, 0)
    waits = odd & (jnp.logical_not(has_after) | (pair_at == reach))
    for h in range(heads):

        @pl.when(even & has_before)
        def _():
            down(h).wait_recv()

        @pl.when(odd & (pair_at == 0))
        def _():
            enter_s[h] = up_s[0, h]

        @pl.when(waits)
        def _():
            hop(last, h).wait_recv()

        @pl.when(odd & (pair_at > 0))
        def _():
            state = up_s[0, h].astype(f32) + mm(up_s[1, h], recv_s[last, h])
            enter_s[h] = state.astype(bf16)

        out = o_s[h] + mm(g_s[h], enter_s[h])
        mean = jnp.sum(out * out, axis=1, keepdims=True) * (1.0 / width)
        flat_s[:, h * width : (h + 1) * width] = (
            out * lax.rsqrt(mean + EPS) * gain_s[...]
        ).astype(bf16)

    chunks, _, chunk = part_s.shape
    share = out_ref.shape[0]
    lower = chunks // 2
    far = lax.rem(x + 2, n_head)

    def rows_for(dest):
        return pl.ds(pl.multiple_of(dest * share, share), share)

    def relay(c):
        return pltpu.make_async_remote_copy(
            src_ref=part_s.at[c, rows_for(far), :],
            dst_ref=relay_s.at[c],
            send_sem=relay_send.at[c],
            recv_sem=relay_recv.at[c],
            device_id={"head": right if c < lower else left},
            device_id_type=MESH,
        )

    def direct(c):
        to = left if c < lower else right
        return pltpu.make_async_remote_copy(
            src_ref=part_s.at[c, rows_for(to), :],
            dst_ref=got_s.at[0, c],
            send_sem=x_send.at[0, c],
            recv_sem=x_recv.at[0, c],
            device_id={"head": to},
            device_id_type=MESH,
        )

    def summed(c):
        to = right if c < lower else left
        return pltpu.make_async_remote_copy(
            src_ref=sum_s.at[c],
            dst_ref=got_s.at[1, c],
            send_sem=x_send.at[1, c],
            recv_sem=x_recv.at[1, c],
            device_id={"head": to},
            device_id_type=MESH,
        )

    order = [c for pair in zip(range(lower), range(lower, chunks)) for c in pair]
    w_copy.wait()
    flat = flat_s[...]
    for c in order:
        part_s[c] = mm(flat, w_s[:, c * chunk : (c + 1) * chunk]).astype(bf16)
        relay(c).start()
    for c in order:
        direct(c).start()
    for c in order:
        relay(c).wait_recv()
        to = right if c < lower else left
        sum_s[c] = (part_s[c, rows_for(to), :].astype(f32) + relay_s[c].astype(f32)).astype(bf16)
        summed(c).start()
    for c in order:
        direct(c).wait_recv()
        total = part_s[c, rows_for(x), :].astype(f32) + got_s[0, c].astype(f32)
        summed(c).wait_recv()
        out_ref[:, c * chunk : (c + 1) * chunk] = (total + got_s[1, c].astype(f32)).astype(bf16)

    for r in range(2):

        @pl.when(sends[r])
        def _():
            for h in range(heads):
                hop(r, h).wait_send()

    @pl.when(relays)
    def _():
        for h in range(heads):
            down(h).wait_send()

    @pl.when(even)
    def _():
        for h in range(heads):
            up_add(h).wait_send()
            up_map(h).wait_send()

    @pl.when(odd & (pair_at == 0))
    def _():
        for h in range(heads):
            up_map(h).wait_recv()

    for c in order:
        relay(c).wait_send()
        direct(c).wait_send()
        summed(c).wait_send()


def solution(mesh):
    n_seq, n_head = mesh.shape["seq"], mesh.shape["head"]

    def body(queries, keys, values, beta, gate, lengths, gain, weight):
        tokens, lanes = queries.shape[1:]
        refl, heads = beta.shape[2:]
        width = lanes // heads
        subs = tokens * refl
        blocks = tokens // BLOCK
        n = refl * BLOCK
        model = weight.shape[1]
        share = tokens // n_head
        rounds = -(-LONGEST // tokens)
        assert blocks == 4 and rounds % 2 == 0 and n_seq % 2 == 0 and n_seq // 2 > rounds // 2 + 1
        chunks = 8
        chunk = model // chunks
        hbm = pl.BlockSpec(memory_space=pltpu.HBM)
        vmem = pl.BlockSpec(memory_space=pltpu.VMEM)
        dma = pltpu.SemaphoreType.DMA
        out = pl.pallas_call(
            functools.partial(kernel, n_seq, n_head, rounds),
            out_shape=jax.ShapeDtypeStruct((share, model), bf16),
            in_specs=[hbm] * 8,
            out_specs=vmem,
            scratch_shapes=[
                pltpu.VMEM((heads, tokens, width), bf16),
                pltpu.VMEM((heads, subs, width), bf16),
                pltpu.VMEM((heads, subs, width), bf16),
                pltpu.VMEM((lanes, model), bf16),
                pltpu.VMEM((refl, heads, tokens), f32),
                pltpu.VMEM((heads, tokens), f32),
                pltpu.SMEM((lengths.shape[1],), jnp.int32),
                pltpu.VMEM((1, width), f32),
                pltpu.VMEM((2 * heads, blocks, 1, n), f32),
                pltpu.VMEM((heads, blocks, n, 1), f32),
                pltpu.VMEM((heads, blocks, BLOCK, 1), f32),
                pltpu.VMEM((blocks, n, n), f32),
                pltpu.VMEM((blocks, BLOCK, n), f32),
                pltpu.VMEM((blocks, 1, n), f32),
                pltpu.VMEM((blocks, BLOCK, 1), f32),
                pltpu.VMEM((blocks, 1, n), f32),
                pltpu.VMEM((n, n), f32),
                pltpu.VMEM((levels_of(n), n, n), bf16),
                pltpu.VMEM((heads, blocks, n, 2 * width), bf16),
                pltpu.VMEM((heads, blocks, 1, n), f32),
                pltpu.VMEM((heads, blocks - 1, width, 2 * width), bf16),
                pltpu.VMEM((heads, width, 2 * width), bf16),
                pltpu.VMEM((heads, width, width), f32),
                pltpu.VMEM((heads, tokens, width), bf16),
                pltpu.VMEM((heads, tokens, width), f32),
                pltpu.VMEM((2, heads, width, width), bf16),
                pltpu.VMEM((2, heads, width, width), bf16),
                pltpu.VMEM((2, heads, width, width), bf16),
                pltpu.VMEM((heads, width, width), bf16),
                pltpu.VMEM((heads, width, width), bf16),
                pltpu.VMEM((tokens, lanes), bf16),
                pltpu.VMEM((chunks, tokens, chunk), bf16),
                pltpu.VMEM((chunks, share, chunk), bf16),
                pltpu.VMEM((chunks, share, chunk), bf16),
                pltpu.VMEM((2, chunks, share, chunk), bf16),
                dma((3, heads)),
                dma((4,)),
                dma,
                dma((3, heads)),
                dma((3, heads)),
                dma((2, heads)),
                dma((2, heads)),
                dma((chunks,)),
                dma((chunks,)),
                dma((2, chunks)),
                dma((2, chunks)),
            ],
            compiler_params=pltpu.CompilerParams(
                collective_id=0, has_side_effects=True, vmem_limit_bytes=40 * 1024 * 1024
            ),
        )(
            *[
                pltpu.with_memory_space_constraint(a, pltpu.HBM)
                for a in (
            queries[0],
            keys[0],
            values[0],
            jnp.transpose(beta[0], (1, 2, 0)),
            jnp.transpose(gate[0], (1, 0)),
            lengths[0],
            gain[None, :],
            weight,
                )
            ]
        )
        return out[None]

    packs = ("parts", "rep")
    in_specs = (
        P(packs, "seq", "head"),
        P(packs, "seq", None, "head"),
        P(packs, "seq", None, "head"),
        P(packs, "seq", None, "head"),
        P(packs, "seq", "head"),
        P(packs, None),
        P(),
        P("head", None),
    )
    out_specs = P(packs, ("seq", "head"), None)
    return jax.shard_map(body, mesh=mesh, in_specs=in_specs, out_specs=out_specs, check_vma=False)
```

```python
import functools

import jax
import jax.numpy as jnp
from jax import lax
from jax.experimental import pallas as pl
from jax.experimental.pallas import tpu as pltpu
from jax.sharding import PartitionSpec as P

BLOCK = 64
LONGEST = 2048
EPS = 1e-06
FAR = -1e30
MESH = pl.DeviceIdType.MESH
f32 = jnp.float32
bf16 = jnp.bfloat16


def mm(a, b):
    return lax.dot_general(a, b, (((1,), (0,)), ((), ())), preferred_element_type=f32)


def mm_t(a, b):
    return lax.dot_general(a, b, (((1,), (1,)), ((), ())), preferred_element_type=f32)


def split(x):
    hi = x.astype(bf16)
    return hi, (x - hi.astype(f32)).astype(bf16)


def iota(shape, dim):
    return lax.broadcasted_iota(jnp.int32, shape, dim)


def split3(x):
    first = x.astype(bf16)
    rest = x - first.astype(f32)
    second = rest.astype(bf16)
    return first, second, (rest - second.astype(f32)).astype(bf16)


def seg_of(pos, ends):
    total = jnp.zeros_like(pos)
    for end in ends:
        total = total + (pos >= end).astype(jnp.int32)
    return total


def vectors(gate, beta):
    heads, tokens = gate.shape
    n = 2 * BLOCK
    blocks = tokens // BLOCK
    left = []
    for b in range(blocks):
        at = slice(b * BLOCK, (b + 1) * BLOCK)
        part = gate[:, at]
        left.append(jnp.concatenate([part, jnp.zeros_like(part)], axis=1))
        left.append(jnp.concatenate([beta[0][:, at], beta[1][:, at]], axis=1))
    left = jnp.concatenate(left, axis=0)
    count = left.shape[0]
    k, r = iota((n, n), 0), iota((n, n), 1)
    upto = ((k < BLOCK) & (k <= r // 2)).astype(f32)
    place = (r == 2 * (k % BLOCK) + k // BLOCK).astype(f32)
    token = ((k < BLOCK) & (k <= r)).astype(f32)
    table = jnp.concatenate([upto, place, token], axis=1).astype(bf16)
    got = mm(jnp.concatenate(split3(left), axis=0), table)
    got = got[:count] + got[count : 2 * count] + got[2 * count :]
    both = 2 * heads
    first = iota((both, n), 0) < heads
    rows, toks = [], []
    for b in range(blocks):
        mine = got[b * both : (b + 1) * both]
        rows.append(jnp.where(first, mine[:, :n], mine[:, n : 2 * n]))
        toks.append(mine[:, 2 * n :])
    return rows, toks


def block_masks(offset, ends, block):
    n = 2 * BLOCK
    start = offset + block * BLOCK
    before = sum((start - 1 >= e).astype(jnp.int32) for e in ends)
    before = jnp.where(start == 0, -1, before)
    last = sum((start + BLOCK - 1 >= e).astype(jnp.int32) for e in ends)
    seg_row = seg_of(start + iota((1, n), 1) // 2, ends)
    seg_col = seg_of(start + iota((n, 1), 0) // 2, ends)
    seg_tok = seg_of(start + iota((BLOCK, 1), 0), ends)
    i, j = iota((n, n), 0), iota((n, n), 1)
    pair = jnp.where((i >= j) & (seg_col == seg_row), 0.0, FAR)
    ti, tj = iota((BLOCK, n), 0), iota((BLOCK, n), 1)
    read = jnp.where((ti >= tj // 2) & (seg_tok == seg_row), 0.0, FAR)
    carry_row = jnp.where(seg_row == before, 0.0, FAR)
    carry_tok = jnp.where(seg_tok == before, 0.0, FAR)
    end_row = jnp.where(seg_row == last, 0.0, FAR)
    return pair, read, carry_row, carry_tok, end_row


def level_mask(n, level):
    i, j = iota((n, n), 0), iota((n, n), 1)
    return ((i > j) & (lax.shift_right_logical(i ^ j, level) == 1)).astype(f32).astype(bf16)


def levels_of(n):
    return n.bit_length() - 1


def as_cols(rows):
    cols = jnp.transpose(jnp.concatenate(rows, axis=0))
    return [cols[:, u : u + 1] for u in range(len(rows))]


def state_maps(units, masks, eye, levels):
    n = eye.shape[0]
    width = units[0][0].shape[1]
    eye16 = eye.astype(bf16)
    grams = [mm_t(k, k) for k, *_ in units]
    norms = [
        lax.rsqrt(jnp.sum(gram * eye, axis=0, keepdims=True) + EPS) for gram in grams
    ]
    beta_cols = as_cols([norm * unit[4] for norm, unit in zip(norms, units)])
    end_cols = as_cols(
        [
            jnp.exp((unit[2][:, n - 1 :] - unit[2]) + mask[4]) * norm
            for norm, unit, mask in zip(norms, units, masks)
        ]
    )
    lowers = []
    for gram, norm, beta_col, (k, v, c_row, c_col, b_row), mask in zip(
        grams, norms, beta_cols, units, masks
    ):
        ratio = jnp.exp((c_col - c_row) + mask[0])
        lower = (beta_col * ratio) * (norm * gram)
        lowers.append(split(lower - lower * eye))
    xs = [eye16 - low[0] * levels(0) for low in lowers]
    for level in range(1, levels_of(n)):
        mask = levels(level)
        ys = [mm(low[0] * mask, x).astype(bf16) for low, x in zip(lowers, xs)]
        xs = [x - mm(x, y).astype(bf16) for x, y in zip(xs, ys)]
    lefts = [
        mm(jnp.concatenate(low, axis=1), jnp.concatenate([x, x], axis=0))
        for low, x in zip(lowers, xs)
    ]
    rests = [((eye - x.astype(f32)) - left).astype(bf16) for x, left in zip(xs, lefts)]
    invs = [x.astype(f32) + mm(x, rest) for x, rest in zip(xs, rests)]
    writes = []
    for inv, norm, (k, v, c_row, c_col, b_row), mask in zip(invs, norms, units, masks):
        for_value = inv * b_row
        for_key = inv * (b_row * jnp.exp(c_row + mask[2]) * norm)
        wv = mm(jnp.concatenate(split(for_value), axis=1), jnp.concatenate([v, v], axis=0))
        wk = mm(jnp.concatenate(split(for_key), axis=1), jnp.concatenate([k, k], axis=0))
        writes.append(jnp.concatenate([wv, wk], axis=1))
    outs = []
    for write, end, norm, (k, v, c_row, c_col, b_row), mask in zip(
        writes, end_cols, norms, units, masks
    ):
        hi, lo = split(write * end)
        kt = jnp.transpose(k)
        ew = mm(jnp.concatenate([kt, kt], axis=1), jnp.concatenate([hi, lo], axis=0))
        carry_last = jnp.exp(c_row[:, n - 1 :] + mask[2][:, n - 1 :])
        outs.append((carry_last * eye - ew[:, width:], ew[:, :width], write.astype(bf16), norm))
    return outs


def after(later, earlier):
    width = later.shape[0]
    hi, lo = split(earlier)
    m_hi, m_lo = split(later[:, :width])
    total = mm(jnp.concatenate([m_hi, m_lo], axis=1), jnp.concatenate([hi, hi], axis=0))
    total = total + mm(m_hi, lo)
    return jnp.concatenate([total[:, :width], total[:, width:] + later[:, width:]], axis=1)


def compose(maps):
    first, second, third, fourth = (jnp.concatenate(m, axis=1) for m in maps)
    width = third.shape[0]
    early = after(second, first)
    whole = after(after(fourth, third), early)
    early16 = early.astype(bf16)
    three = mm(third[:, :width].astype(bf16), early16)
    three = jnp.concatenate([three[:, :width], three[:, width:] + third[:, width:]], axis=1)
    return first.astype(bf16), early16, three.astype(bf16), whole


def block_reads(q, k, write, norm, c_row, ct_col, mask, before):
    width = q.shape[1]
    qf = q.astype(f32)
    nq = lax.rsqrt(jnp.sum(qf * qf, axis=1, keepdims=True) + EPS) * width**-0.5
    weights = (jnp.exp((ct_col - c_row) + mask[1]) * nq) * (norm * mm_t(q, k))
    got = mm(weights.astype(bf16), write)
    reads = (jnp.exp(ct_col + mask[3]) * nq) * qf - got[:, width:]
    if before is None:
        return reads.astype(bf16), got[:, :width]
    wide = mm(reads.astype(bf16), before)
    return wide[:, :width].astype(bf16), got[:, :width] + wide[:, width:]


def kernel(
    n_seq,
    n_head,
    rounds,
    q_hbm,
    k_hbm,
    v_hbm,
    beta_hbm,
    gate_hbm,
    len_hbm,
    gain_hbm,
    w_hbm,
    out_ref,
    q_s,
    k_s,
    v_s,
    w_s,
    beta_s,
    gate_s,
    len_s,
    gain_s,
    row_s,
    col_s,
    tok_s,
    pair_s,
    read_s,
    crow_s,
    ctok_s,
    erow_s,
    eye_s,
    lev_s,
    write_s,
    norm_s,
    before_s,
    map_s,
    add_s,
    g_s,
    o_s,
    send_s,
    recv_s,
    up_s,
    own_s,
    enter_s,
    flat_s,
    part_s,
    relay_s,
    sum_s,
    got_s,
    in_sem,
    small_sem,
    w_sem,
    near_send,
    near_recv,
    ring_send,
    ring_recv,
    relay_send,
    relay_recv,
    x_send,
    x_recv,
):
    z = lax.axis_index("seq")
    x = lax.axis_index("head")
    heads, subs, width = k_s.shape
    tokens = q_s.shape[1]
    blocks = tokens // BLOCK
    n = 2 * BLOCK
    right, left = lax.rem(x + 1, n_head), lax.rem(x + n_head - 1, n_head)
    has_before, has_after = z > 0, z < n_seq - 1
    odd = lax.rem(z, 2) == 1
    even = jnp.logical_not(odd)
    pair_at = z // 2
    reach = rounds // 2
    relays = odd & has_after
    last = (pair_at > reach).astype(jnp.int32)
    down_at = (pair_at + 1 > reach).astype(jnp.int32)
    sends = (relays & (pair_at < reach), relays & (pair_at > 0))

    smalls = [
        pltpu.make_async_copy(src, dst, small_sem.at[i])
        for i, (src, dst) in enumerate(
            ((len_hbm, len_s), (gate_hbm, gate_s), (beta_hbm, beta_s), (gain_hbm, gain_s))
        )
    ]
    for copy in smalls:
        copy.start()
    k_rows = k_hbm.reshape(subs, heads * width)
    v_rows = v_hbm.reshape(subs, heads * width)

    def loads(h):
        lanes = pl.ds(pl.multiple_of(h * width, width), width)
        return (
            pltpu.make_async_copy(k_rows.at[:, lanes], k_s.at[h], in_sem.at[0, h]),
            pltpu.make_async_copy(v_rows.at[:, lanes], v_s.at[h], in_sem.at[1, h]),
            pltpu.make_async_copy(q_hbm.at[:, lanes], q_s.at[h], in_sem.at[2, h]),
        )

    for h in range(heads):
        for copy in loads(h)[:2]:
            copy.start()
    for h in range(heads):
        loads(h)[2].start()
    w_copy = pltpu.make_async_copy(w_hbm, w_s, w_sem)
    w_copy.start()

    barrier = pltpu.get_barrier_semaphore()
    for side in (right, left):
        pl.semaphore_signal(barrier, inc=1, device_id={"head": side}, device_id_type=MESH)

    @pl.when(has_before)
    def _():
        pl.semaphore_signal(barrier, inc=1, device_id={"seq": z - 1}, device_id_type=MESH)

    @pl.when(odd & (z > 1))
    def _():
        pl.semaphore_signal(barrier, inc=1, device_id={"seq": z - 2}, device_id_type=MESH)

    eye_s[...] = (iota((n, n), 0) == iota((n, n), 1)).astype(f32)
    for level in range(levels_of(n)):
        lev_s[level] = level_mask(n, level)
    for copy in smalls:
        copy.wait()
    offset = z * tokens
    ends, run = [], 0
    for i in range(len_s.shape[0]):
        run = run + len_s[i]
        ends.append(run)
    rows, toks = vectors(gate_s[...], [beta_s[j] for j in range(2)])
    for b in range(blocks):
        cols = jnp.transpose(rows[b])
        t_cols = jnp.transpose(toks[b])
        for h in range(heads):
            row_s[h, b] = rows[b][h : h + 1]
            row_s[heads + h, b] = rows[b][heads + h : heads + h + 1]
            col_s[h, b] = cols[:, h : h + 1]
            tok_s[h, b] = t_cols[:BLOCK, h : h + 1]
        pair_s[b], read_s[b], crow_s[b], ctok_s[b], erow_s[b] = block_masks(offset, ends, b)

    @pl.when(jnp.logical_not(has_before))
    def _():
        enter_s[...] = jnp.zeros_like(enter_s)

    def to_next(what, src, dst, sem, h, step):
        return pltpu.make_async_remote_copy(
            src_ref=src,
            dst_ref=dst,
            send_sem=sem[0].at[what, h],
            recv_sem=sem[1].at[what, h],
            device_id={"seq": jnp.minimum(z + step, n_seq - 1)},
            device_id_type=MESH,
        )

    near = (near_send, near_recv)
    ring = (ring_send, ring_recv)

    def up_add(h):
        return to_next(0, send_s.at[0, h], up_s.at[0, h], near, h, 1)

    def up_map(h):
        return to_next(1, own_s.at[h], up_s.at[1, h], near, h, 1)

    def down(h):
        return to_next(2, send_s.at[down_at, h], enter_s.at[h], near, h, 1)

    def hop(r, h):
        return to_next(r, send_s.at[r, h], recv_s.at[r, h], ring, h, 2)

    def masks_of(b):
        return pair_s[b], read_s[b], crow_s[b], ctok_s[b], erow_s[b]

    units, masks = [], []
    for h in range(heads):
        for copy in loads(h)[:2]:
            copy.wait()
    for h in range(heads):
        for b in range(blocks):
            at = pl.ds(b * n, n)
            units.append(
                (k_s[h, at, :], v_s[h, at, :], row_s[h, b], col_s[h, b], row_s[heads + h, b])
            )
            masks.append(masks_of(b))
    outs = state_maps(units, masks, eye_s[...], lambda l: lev_s[l])
    totals = [compose([m[:2] for m in outs[h * blocks : (h + 1) * blocks]]) for h in range(heads)]
    for h in range(heads):
        send_s[0, h] = totals[h][-1][:, width:].astype(bf16)
        hi, lo = split(totals[h][-1][:, :width])
        own_s[h] = hi
        map_s[h] = jnp.concatenate([hi, lo], axis=1)

    pl.semaphore_wait(barrier, 2 + has_after.astype(jnp.int32) + relays.astype(jnp.int32))

    @pl.when(even)
    def _():
        for h in range(heads):
            up_add(h).start()
        for h in range(heads):
            up_map(h).start()

    for h in range(heads):
        add_s[h] = totals[h][-1][:, width:]
        for b in range(blocks):
            write_s[h, b] = outs[h * blocks + b][2]
            norm_s[h, b] = outs[h * blocks + b][3]
        for b in range(1, blocks):
            before_s[h, b - 1] = totals[h][b - 1]

    def twice(a):
        return jnp.concatenate([a, a], axis=0)

    def join():
        for h in range(heads):
            up_add(h).wait_recv()
            add = add_s[h] + mm(map_s[h], twice(up_s[0, h]))
            add_s[h] = add

            @pl.when(relays & (pair_at < 2))
            def _():
                send_s[pair_at, h] = add.astype(bf16)
                hop(pair_at, h).start()

            @pl.when(pair_at == 0)
            def _():
                down(h).start()

        @pl.when(pair_at > 0)
        def _():
            for h in range(heads):
                up_map(h).wait_recv()
                map_s[h] = jnp.concatenate(split(mm(map_s[h], twice(up_s[1, h]))), axis=1)

    def step(r):
        for h in range(heads):
            hop(r, h).wait_recv()
            state = add_s[h] + mm(map_s[h], twice(recv_s[r, h]))
            send_s[r, h] = state.astype(bf16)
            hop(r, h).start()

            @pl.when(r == down_at)
            def _():
                down(h).start()

    def reads_and_join(i, carry):
        for h in (2 * i, 2 * i + 1):
            loads(h)[2].wait()
        for h in (2 * i, 2 * i + 1):
            for b in range(blocks):
                at = pl.ds(b * BLOCK, BLOCK)
                g_s[h, at, :], o_s[h, at, :] = block_reads(
                    q_s[h, at, :],
                    k_s[h, pl.ds(b * n, n), :],
                    write_s[h, b],
                    norm_s[h, b],
                    row_s[h, b],
                    tok_s[h, b],
                    masks_of(b),
                    before_s[h, b - 1] if b else None,
                )

        @pl.when(odd & (i == (pair_at == 0).astype(jnp.int32)))
        def _():
            join()

        return carry

    lax.fori_loop(0, heads // 2, reads_and_join, 0)

    def next_chain(i, carry):
        r = 1 - i

        @pl.when((sends[1] & (r == 1) & (pair_at > 1)) | (sends[0] & (r == 0) & (pair_at > 0)))
        def _():
            step(r)

        return carry

    lax.fori_loop(0, 2, next_chain, 0)
    waits = odd & (jnp.logical_not(has_after) | (pair_at == reach))
    for h in range(heads):

        @pl.when(even & has_before)
        def _():
            down(h).wait_recv()

        @pl.when(odd & (pair_at == 0))
        def _():
            enter_s[h] = up_s[0, h]

        @pl.when(waits)
        def _():
            hop(last, h).wait_recv()

        @pl.when(odd & (pair_at > 0))
        def _():
            state = up_s[0, h].astype(f32) + mm(up_s[1, h], recv_s[last, h])
            enter_s[h] = state.astype(bf16)

        out = o_s[h] + mm(g_s[h], enter_s[h])
        mean = jnp.sum(out * out, axis=1, keepdims=True) * (1.0 / width)
        flat_s[:, h * width : (h + 1) * width] = (
            out * lax.rsqrt(mean + EPS) * gain_s[...]
        ).astype(bf16)

    chunks, _, chunk = part_s.shape
    share = out_ref.shape[0]
    lower = chunks // 2
    far = lax.rem(x + 2, n_head)

    def rows_for(dest):
        return pl.ds(pl.multiple_of(dest * share, share), share)

    def relay(c):
        return pltpu.make_async_remote_copy(
            src_ref=part_s.at[c, rows_for(far), :],
            dst_ref=relay_s.at[c],
            send_sem=relay_send.at[c],
            recv_sem=relay_recv.at[c],
            device_id={"head": right if c < lower else left},
            device_id_type=MESH,
        )

    def direct(c):
        to = left if c < lower else right
        return pltpu.make_async_remote_copy(
            src_ref=part_s.at[c, rows_for(to), :],
            dst_ref=got_s.at[0, c],
            send_sem=x_send.at[0, c],
            recv_sem=x_recv.at[0, c],
            device_id={"head": to},
            device_id_type=MESH,
        )

    def summed(c):
        to = right if c < lower else left
        return pltpu.make_async_remote_copy(
            src_ref=sum_s.at[c],
            dst_ref=got_s.at[1, c],
            send_sem=x_send.at[1, c],
            recv_sem=x_recv.at[1, c],
            device_id={"head": to},
            device_id_type=MESH,
        )

    order = [c for pair in zip(range(lower), range(lower, chunks)) for c in pair]
    w_copy.wait()
    flat = flat_s[...]
    for c in order:
        part_s[c] = mm(flat, w_s[:, c * chunk : (c + 1) * chunk]).astype(bf16)
        relay(c).start()
    for c in order:
        direct(c).start()
    for c in order:
        relay(c).wait_recv()
        to = right if c < lower else left
        sum_s[c] = (part_s[c, rows_for(to), :].astype(f32) + relay_s[c].astype(f32)).astype(bf16)
        summed(c).start()
    for c in order:
        direct(c).wait_recv()
        total = part_s[c, rows_for(x), :].astype(f32) + got_s[0, c].astype(f32)
        summed(c).wait_recv()
        out_ref[:, c * chunk : (c + 1) * chunk] = (total + got_s[1, c].astype(f32)).astype(bf16)

    for r in range(2):

        @pl.when(sends[r])
        def _():
            for h in range(heads):
                hop(r, h).wait_send()

    @pl.when(relays)
    def _():
        for h in range(heads):
            down(h).wait_send()

    @pl.when(even)
    def _():
        for h in range(heads):
            up_add(h).wait_send()
            up_map(h).wait_send()

    @pl.when(odd & (pair_at == 0))
    def _():
        for h in range(heads):
            up_map(h).wait_recv()

    for c in order:
        relay(c).wait_send()
        direct(c).wait_send()
        summed(c).wait_send()


def solution(mesh):
    n_seq, n_head = mesh.shape["seq"], mesh.shape["head"]

    def body(queries, keys, values, beta, gate, lengths, gain, weight):
        tokens, lanes = queries.shape[1:]
        refl, heads = beta.shape[2:]
        width = lanes // heads
        subs = tokens * refl
        blocks = tokens // BLOCK
        n = refl * BLOCK
        model = weight.shape[1]
        share = tokens // n_head
        rounds = -(-LONGEST // tokens)
        assert blocks == 4 and rounds % 2 == 0 and n_seq % 2 == 0 and n_seq // 2 > rounds // 2 + 1
        chunks = 4
        chunk = model // chunks
        hbm = pl.BlockSpec(memory_space=pltpu.HBM)
        vmem = pl.BlockSpec(memory_space=pltpu.VMEM)
        dma = pltpu.SemaphoreType.DMA
        out = pl.pallas_call(
            functools.partial(kernel, n_seq, n_head, rounds),
            out_shape=jax.ShapeDtypeStruct((share, model), bf16),
            in_specs=[hbm] * 8,
            out_specs=vmem,
            scratch_shapes=[
                pltpu.VMEM((heads, tokens, width), bf16),
                pltpu.VMEM((heads, subs, width), bf16),
                pltpu.VMEM((heads, subs, width), bf16),
                pltpu.VMEM((lanes, model), bf16),
                pltpu.VMEM((refl, heads, tokens), f32),
                pltpu.VMEM((heads, tokens), f32),
                pltpu.SMEM((lengths.shape[1],), jnp.int32),
                pltpu.VMEM((1, width), f32),
                pltpu.VMEM((2 * heads, blocks, 1, n), f32),
                pltpu.VMEM((heads, blocks, n, 1), f32),
                pltpu.VMEM((heads, blocks, BLOCK, 1), f32),
                pltpu.VMEM((blocks, n, n), f32),
                pltpu.VMEM((blocks, BLOCK, n), f32),
                pltpu.VMEM((blocks, 1, n), f32),
                pltpu.VMEM((blocks, BLOCK, 1), f32),
                pltpu.VMEM((blocks, 1, n), f32),
                pltpu.VMEM((n, n), f32),
                pltpu.VMEM((levels_of(n), n, n), bf16),
                pltpu.VMEM((heads, blocks, n, 2 * width), bf16),
                pltpu.VMEM((heads, blocks, 1, n), f32),
                pltpu.VMEM((heads, blocks - 1, width, 2 * width), bf16),
                pltpu.VMEM((heads, width, 2 * width), bf16),
                pltpu.VMEM((heads, width, width), f32),
                pltpu.VMEM((heads, tokens, width), bf16),
                pltpu.VMEM((heads, tokens, width), f32),
                pltpu.VMEM((2, heads, width, width), bf16),
                pltpu.VMEM((2, heads, width, width), bf16),
                pltpu.VMEM((2, heads, width, width), bf16),
                pltpu.VMEM((heads, width, width), bf16),
                pltpu.VMEM((heads, width, width), bf16),
                pltpu.VMEM((tokens, lanes), bf16),
                pltpu.VMEM((chunks, tokens, chunk), bf16),
                pltpu.VMEM((chunks, share, chunk), bf16),
                pltpu.VMEM((chunks, share, chunk), bf16),
                pltpu.VMEM((2, chunks, share, chunk), bf16),
                dma((3, heads)),
                dma((4,)),
                dma,
                dma((3, heads)),
                dma((3, heads)),
                dma((2, heads)),
                dma((2, heads)),
                dma((chunks,)),
                dma((chunks,)),
                dma((2, chunks)),
                dma((2, chunks)),
            ],
            compiler_params=pltpu.CompilerParams(
                collective_id=0, has_side_effects=True, vmem_limit_bytes=40 * 1024 * 1024
            ),
        )(
            *[
                pltpu.with_memory_space_constraint(a, pltpu.HBM)
                for a in (
            queries[0],
            keys[0],
            values[0],
            jnp.transpose(beta[0], (1, 2, 0)),
            jnp.transpose(gate[0], (1, 0)),
            lengths[0],
            gain[None, :],
            weight,
                )
            ]
        )
        return out[None]

    packs = ("parts", "rep")
    in_specs = (
        P(packs, "seq", "head"),
        P(packs, "seq", None, "head"),
        P(packs, "seq", None, "head"),
        P(packs, "seq", None, "head"),
        P(packs, "seq", "head"),
        P(packs, None),
        P(),
        P("head", None),
    )
    out_specs = P(packs, ("seq", "head"), None)
    return jax.shard_map(body, mesh=mesh, in_specs=in_specs, out_specs=out_specs, check_vma=False)
```
